32 devices in a mesh: dp: 8 (over z, y), fsdp: 4 (over x, core).
Axes of the slice: x: 2, y: 2, z: 4, core: 2. Of those that a mesh axis runs over, the one named last changes fastest.
Arguments:
- tokens: bfloat16 [2, 32768, 512], P(None, ('dp', 'fsdp')), may hold values from -6 to 6
- out_grad: bfloat16 [2, 32768, 512], P(None, ('dp', 'fsdp')), may hold values from -6 to 6
- seq_lengths: int32 [2, 32], P(None, ('dp', 'fsdp')), may hold values from 256 to 1024, as said below
- send_to: int32 [2, 32, 8], P(None, ('dp', 'fsdp')), may hold values from 0 to 7, each once within a row
- slot_of: int32 [2, 32, 8], P(None, ('dp', 'fsdp')), may hold values from 0 to 7, each once within a row
- first_gain: bfloat16 [512], P(('dp', 'fsdp')), may hold values from 0.5 to 1.5
- first_shift: bfloat16 [512], P(('dp', 'fsdp')), may hold values from -1.75 to 1.75
- joint_weight: bfloat16 [512, 1536], P(('dp', 'fsdp')), may hold values from -0.25 to 0.25
- query_bias: bfloat16 [512], P(('dp', 'fsdp')), may hold values from -3 to 3
- value_bias: bfloat16 [512], P(('dp', 'fsdp')), may hold values from -1.75 to 1.75
- mix_weight: bfloat16 [512, 512], P(('dp', 'fsdp')), may hold values from -1 to 1
- mix_bias: bfloat16 [512], P(('dp', 'fsdp')), may hold values from -1.75 to 1.75
- second_gain: bfloat16 [512], P(('dp', 'fsdp')), may hold values from 0.5 to 1.5
- second_shift: bfloat16 [512], P(('dp', 'fsdp')), may hold values from -1.75 to 1.75
- up_weight: bfloat16 [512, 2048], P(('dp', 'fsdp')), may hold values from -0.25 to 0.25
- up_bias: bfloat16 [2048], P(('dp', 'fsdp')), may hold values from -3 to 3
- down_weight: bfloat16 [2048, 512], P(None, ('dp', 'fsdp')), may hold values from -0.125 to 0.125
- down_bias: bfloat16 [512], P(('dp', 'fsdp')), may hold values from -1.75 to 1.75
Outputs:
- layer_output: bfloat16 [2, 32768, 512], P(None, ('dp', 'fsdp'))
- input_grad: bfloat16 [2, 32768, 512], P(None, ('dp', 'fsdp'))
- first_gain_grad: float32 [512], P(('dp', 'fsdp'))
- first_shift_grad: float32 [512], P(('dp', 'fsdp'))
- joint_weight_grad: float32 [512, 1536], P(('dp', 'fsdp'))
- query_bias_grad: float32 [512], P(('dp', 'fsdp'))
- value_bias_grad: float32 [512], P(('dp', 'fsdp'))
- mix_weight_grad: float32 [512, 512], P(('dp', 'fsdp'))
- mix_bias_grad: float32 [512], P(('dp', 'fsdp'))
- second_gain_grad: float32 [512], P(('dp', 'fsdp'))
- second_shift_grad: float32 [512], P(('dp', 'fsdp'))
- up_weight_grad: float32 [512, 2048], P(('dp', 'fsdp'))
- up_bias_grad: float32 [2048], P(('dp', 'fsdp'))
- down_weight_grad: float32 [2048, 512], P(None, ('dp', 'fsdp'))
- down_bias_grad: float32 [512], P(('dp', 'fsdp'))
The draws below stay inside these ranges and needn't reach their ends.
Inputs may be any that keep to these rules, and one draw needn't show every extreme that they name: `seq_lengths`: in every micro-batch some device's sequence fills all 1024 slots; the live slots are the first of a buffer. `send_to`: each row is a permutation: a device sends exactly one piece to each device of its fsdp index. `slot_of`: each row is a permutation: a device receives exactly one piece from each device of its fsdp index.
All inputs are finite; a program needn't handle non-finite values.
Results may differ from the reference program's by a relative error of at most 0.017.
Values may be sent and summed in bfloat16 or wider, within the bound.
A program may use at most 320 MiB of HBM per device.

```python
import jax
import jax.numpy as jnp
from jax import lax

D = 512
HEADS = 8
HEAD_DIM = 64
FF = 2048
CAP = 1024
MICRO = 2
TOKENS = 32768
PIECE = 128
MIN_LEN = 256
N_DP = 8
N_FSDP = 4
DEVICES = 32


def draw_seq_lengths(key, part):
    first, second = jax.random.split(key)
    lengths = jax.random.randint(first, (MICRO, DEVICES), MIN_LEN, CAP + 1)
    spot = jax.random.randint(second, (MICRO, 1), 0, DEVICES)
    filled = jnp.arange(DEVICES)[None, :] == spot
    return jnp.where(filled, CAP, lengths).astype(jnp.int32)


def strengthened(values, stream_key, source, target, parts, factor):
    def block_of(position):
        return (jnp.arange(values.shape[position]) // (values.shape[position] // parts)).reshape((-1,) + (1,) * (values.ndim - 1 - position))

    one_side = jax.random.permutation(stream_key, parts)[block_of(target)]
    second = (block_of(target) + parts // 2) % parts
    return jnp.where((block_of(source) == one_side) | (block_of(source) == second), factor * values, values)


def shard_levels(own_key, extent, shards, least, high):
    level, own = 1.0, jax.random.fold_in(own_key, 6)
    for position, parts in shards:
        draws = jnp.exp(jax.random.uniform(jax.random.fold_in(own, position), (parts,), jnp.float32, least / len(shards), high / len(shards)))
        level = level * jnp.repeat(draws, extent[position] // parts).reshape([-1 if axis == position else 1 for axis in range(len(extent))])
    return level


def normal_values(rng, dims, scale, most, cuts=(), kind=jnp.bfloat16):
    drawn = jax.random.normal(rng, dims, jnp.float32) * scale
    if len(cuts) > 0:
        drawn = shard_levels(rng, dims, cuts, -0.22, 0.18) * drawn
    return jnp.clip(drawn, min=-most, max=most).astype(kind)


def gaussian_with(own_key, shape, width, bound, cuts, heavy, kind=jnp.bfloat16):
    values = width * jax.random.normal(own_key, shape, jnp.float32)
    if cuts:
        values = values * shard_levels(own_key, shape, cuts, -0.22, 0.18)
    return jnp.clip(strengthened(values, jax.random.fold_in(own_key, 3), *heavy), -bound, bound).astype(kind)


def setup_inputs(seed: int = 0) -> dict:
    key_of = jax.random.split(jax.random.key(seed), 19)
    return {
        "tokens": normal_values(key_of[0], (MICRO, TOKENS, D), 1.0, 6.0, ((1, 32),)),
        "out_grad": gaussian_with(key_of[1], (MICRO, TOKENS, D), 1.0, 6.0, ((1, 32),), (1, 2, 32, 2.75)),
        "seq_lengths": draw_seq_lengths(jax.random.fold_in(key_of[18], 71), 0),
        "send_to": jax.vmap(lambda own: jax.random.permutation(own, N_DP))(jax.random.split(key_of[3], MICRO * DEVICES)).reshape((MICRO, DEVICES, N_DP)).astype(jnp.int32),
        "slot_of": jax.vmap(lambda own: jax.random.permutation(own, N_DP))(jax.random.split(key_of[4], MICRO * DEVICES)).reshape((MICRO, DEVICES, N_DP)).astype(jnp.int32),
        "first_gain": jnp.clip(1.0 + 0.1 * jax.random.normal(key_of[5], (D,), jnp.float32), 0.5, 1.5).astype(jnp.bfloat16),
        "first_shift": normal_values(key_of[6], (D,), 0.3, 1.75, ((0, 32),)),
        "joint_weight": normal_values(key_of[7], (D, 3 * D), D ** -0.5, 0.25, ((0, 32),)),
        "query_bias": normal_values(key_of[8], (D,), 0.5, 3.0, ((0, 32),)),
        "value_bias": normal_values(key_of[9], (D,), 0.3, 1.75, ((0, 32),)),
        "mix_weight": normal_values(key_of[10], (D, D), (D // 16) ** -0.5, 1.0, ((0, 32),)),
        "mix_bias": normal_values(key_of[11], (D,), 0.3, 1.75, ((0, 32),)),
        "second_gain": jnp.clip(1.0 + 0.1 * jax.random.normal(key_of[12], (D,), jnp.float32), 0.5, 1.5).astype(jnp.bfloat16),
        "second_shift": normal_values(key_of[13], (D,), 0.3, 1.75, ((0, 32),)),
        "up_weight": normal_values(key_of[14], (D, FF), D ** -0.5, 0.25, ((0, 32),)),
        "up_bias": normal_values(key_of[15], (FF,), 0.5, 3.0, ((0, 32),)),
        "down_weight": normal_values(key_of[16], (FF, D), FF ** -0.5, 0.125, ((1, 32),)),
        "down_bias": normal_values(key_of[17], (D,), 0.3, 1.75, ((0, 32),)),
    }


precise = lax.Precision.HIGHEST
masked_score = -1e+30

@jax.custom_vjp
def low(v):
    return lax.optimization_barrier(v.astype(jnp.bfloat16)).astype(jnp.float32)

@jax.custom_vjp
def low_back(v):
    return v

def low_keep(v):
    return (low(v), None)

def low_pass(kept, grad):
    return (grad,)

def back_keep(v):
    return (v, None)

def back_low(kept, grad):
    return (low(grad),)
low.defvjp(low_keep, low_pass)
low_back.defvjp(back_keep, back_low)

def layer_norm(rows, gain, shift):
    center = rows - lax.optimization_barrier(jnp.mean(rows, axis=-1, keepdims=True))
    spread = lax.optimization_barrier(jnp.mean(center * center, axis=-1, keepdims=True))
    return center * lax.rsqrt(spread + 1e-05) * gain + shift

def inverse_last(order):
    count = order.shape[-1]
    hits = order[..., :, None] == jnp.arange(count, dtype=jnp.int32)
    picks = jnp.arange(count, dtype=jnp.int32)[:, None]
    return lax.optimization_barrier(jnp.sum(jnp.where(hits, picks, 0), axis=-2)).astype(jnp.int32)

def one_sequence(tables, inputs, length):
    first_gain, first_shift, joint_weight, query_bias, value_bias, mix_weight, mix_bias, second_gain, second_shift, up_weight, up_bias, down_weight, down_bias = tables
    slots = jnp.arange(CAP, dtype=jnp.int32)
    key_live = slots < length
    live = key_live.astype(jnp.float32)[:, None]
    first_in = low(layer_norm(inputs, first_gain, first_shift))
    joint_bias = jnp.concatenate([query_bias, jnp.zeros_like(query_bias), value_bias])
    joint = low(low_back(jnp.dot(first_in, joint_weight, precision=precise) + joint_bias))
    queries = joint[:, :D].reshape(CAP, HEADS, HEAD_DIM)
    keys = joint[:, D:2 * D].reshape(CAP, HEADS, HEAD_DIM)
    values = joint[:, 2 * D:].reshape(CAP, HEADS, HEAD_DIM)
    scores = low_back(jnp.einsum('qhd,khd->hqk', queries, keys, precision=precise) * HEAD_DIM ** (-0.5))
    scores = jnp.where(key_live[None, None, :], scores, masked_score)
    probs = low(jax.nn.softmax(scores, axis=-1))
    attended = low(low_back(jnp.einsum('hqk,khd->qhd', probs, values, precision=precise))).reshape(CAP, D)
    middle = inputs + live * low_back(jnp.dot(attended, mix_weight, precision=precise) + mix_bias)
    second_in = low(layer_norm(middle, second_gain, second_shift))
    pre_act = low_back(jnp.dot(second_in, up_weight, precision=precise) + up_bias)
    hidden = low(jax.nn.gelu(pre_act, approximate=False))
    return middle + live * low_back(jnp.dot(hidden, down_weight, precision=precise) + down_bias)

def reference(tokens, out_grad, seq_lengths, send_to, slot_of, first_gain, first_shift, joint_weight, query_bias, value_bias, mix_weight, mix_bias, second_gain, second_shift, up_weight, up_bias, down_weight, down_bias):
    tables = tuple((item.astype(jnp.float32) for item in (first_gain, first_shift, joint_weight, query_bias, value_bias, mix_weight, mix_bias, second_gain, second_shift, up_weight, up_bias, down_weight, down_bias)))
    sends = send_to.reshape(MICRO, N_DP, N_FSDP, N_DP)
    slots = slot_of.reshape(MICRO, N_DP, N_FSDP, N_DP)
    send_inverse = inverse_last(sends)
    slot_inverse = inverse_last(slots)
    at_micro = jnp.arange(MICRO, dtype=jnp.int32)[:, None, None, None]
    at_first = jnp.arange(N_DP, dtype=jnp.int32)[None, :, None, None]
    at_fsdp = jnp.arange(N_FSDP, dtype=jnp.int32)[None, None, :, None]
    source_dev = slot_inverse
    source_piece = send_inverse[at_micro, source_dev, at_fsdp, at_first]
    target_dev = sends
    target_slot = slots[at_micro, target_dev, at_fsdp, at_first]
    lengths = seq_lengths.reshape(MICRO * DEVICES)
    checked = jax.checkpoint(one_sequence)

    def run(inputs, weights):
        pieces = inputs.reshape(MICRO, N_DP, N_FSDP, N_DP, PIECE, D)
        routed = pieces[at_micro, source_dev, at_fsdp, source_piece].reshape(MICRO * DEVICES, CAP, D)

        def advance(carry, item):
            return (carry, checked(weights, item[0], item[1]))
        unused, done = lax.scan(advance, jnp.zeros((), jnp.float32), (routed, lengths))
        done = done.reshape(MICRO, N_DP, N_FSDP, N_DP, PIECE, D)
        back = done[at_micro, target_dev, at_fsdp, target_slot]
        return back.reshape(MICRO, TOKENS, D)
    result, pull = jax.vjp(run, tokens.astype(jnp.float32), tables)
    token_grad, grads = pull(out_grad.astype(jnp.float32))
    return (result.astype(jnp.bfloat16), token_grad.astype(jnp.bfloat16), grads[0], grads[1], grads[2], grads[3], grads[4], grads[5], grads[6], grads[7], grads[8], grads[9], grads[10], grads[11], grads[12])
```

```python
import functools
import math

import jax
import jax.numpy as jnp
from jax import lax
from jax.experimental import pallas as pl
from jax.experimental.pallas import tpu as pltpu
from jax.sharding import PartitionSpec as P

HEADS = 8
HEAD_DIM = 64
BLK = 256

f32, bf16 = jnp.float32, jnp.bfloat16
epsilon = 1e-05
masked_score = -1e30
root_half = math.sqrt(0.5)
gauss_norm = 1.0 / math.sqrt(2.0 * math.pi)


def nn(a, b):
    return lax.dot_general(a, b, (((1,), (0,)), ((), ())), preferred_element_type=f32)


def nt(a, b):
    return lax.dot_general(a, b, (((1,), (1,)), ((), ())), preferred_element_type=f32)


def tn(a, b):
    return lax.dot_general(a, b, (((0,), (0,)), ((), ())), preferred_element_type=f32)


def normalize(rows):
    center = rows - jnp.mean(rows, axis=-1, keepdims=True)
    spread = jnp.mean(center * center, axis=-1, keepdims=True)
    factor = lax.rsqrt(spread + epsilon)
    return center * factor, factor


def norm_back(grad_norm, normed, factor):
    first_mean = jnp.mean(grad_norm, axis=-1, keepdims=True)
    second_mean = jnp.mean(grad_norm * normed, axis=-1, keepdims=True)
    return factor * (grad_norm - first_mean - normed * second_mean)


def three_parts(v):
    hi = v.astype(bf16).astype(f32)
    mid = (v - hi).astype(bf16).astype(f32)
    return hi, mid, v - hi - mid


def col_sum(v):
    return jnp.sum(v, axis=0, keepdims=True)


def micro_kernel(first, *refs):
    x_ref, g_ref, live_ref, w_ref, vec_ref, upb_ref = refs[:6]
    refs = refs[6:]
    if not first:
        prev_ref, vprev_ref, uprev_ref = refs[:3]
        refs = refs[3:]
    final_ref, tg_ref, grad_ref, vsum_ref, usum_ref = refs[:5]
    (q_ref, k_ref, v_ref, att_ref, qaug_ref, first_t, second_t, down_t, att_t, mixin_ref, mg_ref,
     dout_ref, hid_ref, pre_ref, kaug, vaug_a, vaug_b, dk_acc, dv_acc, acc_a, acc_b) = refs[5:]
    rows, width = x_ref.shape
    hidden = upb_ref.shape[1]
    blocks = rows // BLK
    pairs = width // 128
    mix_at = 3 * width
    up_at = mix_at + width
    down_at = up_at + hidden
    lane = lax.broadcasted_iota(jnp.int32, (1, 128), 1)
    low_half = lane < HEAD_DIM

    def at(i, size=BLK):
        return pl.ds(pl.multiple_of(i * size, size), size)

    if first:
        vsum_ref[...] = jnp.zeros_like(vsum_ref)
        usum_ref[...] = jnp.zeros_like(usum_ref)
    else:
        vsum_ref[...] = vprev_ref[...]
        usum_ref[...] = uprev_ref[...]

    def row(ref, n):
        return ref[n : n + 1, :]

    live_all = live_ref[...]
    mask_aug = jnp.where(
        lane == 0, (live_all - 1.0) * (-masked_score), jnp.where(lane < 4, 1.0, 0.0)
    ).astype(bf16)
    kaug[:, 128:] = mask_aug
    vaug_a[:, 128:] = jnp.ones((rows, 128), bf16)
    vaug_b[:, 128:] = jnp.ones((rows, 128), bf16)

    def project(i, carry):
        rs = at(i)
        normed, _ = normalize(x_ref[rs, :].astype(f32))
        first_in = (normed * row(vec_ref, 0) + row(vec_ref, 1)).astype(bf16)
        first_t[:, rs] = first_in.T
        query = (nn(first_in, w_ref[:, :width]) + row(vec_ref, 2)).astype(bf16)
        q_ref[rs, :] = query * jnp.array(HEAD_DIM ** (-0.5), bf16)
        k_ref[rs, :] = nn(first_in, w_ref[:, width : 2 * width]).astype(bf16)
        v_ref[rs, :] = (nn(first_in, w_ref[:, 2 * width : 3 * width]) + row(vec_ref, 3)).astype(bf16)
        return carry

    lax.fori_loop(0, blocks, project, 0)

    def attend_pair(p, carry):
        ls = at(p, 128)
        kaug[:, :128] = k_ref[:, ls]
        values = v_ref[:, ls]
        zero = jnp.zeros_like(values)
        vaug_a[:, :128] = jnp.where(low_half, values, zero)
        vaug_b[:, :128] = jnp.where(low_half, zero, values)

        def attend(i, carry):
            rs = at(i)
            query = q_ref[rs, ls]
            qzero = jnp.zeros_like(query)
            one = jnp.broadcast_to(jnp.where(lane == 0, 1.0, 0.0), (BLK, 128)).astype(bf16)
            out = None
            for half, vaug in ((0, vaug_a), (1, vaug_b)):
                mine = jnp.where(low_half if half == 0 else jnp.logical_not(low_half), query, qzero)
                scores = nt(jnp.concatenate([mine, one], axis=1), kaug[...])
                peak = jnp.max(scores, axis=-1, keepdims=True)
                chances = jnp.exp(scores - peak).astype(bf16)
                got = nn(chances, vaug[...])
                total = got[:, 128:]
                lse = peak + jnp.log(total)
                hi, mid, lo = three_parts(lse)
                qaug_ref[2 * p + half, rs, :] = jnp.where(
                    lane == 0, 1.0,
                    jnp.where(lane == 1, -hi, jnp.where(lane == 2, -mid, jnp.where(lane == 3, -lo, 0.0))),
                ).astype(bf16)
                part = got[:, :128] / total
                out = part if out is None else out + part
            att_ref[rs, ls] = out
            return carry

        return lax.fori_loop(0, blocks, attend, carry)

    lax.fori_loop(0, pairs, attend_pair, 0)

    chunk = 512
    mix_w = w_ref.at[:, mix_at:up_at]

    def feed(i, carry):
        rs = at(i)
        live = live_ref[rs, :]
        attended = att_ref[rs, :].astype(bf16)
        att_t[:, rs] = attended.T
        middle = x_ref[rs, :].astype(f32) + live * (nn(attended, mix_w[...]) + row(vec_ref, 4))
        second_norm, factor = normalize(middle)
        second_in = (second_norm * row(vec_ref, 5) + row(vec_ref, 6)).astype(bf16)
        second_t[:, rs] = second_in.T
        outer = g_ref[rs, :].astype(f32)
        down_in = (live * outer).astype(bf16)
        down_t[:, rs] = down_in.T
        vsum_ref[7:8, :] += col_sum(down_in.astype(f32))
        acc_a[...] = jnp.zeros_like(acc_a)
        acc_b[...] = jnp.zeros_like(acc_b)

        def part(c, carry):
            cs = at(c, chunk)
            up = w_ref[:, pl.ds(pl.multiple_of(up_at + c * chunk, chunk), chunk)]
            down = w_ref[:, pl.ds(pl.multiple_of(down_at + c * chunk, chunk), chunk)]
            pre = nn(second_in, up) + upb_ref[:, cs]
            phi = 0.5 * (1.0 + lax.erf(pre * root_half))
            hid = (pre * phi).astype(bf16)
            slope = phi + pre * jnp.exp(-0.5 * pre * pre) * gauss_norm
            hid_ref[rs, cs] = hid
            acc_a[...] += nt(hid, down)
            pre_grad = (nn(down_in, down) * slope).astype(bf16)
            pre_ref[rs, cs] = pre_grad
            usum_ref[:, cs] += col_sum(pre_grad.astype(f32))
            acc_b[...] += nt(pre_grad, up)
            return carry

        lax.fori_loop(0, hidden // chunk, part, 0)
        final_ref[rs, :] = (middle + live * (acc_a[...] + row(vec_ref, 7))).astype(bf16)
        second_in_grad = acc_b[...]
        vsum_ref[5:6, :] += col_sum(second_in_grad * second_norm)
        vsum_ref[6:7, :] += col_sum(second_in_grad)
        middle_grad = outer + norm_back(second_in_grad * row(vec_ref, 5), second_norm, factor)
        mg_ref[rs, :] = middle_grad
        mix_in = (live * middle_grad).astype(bf16)
        mixin_ref[rs, :] = mix_in
        vsum_ref[4:5, :] += col_sum(mix_in.astype(f32))
        dout_ref[rs, :] = nt(mix_in, mix_w[...]).astype(bf16)
        return carry

    lax.fori_loop(0, blocks, feed, 0)

    def put(value, cs):
        if not first:
            value = value + prev_ref[:, cs]
        grad_ref[:, cs] = value.astype(grad_ref.dtype)

    def wide(lhs_t, rhs_ref, base, count):
        def one(c, carry):
            put(nn(lhs_t[...], rhs_ref[:, at(c, chunk)]),
                pl.ds(pl.multiple_of(base + c * chunk, chunk), chunk))
            return carry
        lax.fori_loop(0, count, one, 0)

    wide(down_t, hid_ref, down_at, hidden // chunk)
    wide(second_t, pre_ref, up_at, hidden // chunk)
    wide(att_t, mixin_ref, mix_at, width // chunk)

    joint_grad = hid_ref

    def back_pair(p, carry):
        ls = at(p, 128)
        keys = k_ref[:, ls]
        kaug[:, :128] = keys
        vaug_a[:, :128] = v_ref[:, ls]
        vaug_a[:, 128:] = kaug[:, 128:]
        zero = jnp.zeros_like(keys)
        vaug_b[:, :128] = jnp.where(low_half, keys, zero)
        vaug_b[:, 128:] = jnp.where(low_half, zero, keys)
        dk_acc[...] = jnp.zeros_like(dk_acc)
        dv_acc[...] = jnp.zeros_like(dv_acc)

        def back(i, carry):
            rs = at(i)
            query = q_ref[rs, ls]
            grad = dout_ref[rs, ls]
            both = grad.astype(f32) * att_ref[rs, ls]
            dq = None
            for half in (0, 1):
                keep = low_half if half == 0 else jnp.logical_not(low_half)
                mine = jnp.where(keep, query, jnp.zeros_like(query))
                grads = jnp.where(keep, grad, jnp.zeros_like(grad))
                inner = jnp.sum(jnp.where(keep, both, 0.0), axis=-1, keepdims=True)
                hi, mid, lo = three_parts(inner)
                gaug = jnp.where(
                    lane == 1, -hi, jnp.where(lane == 2, -mid, jnp.where(lane == 3, -lo, 0.0))
                ).astype(bf16)
                scores = nt(kaug[...], jnp.concatenate([mine, qaug_ref[2 * p + half, rs, :]], axis=1))
                chances = jnp.exp(scores)
                centered = nt(vaug_a[...], jnp.concatenate([grads, gaug], axis=1))
                score_grad = (chances * centered).astype(bf16)
                dv_acc[...] += nn(chances.astype(bf16), grads)
                dk_acc[...] += nn(score_grad, mine)
                part = tn(score_grad, vaug_b[:, 128 * half : 128 * half + 128])
                dq = part if dq is None else dq + part
            joint_grad[rs, ls] = (dq * HEAD_DIM ** (-0.5)).astype(bf16)
            return carry

        lax.fori_loop(0, blocks, back, 0)
        joint_grad[:, pl.ds(pl.multiple_of(width + p * 128, 128), 128)] = dk_acc[...].astype(bf16)
        joint_grad[:, pl.ds(pl.multiple_of(2 * width + p * 128, 128), 128)] = dv_acc[...].astype(bf16)
        return carry

    lax.fori_loop(0, pairs, back_pair, 0)

    wide(first_t, joint_grad, 0, 3 * width // chunk)

    def back_first(i, carry):
        rs = at(i)
        grads = joint_grad[rs, : 3 * width]
        vsum_ref[2:3, :] += col_sum(grads[:, :width].astype(f32))
        vsum_ref[3:4, :] += col_sum(grads[:, 2 * width :].astype(f32))
        first_in_grad = nt(grads, w_ref[:, : 3 * width])
        normed, factor = normalize(x_ref[rs, :].astype(f32))
        vsum_ref[0:1, :] += col_sum(first_in_grad * normed)
        vsum_ref[1:2, :] += col_sum(first_in_grad)
        tg_ref[rs, :] = (
            mg_ref[rs, :] + norm_back(first_in_grad * row(vec_ref, 0), normed, factor)
        ).astype(bf16)
        return carry

    lax.fori_loop(0, blocks, back_first, 0)


def micro_call(x, g, live, weights, vec, upb, previous=None):
    rows, width = x.shape
    hidden = upb.shape[1]
    columns = weights.shape[1]
    first = previous is None
    vmem = pl.BlockSpec(memory_space=pltpu.VMEM)
    args = (x, g, live, weights, vec, upb) + (() if first else previous)
    scratch = [
        pltpu.VMEM((rows, width), bf16),
        pltpu.VMEM((rows, width), bf16),
        pltpu.VMEM((rows, width), bf16),
        pltpu.VMEM((rows, width), f32),
        pltpu.VMEM((HEADS, rows, 128), bf16),
        pltpu.VMEM((width, rows), bf16),
        pltpu.VMEM((width, rows), bf16),
        pltpu.VMEM((width, rows), bf16),
        pltpu.VMEM((width, rows), bf16),
        pltpu.VMEM((rows, width), bf16),
        pltpu.VMEM((rows, width), f32),
        pltpu.VMEM((rows, width), bf16),
        pltpu.VMEM((rows, hidden), bf16),
        pltpu.VMEM((rows, hidden), bf16),
        pltpu.VMEM((rows, 256), bf16),
        pltpu.VMEM((rows, 256), bf16),
        pltpu.VMEM((rows, 256), bf16),
        pltpu.VMEM((rows, 128), f32),
        pltpu.VMEM((rows, 128), f32),
        pltpu.VMEM((BLK, width), f32),
        pltpu.VMEM((BLK, width), f32),
    ]
    flops = 2 * rows * width * columns * 3 + 7 * 2 * rows * rows * width * 4
    return pl.pallas_call(
        functools.partial(micro_kernel, first),
        out_shape=(
            jax.ShapeDtypeStruct((rows, width), bf16),
            jax.ShapeDtypeStruct((rows, width), bf16),
            jax.ShapeDtypeStruct((width, 4 * width + 2 * hidden), f32 if first else bf16),
            jax.ShapeDtypeStruct((8, width), f32),
            jax.ShapeDtypeStruct((1, hidden), f32),
        ),
        in_specs=[vmem] * len(args),
        out_specs=(vmem,) * 5,
        scratch_shapes=scratch,
        compiler_params=pltpu.CompilerParams(vmem_limit_bytes=63 * 1024 * 1024),
        cost_estimate=pl.CostEstimate(flops=flops, bytes_accessed=30_000_000, transcendentals=3 * HEADS * rows * rows),
        name="micro_first" if first else "micro_second",
    )(*args)


MESH = pl.DeviceIdType.MESH


def split_axes():
    members, others = lax.axis_size("dp"), lax.axis_size("fsdp")
    return members // 2, 2, others // 2, 2


def my_place():
    d, f = lax.axis_index("dp"), lax.axis_index("fsdp")
    return d, f, (d // 2, lax.rem(d, 2), f // 2, lax.rem(f, 2))


def greet(members, others):
    d, f = lax.axis_index("dp"), lax.axis_index("fsdp")
    barrier = pltpu.get_barrier_semaphore()
    for s in range(1, members):
        pl.semaphore_signal(barrier, inc=1, device_id={"dp": lax.rem(d + s, members)}, device_id_type=MESH)
    for s in range(1, others):
        pl.semaphore_signal(barrier, inc=1, device_id={"fsdp": lax.rem(f + s, others)}, device_id_type=MESH)
    pl.semaphore_wait(barrier, members + others - 2)


class Swap:
    def __init__(self, src, dst, local, send, recv, members):
        d = lax.axis_index("dp")
        self.copies = []
        for s in range(1, members):
            to = lax.rem(d + s, members)
            self.copies.append(pltpu.make_async_remote_copy(
                src_ref=src.at[to], dst_ref=dst.at[d], send_sem=send.at[s], recv_sem=recv.at[s],
                device_id={"dp": to}, device_id_type=MESH))
        self.own = pltpu.make_async_copy(src.at[d], dst.at[d], local)

    def start(self):
        for copy in self.copies:
            copy.start()
        self.own.start()

    def wait(self):
        for copy in self.copies:
            copy.wait_recv()
        self.own.wait()

    def wait_sent(self):
        for copy in self.copies:
            copy.wait_send()


class Gather:
    def __init__(self, src, out, cs, order, local, send, recv, sizes):
        a, b, c, e = my_place()[2]
        d, f = lax.axis_index("dp"), lax.axis_index("fsdp")
        high, _, wide, _ = sizes
        every = slice(None)
        place = [a, b, c, e]
        self.own = pltpu.make_async_copy(src.at[:, cs], out.at[a, b, c, e, :, cs], local)
        self.stages = []
        done = [False] * 4
        slot = 0
        for number, axis in enumerate(order):
            copies = []
            size = (high, 2, wide, 2)[axis]
            for s in range(1, size):
                other = lax.rem(place[axis] + s, size)
                if axis == 0:
                    target = {"dp": other * 2 + b}
                elif axis == 1:
                    target = {"dp": a * 2 + other}
                elif axis == 2:
                    target = {"fsdp": other * 2 + e}
                else:
                    target = {"fsdp": c * 2 + other}
                where = tuple(every if done[k] else place[k] for k in range(4)) + (every, cs)
                source = src.at[:, cs] if number == 0 else out.at[where]
                copies.append(pltpu.make_async_remote_copy(
                    src_ref=source, dst_ref=out.at[where], send_sem=send.at[slot], recv_sem=recv.at[slot],
                    device_id=target, device_id_type=MESH))
                slot += 1
            self.stages.append(copies)
            done[axis] = True

    def start(self, number):
        if number == 0:
            self.own.start()
        for copy in self.stages[number]:
            copy.start()

    def wait(self, number):
        for copy in self.stages[number]:
            copy.wait_recv()
        if number == 0:
            self.own.wait()

    def wait_sent(self):
        for stage in self.stages:
            for copy in stage:
                copy.wait_send()


class Reduce:
    def __init__(self, grads, cs, wide_first, emit, scratch, send, recv, high):
        self.grads, self.cs, self.wide_first, self.emit, self.high = grads, cs, wide_first, emit, high
        self.from_core, self.after_core, self.from_one, self.after_one, self.from_two, self.after_two, self.last = scratch
        self.send, self.recv = send, recv
        self.sent = []

    def push(self, source, target, slot, device):
        copy = pltpu.make_async_remote_copy(
            src_ref=source, dst_ref=target, send_sem=self.send.at[slot], recv_sem=self.recv.at[slot],
            device_id=device, device_id_type=MESH)
        copy.start()
        self.sent.append(copy)
        self.copy = copy

    def start(self):
        _, _, (a, b, c, e) = my_place()
        self.push(self.grads.at[:, :, :, 1 - e, :, self.cs], self.from_core, 0, {"fsdp": c * 2 + 1 - e})

    def step(self, number):
        d, f, (a, b, c, e) = my_place()
        across = {"fsdp": (1 - c) * 2 + e}, {"dp": a * 2 + 1 - b}
        if number == 0:
            self.copy.wait_recv()

            def one(i, carry):
                mine = self.grads[i, :, :, e, :, self.cs]
                self.after_core[i] = (mine.astype(f32) + self.from_core[i].astype(f32)).astype(bf16)
                return carry

            lax.fori_loop(0, self.high, one, 0)
            if self.wide_first:
                self.push(self.after_core.at[:, :, 1 - c], self.from_one, 1, across[0])
            else:
                self.push(self.after_core.at[:, 1 - b], self.from_one, 1, across[1])
        elif number == 1:
            self.copy.wait_recv()

            def two(i, carry):
                mine = self.after_core[i, :, c] if self.wide_first else self.after_core[i, b]
                self.after_one[i] = (mine.astype(f32) + self.from_one[i].astype(f32)).astype(bf16)
                return carry

            lax.fori_loop(0, self.high, two, 0)
            if self.wide_first:
                self.push(self.after_one.at[:, 1 - b], self.from_two, 2, across[1])
            else:
                self.push(self.after_one.at[:, 1 - c], self.from_two, 2, across[0])
        elif number == 2:
            self.copy.wait_recv()

            def three(i, carry):
                mine = self.after_one[i, b] if self.wide_first else self.after_one[i, c]
                self.after_two[i] = (mine.astype(f32) + self.from_two[i].astype(f32)).astype(bf16)
                return carry

            lax.fori_loop(0, self.high, three, 0)
            self.copies = []
            for s in range(1, self.high):
                other = lax.rem(a + s, self.high)
                self.push(self.after_two.at[other], self.last.at[a], 2 + s, {"dp": other * 2 + b})
                self.copies.append(self.copy)
        else:
            for copy in self.copies:
                copy.wait_recv()
            total = self.after_two[a].astype(f32)
            for s in range(1, self.high):
                total = total + self.last[lax.rem(a + s, self.high)].astype(f32)
            self.emit(total)

    def wait_sent(self):
        for copy in self.sent:
            copy.wait_send()


def reduce_scratch(high, rows, columns):
    shapes = [(high, 2, 2), (high, 2, 2), (high, 2), (high, 2), (high,), (high,), (high,)]
    return [pltpu.VMEM(lead + (rows, columns), bf16) for lead in shapes]


def gather_kernel(sizes, members, others, ranges, shard, tokens, grads, out, tokens_out, grads_out, wsend, wrecv, tsend, trecv, local):
    greet(members, others)
    micro = tokens.shape[0]
    swaps = []
    for step in range(micro):
        for kind, (src, dst) in enumerate(((tokens, tokens_out), (grads, grads_out))):
            n = step * 2 + kind
            swaps.append(Swap(src.at[step], dst.at[step], local.at[n], tsend.at[n], trecv.at[n], members))
    gathers = [
        Gather(shard, out, cs, order, local.at[2 * micro + n], wsend.at[n], wrecv.at[n], sizes)
        for n, (cs, order) in enumerate(ranges)
    ]
    swaps[0].start()
    for gather in gathers:
        gather.start(0)
    for number in range(1, 4):
        for gather in gathers:
            gather.wait(number - 1)
            gather.start(number)
        if number == 1:
            for swap in swaps[1:]:
                swap.start()
    for gather in gathers:
        gather.wait(3)
    for swap in swaps:
        swap.wait()
    for item in swaps + gathers:
        item.wait_sent()


def scatter_kernel(high, members, others, widths, grads, extra, *refs):
    sources, refs = refs[:4], refs[4:]
    outs, refs = refs[:5], refs[5:]
    returned, refs = refs[:4], refs[4:]
    wsend, wrecv, tsend, trecv, local = refs[-5:]
    scratch = refs[:-5]
    greet(members, others)
    width, hidden = widths
    swaps = [
        Swap(src, dst, local.at[n], tsend.at[n], trecv.at[n], members)
        for n, (src, dst) in enumerate(zip(sources, returned))
    ]

    def emit_first(total):
        outs[0][...] = total[:, : 3 * width]
        outs[1][...] = total[:, 3 * width :]

    def emit_to(ref):
        def emit(total):
            ref[...] = total
        return emit

    up_at, down_at = 4 * width, 4 * width + hidden
    items = [
        Reduce(grads, pl.ds(down_at, hidden), True, emit_to(outs[3]), scratch[0:7], wsend.at[0], wrecv.at[0], high),
        Reduce(grads, pl.ds(up_at, hidden), False, emit_to(outs[2]), scratch[7:14], wsend.at[1], wrecv.at[1], high),
        Reduce(grads, pl.ds(0, up_at), True, emit_first, scratch[14:21], wsend.at[2], wrecv.at[2], high),
        Reduce(extra, pl.ds(0, 128), False, emit_to(outs[4]), scratch[21:28], wsend.at[3], wrecv.at[3], high),
    ]
    for item in items:
        item.start()
    for swap in swaps:
        swap.start()
    for number in range(4):
        for item in items:
            item.step(number)
    for swap in swaps:
        swap.wait()
    for item in items + swaps:
        item.wait_sent()


def order_kernel(scatter, table, *refs):
    count = (len(refs) - 3) // 2
    sources, targets = refs[:count], refs[count : 2 * count]
    held, in_sem, out_sem = refs[2 * count :]
    micro, members = sources[0].shape[:2]
    incoming, outgoing = [], []
    for n in range(count):
        for m in range(micro):
            for p in range(members):
                other = table[m, p]
                src, dst = (p, other) if scatter else (other, p)
                slot = (n * micro + m) * members + p
                copy = pltpu.make_async_copy(sources[n].at[m, src], held.at[slot], in_sem.at[slot])
                copy.start()
                incoming.append(copy)
                outgoing.append(pltpu.make_async_copy(held.at[slot], targets[n].at[m, dst], out_sem.at[slot]))
    for one, two in zip(incoming, outgoing):
        one.wait()
        two.start()
    for two in outgoing:
        two.wait()


ANY = pl.BlockSpec(memory_space=pl.ANY)
VMEM = pl.BlockSpec(memory_space=pltpu.VMEM)


def reorder(scatter, table, *arrays):
    micro, members, piece, width = arrays[0].shape
    slots = len(arrays) * micro * members
    return pl.pallas_call(
        functools.partial(order_kernel, scatter),
        out_shape=tuple(jax.ShapeDtypeStruct(item.shape, item.dtype) for item in arrays),
        in_specs=[pl.BlockSpec(memory_space=pltpu.SMEM)] + [ANY] * len(arrays),
        out_specs=(ANY,) * len(arrays),
        scratch_shapes=[
            pltpu.VMEM((slots, piece, width), arrays[0].dtype),
            pltpu.SemaphoreType.DMA((slots,)),
            pltpu.SemaphoreType.DMA((slots,)),
        ],
        name="order_out" if scatter else "order_in",
    )(table, *arrays)


def gather_call(shard, tokens, grads, members, others):
    rows, columns = shard.shape
    high, wide = members // 2, others // 2
    sizes = (high, 2, wide, 2)
    micro = tokens.shape[0]
    third = 2048
    ranges = (
        (pl.ds(0, third), (0, 1, 2, 3)),
        (pl.ds(third, third), (0, 2, 1, 3)),
        (pl.ds(2 * third, columns - 2 * third), (0, 1, 2, 3)),
    )
    slots = high + 1 + wide
    return pl.pallas_call(
        functools.partial(gather_kernel, sizes, members, others, ranges),
        out_shape=(
            jax.ShapeDtypeStruct(sizes + (rows, columns), shard.dtype),
            jax.ShapeDtypeStruct(tokens.shape, tokens.dtype),
            jax.ShapeDtypeStruct(grads.shape, grads.dtype),
        ),
        in_specs=[VMEM, ANY, ANY],
        out_specs=(ANY,) * 3,
        scratch_shapes=[
            pltpu.SemaphoreType.DMA((len(ranges), slots)),
            pltpu.SemaphoreType.DMA((len(ranges), slots)),
            pltpu.SemaphoreType.DMA((2 * micro, members)),
            pltpu.SemaphoreType.DMA((2 * micro, members)),
            pltpu.SemaphoreType.DMA((2 * micro + len(ranges),)),
        ],
        compiler_params=pltpu.CompilerParams(collective_id=0, has_side_effects=True),
        name="gather_in",
    )(shard, tokens, grads)


def scatter_call(grads, extra, arrays, members, others, width, hidden):
    high = members // 2
    rows = grads.shape[4]
    scratch = []
    for columns in (hidden, hidden, 4 * width, 128):
        scratch += reduce_scratch(high, rows, columns)
    shapes = [(rows, 3 * width), (rows, width), (rows, hidden), (rows, hidden), (rows, 128)]
    return pl.pallas_call(
        functools.partial(scatter_kernel, high, members, others, (width, hidden)),
        out_shape=tuple(jax.ShapeDtypeStruct(shape, f32) for shape in shapes)
        + tuple(jax.ShapeDtypeStruct(item.shape, item.dtype) for item in arrays),
        in_specs=[VMEM, VMEM] + [ANY] * 4,
        out_specs=(VMEM,) * 5 + (ANY,) * 4,
        scratch_shapes=scratch + [
            pltpu.SemaphoreType.DMA((4, high + 2)),
            pltpu.SemaphoreType.DMA((4, high + 2)),
            pltpu.SemaphoreType.DMA((4, members)),
            pltpu.SemaphoreType.DMA((4, members)),
            pltpu.SemaphoreType.DMA((4,)),
        ],
        compiler_params=pltpu.CompilerParams(
            collective_id=1, has_side_effects=True, vmem_limit_bytes=63 * 1024 * 1024),
        name="scatter_out",
    )(grads, extra, *arrays)


def body(
    tokens, out_grad, seq_lengths, send_to, slot_of, first_gain, first_shift, joint_weight, query_bias,
    value_bias, mix_weight, mix_bias, second_gain, second_shift, up_weight, up_bias, down_weight, down_bias,
):
    members, others = lax.axis_size("dp"), lax.axis_size("fsdp")
    devices = members * others
    micro, rows, width = tokens.shape
    piece = rows // members
    own = first_gain.shape[0]
    hidden = down_weight.shape[0]
    per = hidden // width
    vectors = (first_gain, first_shift, query_bias, value_bias, mix_bias, second_gain, second_shift, down_bias)
    small = jnp.concatenate(
        [jnp.stack(vectors, axis=1), up_bias.reshape(own, per), jnp.zeros((own, 128 - 8 - per), bf16)], axis=1)
    shard = jnp.concatenate([joint_weight, mix_weight, up_weight, down_weight.T, small], axis=1)
    table = send_to[:, 0]
    pieces = (micro, members, piece, width)
    sent = reorder(True, table, tokens.reshape(pieces), out_grad.reshape(pieces))
    gathered, routed, routed_grad = gather_call(shard, *sent, members, others)
    whole = gathered.reshape(width, shard.shape[1])
    tail = whole[:, 4 * width + 2 * hidden :].astype(f32)
    vec = tail[:, :8].T
    upb = tail[:, 8 : 8 + per].reshape(1, hidden)
    spots = slot_of[:, 0, :, None] * piece + jnp.arange(piece, dtype=jnp.int32)
    live = (spots.reshape(micro, rows) < seq_lengths).astype(f32)[:, :, None]
    previous = None
    results = []
    for step in range(micro):
        final, token_grad, *previous = micro_call(
            routed[step].reshape(rows, width), routed_grad[step].reshape(rows, width), live[step], whole, vec, upb,
            previous and tuple(previous))
        results += [final.reshape(members, piece, width), token_grad.reshape(members, piece, width)]
    total, vsum, usum = previous
    sizes = (members // 2, 2, others // 2, 2, own)
    grads = total.reshape(sizes + (total.shape[1],))
    extra = jnp.concatenate(
        [vsum.T, usum.reshape(width, per), jnp.zeros((width, 128 - 8 - per), f32)], axis=1
    ).astype(bf16).reshape(sizes + (128,))
    joint, mix, up, down, tail, *returned = scatter_call(grads, extra, results, members, others, width, hidden)
    layer_output, input_grad = reorder(
        False, table, jnp.stack([returned[0], returned[2]]), jnp.stack([returned[1], returned[3]]))
    vec_grad = [tail[:, n] for n in range(8)]
    return (
        layer_output.reshape(tokens.shape), input_grad.reshape(tokens.shape),
        vec_grad[0], vec_grad[1], joint, vec_grad[2], vec_grad[3], mix, vec_grad[4], vec_grad[5], vec_grad[6],
        up, tail[:, 8 : 8 + per].reshape(up_bias.shape), down.T, vec_grad[7],
    )


def solution(mesh):
    both = ("dp", "fsdp")
    row3, row2, vector, matrix = P(None, both, None), P(None, both), P(both), P(both, None)
    turned = P(None, both)
    return jax.shard_map(
        body,
        mesh=mesh,
        in_specs=(row3, row3, row2, row3, row3, vector, vector, matrix, vector, vector, matrix, vector, vector,
                  vector, matrix, vector, turned, vector),
        out_specs=(row3, row3, vector, vector, matrix, vector, vector, matrix, vector, vector, vector, matrix,
                   vector, turned, vector),
        check_vma=False,
    )
```

```python
import functools
import math

import jax
import jax.numpy as jnp
from jax import lax
from jax.experimental import pallas as pl
from jax.experimental.pallas import tpu as pltpu
from jax.sharding import PartitionSpec as P

HEADS = 8
HEAD_DIM = 64
BLK = 256

f32, bf16 = jnp.float32, jnp.bfloat16
epsilon = 1e-05
masked_score = -1e30
root_half = math.sqrt(0.5)
gauss_norm = 1.0 / math.sqrt(2.0 * math.pi)


def nn(a, b):
    return lax.dot_general(a, b, (((1,), (0,)), ((), ())), preferred_element_type=f32)


def nt(a, b):
    return lax.dot_general(a, b, (((1,), (1,)), ((), ())), preferred_element_type=f32)


def tn(a, b):
    return lax.dot_general(a, b, (((0,), (0,)), ((), ())), preferred_element_type=f32)


def normalize(rows):
    center = rows - jnp.mean(rows, axis=-1, keepdims=True)
    spread = jnp.mean(center * center, axis=-1, keepdims=True)
    factor = lax.rsqrt(spread + epsilon)
    return center * factor, factor


def norm_back(grad_norm, normed, factor):
    first_mean = jnp.mean(grad_norm, axis=-1, keepdims=True)
    second_mean = jnp.mean(grad_norm * normed, axis=-1, keepdims=True)
    return factor * (grad_norm - first_mean - normed * second_mean)


def three_parts(v):
    hi = v.astype(bf16).astype(f32)
    mid = (v - hi).astype(bf16).astype(f32)
    return hi, mid, v - hi - mid


def col_sum(v):
    return jnp.sum(v, axis=0, keepdims=True)


def micro_kernel(first, *refs):
    x_ref, g_ref, live_ref, w_ref, vec_ref, upb_ref = refs[:6]
    refs = refs[6:]
    if not first:
        prev_ref, vprev_ref, uprev_ref = refs[:3]
        refs = refs[3:]
    final_ref, tg_ref, grad_ref, vsum_ref, usum_ref = refs[:5]
    (q_ref, k_ref, v_ref, att_ref, qaug_ref, first_t, second_t, down_t, att_t, mixin_ref, mg_ref,
     dout_ref, hid_ref, pre_ref, kaug, vaug_a, vaug_b, dk_acc, dv_acc, acc_a, acc_b) = refs[5:]
    rows, width = x_ref.shape
    hidden = upb_ref.shape[1]
    blocks = rows // BLK
    pairs = width // 128
    mix_at = 3 * width
    up_at = mix_at + width
    down_at = up_at + hidden
    lane = lax.broadcasted_iota(jnp.int32, (1, 128), 1)
    low_half = lane < HEAD_DIM

    def at(i, size=BLK):
        return pl.ds(pl.multiple_of(i * size, size), size)

    if first:
        vsum_ref[...] = jnp.zeros_like(vsum_ref)
        usum_ref[...] = jnp.zeros_like(usum_ref)
    else:
        vsum_ref[...] = vprev_ref[...]
        usum_ref[...] = uprev_ref[...]

    def row(ref, n):
        return ref[n : n + 1, :]

    live_all = live_ref[...]
    mask_aug = jnp.where(
        lane == 0, (live_all - 1.0) * (-masked_score), jnp.where(lane < 4, 1.0, 0.0)
    ).astype(bf16)
    kaug[:, 128:] = mask_aug
    vaug_a[:, 128:] = jnp.ones((rows, 128), bf16)
    vaug_b[:, 128:] = jnp.ones((rows, 128), bf16)

    def project(i, carry):
        rs = at(i)
        normed, _ = normalize(x_ref[rs, :].astype(f32))
        first_in = (normed * row(vec_ref, 0) + row(vec_ref, 1)).astype(bf16)
        first_t[:, rs] = first_in.T
        query = (nn(first_in, w_ref[:, :width]) + row(vec_ref, 2)).astype(bf16)
        q_ref[rs, :] = query * jnp.array(HEAD_DIM ** (-0.5), bf16)
        k_ref[rs, :] = nn(first_in, w_ref[:, width : 2 * width]).astype(bf16)
        v_ref[rs, :] = (nn(first_in, w_ref[:, 2 * width : 3 * width]) + row(vec_ref, 3)).astype(bf16)
        return carry

    lax.fori_loop(0, blocks, project, 0)

    def attend_pair(p, carry):
        ls = at(p, 128)
        kaug[:, :128] = k_ref[:, ls]
        values = v_ref[:, ls]
        zero = jnp.zeros_like(values)
        vaug_a[:, :128] = jnp.where(low_half, values, zero)
        vaug_b[:, :128] = jnp.where(low_half, zero, values)

        def attend(i, carry):
            rs = at(i)
            query = q_ref[rs, ls]
            qzero = jnp.zeros_like(query)
            one = jnp.broadcast_to(jnp.where(lane == 0, 1.0, 0.0), (BLK, 128)).astype(bf16)
            out = None
            for half, vaug in ((0, vaug_a), (1, vaug_b)):
                mine = jnp.where(low_half if half == 0 else jnp.logical_not(low_half), query, qzero)
                scores = nt(jnp.concatenate([mine, one], axis=1), kaug[...])
                peak = jnp.max(scores, axis=-1, keepdims=True)
                chances = jnp.exp(scores - peak).astype(bf16)
                got = nn(chances, vaug[...])
                total = got[:, 128:]
                lse = peak + jnp.log(total)
                hi, mid, lo = three_parts(lse)
                qaug_ref[2 * p + half, rs, :] = jnp.where(
                    lane == 0, 1.0,
                    jnp.where(lane == 1, -hi, jnp.where(lane == 2, -mid, jnp.where(lane == 3, -lo, 0.0))),
                ).astype(bf16)
                part = got[:, :128] / total
                out = part if out is None else out + part
            att_ref[rs, ls] = out
            return carry

        return lax.fori_loop(0, blocks, attend, carry)

    lax.fori_loop(0, pairs, attend_pair, 0)

    chunk = 512
    mix_w = w_ref.at[:, mix_at:up_at]

    def feed(i, carry):
        rs = at(i)
        live = live_ref[rs, :]
        attended = att_ref[rs, :].astype(bf16)
        att_t[:, rs] = attended.T
        middle = x_ref[rs, :].astype(f32) + live * (nn(attended, mix_w[...]) + row(vec_ref, 4))
        second_norm, factor = normalize(middle)
        second_in = (second_norm * row(vec_ref, 5) + row(vec_ref, 6)).astype(bf16)
        second_t[:, rs] = second_in.T
        outer = g_ref[rs, :].astype(f32)
        down_in = (live * outer).astype(bf16)
        down_t[:, rs] = down_in.T
        vsum_ref[7:8, :] += col_sum(down_in.astype(f32))
        acc_a[...] = jnp.zeros_like(acc_a)
        acc_b[...] = jnp.zeros_like(acc_b)

        def part(c, carry):
            cs = at(c, chunk)
            up = w_ref[:, pl.ds(pl.multiple_of(up_at + c * chunk, chunk), chunk)]
            down = w_ref[:, pl.ds(pl.multiple_of(down_at + c * chunk, chunk), chunk)]
            pre = nn(second_in, up) + upb_ref[:, cs]
            phi = 0.5 * (1.0 + lax.erf(pre * root_half))
            hid = (pre * phi).astype(bf16)
            slope = phi + pre * jnp.exp(-0.5 * pre * pre) * gauss_norm
            hid_ref[rs, cs] = hid
            acc_a[...] += nt(hid, down)
            pre_grad = (nn(down_in, down) * slope).astype(bf16)
            pre_ref[rs, cs] = pre_grad
            usum_ref[:, cs] += col_sum(pre_grad.astype(f32))
            acc_b[...] += nt(pre_grad, up)
            return carry

        lax.fori_loop(0, hidden // chunk, part, 0)
        final_ref[rs, :] = (middle + live * (acc_a[...] + row(vec_ref, 7))).astype(bf16)
        second_in_grad = acc_b[...]
        vsum_ref[5:6, :] += col_sum(second_in_grad * second_norm)
        vsum_ref[6:7, :] += col_sum(second_in_grad)
        middle_grad = outer + norm_back(second_in_grad * row(vec_ref, 5), second_norm, factor)
        mg_ref[rs, :] = middle_grad
        mix_in = (live * middle_grad).astype(bf16)
        mixin_ref[rs, :] = mix_in
        vsum_ref[4:5, :] += col_sum(mix_in.astype(f32))
        dout_ref[rs, :] = nt(mix_in, mix_w[...]).astype(bf16)
        return carry

    lax.fori_loop(0, blocks, feed, 0)

    def put(value, cs):
        if not first:
            value = value + prev_ref[:, cs]
        grad_ref[:, cs] = value.astype(grad_ref.dtype)

    def wide(lhs_t, rhs_ref, base, count):
        def one(c, carry):
            put(nn(lhs_t[...], rhs_ref[:, at(c, chunk)]),
                pl.ds(pl.multiple_of(base + c * chunk, chunk), chunk))
            return carry
        lax.fori_loop(0, count, one, 0)

    wide(down_t, hid_ref, down_at, hidden // chunk)
    wide(second_t, pre_ref, up_at, hidden // chunk)
    wide(att_t, mixin_ref, mix_at, width // chunk)

    joint_grad = hid_ref

    def back_pair(p, carry):
        ls = at(p, 128)
        keys = k_ref[:, ls]
        kaug[:, :128] = keys
        vaug_a[:, :128] = v_ref[:, ls]
        vaug_a[:, 128:] = kaug[:, 128:]
        zero = jnp.zeros_like(keys)
        vaug_b[:, :128] = jnp.where(low_half, keys, zero)
        vaug_b[:, 128:] = jnp.where(low_half, zero, keys)
        dk_acc[...] = jnp.zeros_like(dk_acc)
        dv_acc[...] = jnp.zeros_like(dv_acc)

        def back(i, carry):
            rs = at(i)
            query = q_ref[rs, ls]
            grad = dout_ref[rs, ls]
            both = grad.astype(f32) * att_ref[rs, ls]
            dq = None
            for half in (0, 1):
                keep = low_half if half == 0 else jnp.logical_not(low_half)
                mine = jnp.where(keep, query, jnp.zeros_like(query))
                grads = jnp.where(keep, grad, jnp.zeros_like(grad))
                inner = jnp.sum(jnp.where(keep, both, 0.0), axis=-1, keepdims=True)
                hi, mid, lo = three_parts(inner)
                gaug = jnp.where(
                    lane == 1, -hi, jnp.where(lane == 2, -mid, jnp.where(lane == 3, -lo, 0.0))
                ).astype(bf16)
                scores = nt(kaug[...], jnp.concatenate([mine, qaug_ref[2 * p + half, rs, :]], axis=1))
                chances = jnp.exp(scores)
                centered = nt(vaug_a[...], jnp.concatenate([grads, gaug], axis=1))
                score_grad = (chances * centered).astype(bf16)
                dv_acc[...] += nn(chances.astype(bf16), grads)
                dk_acc[...] += nn(score_grad, mine)
                part = tn(score_grad, vaug_b[:, 128 * half : 128 * half + 128])
                dq = part if dq is None else dq + part
            joint_grad[rs, ls] = (dq * HEAD_DIM ** (-0.5)).astype(bf16)
            return carry

        lax.fori_loop(0, blocks, back, 0)
        joint_grad[:, pl.ds(pl.multiple_of(width + p * 128, 128), 128)] = dk_acc[...].astype(bf16)
        joint_grad[:, pl.ds(pl.multiple_of(2 * width + p * 128, 128), 128)] = dv_acc[...].astype(bf16)
        return carry

    lax.fori_loop(0, pairs, back_pair, 0)

    wide(first_t, joint_grad, 0, 3 * width // chunk)

    def back_first(i, carry):
        rs = at(i)
        grads = joint_grad[rs, : 3 * width]
        vsum_ref[2:3, :] += col_sum(grads[:, :width].astype(f32))
        vsum_ref[3:4, :] += col_sum(grads[:, 2 * width :].astype(f32))
        first_in_grad = nt(grads, w_ref[:, : 3 * width])
        normed, factor = normalize(x_ref[rs, :].astype(f32))
        vsum_ref[0:1, :] += col_sum(first_in_grad * normed)
        vsum_ref[1:2, :] += col_sum(first_in_grad)
        tg_ref[rs, :] = (
            mg_ref[rs, :] + norm_back(first_in_grad * row(vec_ref, 0), normed, factor)
        ).astype(bf16)
        return carry

    lax.fori_loop(0, blocks, back_first, 0)


def micro_call(x, g, live, weights, vec, upb, previous=None):
    rows, width = x.shape
    hidden = upb.shape[1]
    columns = weights.shape[1]
    first = previous is None
    vmem = pl.BlockSpec(memory_space=pltpu.VMEM)
    args = (x, g, live, weights, vec, upb) + (() if first else previous)
    scratch = [
        pltpu.VMEM((rows, width), bf16),
        pltpu.VMEM((rows, width), bf16),
        pltpu.VMEM((rows, width), bf16),
        pltpu.VMEM((rows, width), f32),
        pltpu.VMEM((HEADS, rows, 128), bf16),
        pltpu.VMEM((width, rows), bf16),
        pltpu.VMEM((width, rows), bf16),
        pltpu.VMEM((width, rows), bf16),
        pltpu.VMEM((width, rows), bf16),
        pltpu.VMEM((rows, width), bf16),
        pltpu.VMEM((rows, width), f32),
        pltpu.VMEM((rows, width), bf16),
        pltpu.VMEM((rows, hidden), bf16),
        pltpu.VMEM((rows, hidden), bf16),
        pltpu.VMEM((rows, 256), bf16),
        pltpu.VMEM((rows, 256), bf16),
        pltpu.VMEM((rows, 256), bf16),
        pltpu.VMEM((rows, 128), f32),
        pltpu.VMEM((rows, 128), f32),
        pltpu.VMEM((BLK, width), f32),
        pltpu.VMEM((BLK, width), f32),
    ]
    flops = 2 * rows * width * columns * 3 + 7 * 2 * rows * rows * width * 4
    return pl.pallas_call(
        functools.partial(micro_kernel, first),
        out_shape=(
            jax.ShapeDtypeStruct((rows, width), bf16),
            jax.ShapeDtypeStruct((rows, width), bf16),
            jax.ShapeDtypeStruct((width, 4 * width + 2 * hidden), f32 if first else bf16),
            jax.ShapeDtypeStruct((8, width), f32),
            jax.ShapeDtypeStruct((1, hidden), f32),
        ),
        in_specs=[vmem] * len(args),
        out_specs=(vmem,) * 5,
        scratch_shapes=scratch,
        compiler_params=pltpu.CompilerParams(vmem_limit_bytes=67_043_328),
        cost_estimate=pl.CostEstimate(flops=flops, bytes_accessed=30_000_000, transcendentals=3 * HEADS * rows * rows),
        name="micro_first" if first else "micro_second",
    )(*args)


MESH = pl.DeviceIdType.MESH


def split_axes():
    members, others = lax.axis_size("dp"), lax.axis_size("fsdp")
    return members // 2, 2, others // 2, 2


def my_place():
    d, f = lax.axis_index("dp"), lax.axis_index("fsdp")
    return d, f, (d // 2, lax.rem(d, 2), f // 2, lax.rem(f, 2))


def greet(members, others):
    d, f = lax.axis_index("dp"), lax.axis_index("fsdp")
    barrier = pltpu.get_barrier_semaphore()
    for s in range(1, members):
        pl.semaphore_signal(barrier, inc=1, device_id={"dp": lax.rem(d + s, members)}, device_id_type=MESH)
    for s in range(1, others):
        pl.semaphore_signal(barrier, inc=1, device_id={"fsdp": lax.rem(f + s, others)}, device_id_type=MESH)
    pl.semaphore_wait(barrier, members + others - 2)


class Swap:
    def __init__(self, src, dst, local, send, recv, members):
        d = lax.axis_index("dp")
        self.copies = []
        for s in range(1, members):
            to = lax.rem(d + s, members)
            self.copies.append(pltpu.make_async_remote_copy(
                src_ref=src.at[to], dst_ref=dst.at[d], send_sem=send.at[s], recv_sem=recv.at[s],
                device_id={"dp": to}, device_id_type=MESH))
        self.own = pltpu.make_async_copy(src.at[d], dst.at[d], local)

    def start(self):
        for copy in self.copies:
            copy.start()
        self.own.start()

    def wait(self):
        for copy in self.copies:
            copy.wait_recv()
        self.own.wait()

    def wait_sent(self):
        for copy in self.copies:
            copy.wait_send()


class Gather:
    def __init__(self, src, out, cs, order, local, send, recv, sizes):
        a, b, c, e = my_place()[2]
        d, f = lax.axis_index("dp"), lax.axis_index("fsdp")
        high, _, wide, _ = sizes
        every = slice(None)
        place = [a, b, c, e]
        self.own = pltpu.make_async_copy(src.at[:, cs], out.at[a, b, c, e, :, cs], local)
        self.stages = []
        done = [False] * 4
        slot = 0
        for number, axis in enumerate(order):
            copies = []
            size = (high, 2, wide, 2)[axis]
            for s in range(1, size):
                other = lax.rem(place[axis] + s, size)
                if axis == 0:
                    target = {"dp": other * 2 + b}
                elif axis == 1:
                    target = {"dp": a * 2 + other}
                elif axis == 2:
                    target = {"fsdp": other * 2 + e}
                else:
                    target = {"fsdp": c * 2 + other}
                where = tuple(every if done[k] else place[k] for k in range(4)) + (every, cs)
                source = src.at[:, cs] if number == 0 else out.at[where]
                copies.append(pltpu.make_async_remote_copy(
                    src_ref=source, dst_ref=out.at[where], send_sem=send.at[slot], recv_sem=recv.at[slot],
                    device_id=target, device_id_type=MESH))
                slot += 1
            self.stages.append(copies)
            done[axis] = True

    def start(self, number):
        if number == 0:
            self.own.start()
        for copy in self.stages[number]:
            copy.start()

    def wait(self, number):
        for copy in self.stages[number]:
            copy.wait_recv()
        if number == 0:
            self.own.wait()

    def wait_sent(self):
        for stage in self.stages:
            for copy in stage:
                copy.wait_send()


class Reduce:
    def __init__(self, grads, cs, wide_first, emit, scratch, send, recv, high):
        self.grads, self.cs, self.wide_first, self.emit, self.high = grads, cs, wide_first, emit, high
        self.from_core, self.after_core, self.from_one, self.after_one, self.from_two, self.after_two, self.last = scratch
        self.send, self.recv = send, recv
        self.sent = []

    def push(self, source, target, slot, device):
        copy = pltpu.make_async_remote_copy(
            src_ref=source, dst_ref=target, send_sem=self.send.at[slot], recv_sem=self.recv.at[slot],
            device_id=device, device_id_type=MESH)
        copy.start()
        self.sent.append(copy)
        self.copy = copy

    def start(self):
        _, _, (a, b, c, e) = my_place()
        self.push(self.grads.at[:, :, :, 1 - e, :, self.cs], self.from_core, 0, {"fsdp": c * 2 + 1 - e})

    def step(self, number):
        d, f, (a, b, c, e) = my_place()
        across = {"fsdp": (1 - c) * 2 + e}, {"dp": a * 2 + 1 - b}
        if number == 0:
            self.copy.wait_recv()

            def one(i, carry):
                mine = self.grads[i, :, :, e, :, self.cs]
                self.after_core[i] = (mine.astype(f32) + self.from_core[i].astype(f32)).astype(bf16)
                return carry

            lax.fori_loop(0, self.high, one, 0)
            if self.wide_first:
                self.push(self.after_core.at[:, :, 1 - c], self.from_one, 1, across[0])
            else:
                self.push(self.after_core.at[:, 1 - b], self.from_one, 1, across[1])
        elif number == 1:
            self.copy.wait_recv()

            def two(i, carry):
                mine = self.after_core[i, :, c] if self.wide_first else self.after_core[i, b]
                self.after_one[i] = (mine.astype(f32) + self.from_one[i].astype(f32)).astype(bf16)
                return carry

            lax.fori_loop(0, self.high, two, 0)
            if self.wide_first:
                self.push(self.after_one.at[:, 1 - b], self.from_two, 2, across[1])
            else:
                self.push(self.after_one.at[:, 1 - c], self.from_two, 2, across[0])
        elif number == 2:
            self.copy.wait_recv()

            def three(i, carry):
                mine = self.after_one[i, b] if self.wide_first else self.after_one[i, c]
                self.after_two[i] = (mine.astype(f32) + self.from_two[i].astype(f32)).astype(bf16)
                return carry

            lax.fori_loop(0, self.high, three, 0)
            self.copies = []
            for s in range(1, self.high):
                other = lax.rem(a + s, self.high)
                self.push(self.after_two.at[other], self.last.at[a], 2 + s, {"dp": other * 2 + b})
                self.copies.append(self.copy)
        else:
            for copy in self.copies:
                copy.wait_recv()
            total = self.after_two[a].astype(f32)
            for s in range(1, self.high):
                total = total + self.last[lax.rem(a + s, self.high)].astype(f32)
            self.emit(total)

    def wait_sent(self):
        for copy in self.sent:
            copy.wait_send()


def reduce_scratch(high, rows, columns):
    shapes = [(high, 2, 2), (high, 2, 2), (high, 2), (high, 2), (high,), (high,), (high,)]
    return [pltpu.VMEM(lead + (rows, columns), bf16) for lead in shapes]


def gather_kernel(sizes, members, others, ranges, shard, tokens, grads, out, tokens_out, grads_out, wsend, wrecv, tsend, trecv, local):
    greet(members, others)
    micro = tokens.shape[0]
    swaps = []
    for step in range(micro):
        for kind, (src, dst) in enumerate(((tokens, tokens_out), (grads, grads_out))):
            n = step * 2 + kind
            swaps.append(Swap(src.at[step], dst.at[step], local.at[n], tsend.at[n], trecv.at[n], members))
    gathers = [
        Gather(shard, out, cs, order, local.at[2 * micro + n], wsend.at[n], wrecv.at[n], sizes)
        for n, (cs, order) in enumerate(ranges)
    ]
    swaps[0].start()
    for gather in gathers:
        gather.start(0)
    for number in range(1, 4):
        for gather in gathers:
            gather.wait(number - 1)
            gather.start(number)
        if number == 1:
            for swap in swaps[1:]:
                swap.start()
    for gather in gathers:
        gather.wait(3)
    for swap in swaps:
        swap.wait()
    for item in swaps + gathers:
        item.wait_sent()


def scatter_kernel(high, members, others, widths, grads, extra, *refs):
    sources, refs = refs[:4], refs[4:]
    outs, refs = refs[:5], refs[5:]
    returned, refs = refs[:4], refs[4:]
    wsend, wrecv, tsend, trecv, local = refs[-5:]
    scratch = refs[:-5]
    greet(members, others)
    width, hidden = widths
    swaps = [
        Swap(src, dst, local.at[n], tsend.at[n], trecv.at[n], members)
        for n, (src, dst) in enumerate(zip(sources, returned))
    ]

    def emit_first(total):
        outs[0][...] = total[:, : 3 * width]
        outs[1][...] = total[:, 3 * width :]

    def emit_to(ref):
        def emit(total):
            ref[...] = total
        return emit

    up_at, down_at = 4 * width, 4 * width + hidden
    items = [
        Reduce(grads, pl.ds(down_at, hidden), True, emit_to(outs[3]), scratch[0:7], wsend.at[0], wrecv.at[0], high),
        Reduce(grads, pl.ds(up_at, hidden), False, emit_to(outs[2]), scratch[7:14], wsend.at[1], wrecv.at[1], high),
        Reduce(grads, pl.ds(0, up_at), True, emit_first, scratch[14:21], wsend.at[2], wrecv.at[2], high),
        Reduce(extra, pl.ds(0, 128), False, emit_to(outs[4]), scratch[21:28], wsend.at[3], wrecv.at[3], high),
    ]
    for item in items:
        item.start()
    for swap in swaps:
        swap.start()
    for number in range(4):
        for item in items:
            item.step(number)
    for swap in swaps:
        swap.wait()
    for item in items + swaps:
        item.wait_sent()


def order_kernel(scatter, table, *refs):
    count = (len(refs) - 3) // 2
    sources, targets = refs[:count], refs[count : 2 * count]
    held, in_sem, out_sem = refs[2 * count :]
    micro, members = sources[0].shape[:2]
    incoming, outgoing = [], []
    for n in range(count):
        for m in range(micro):
            for p in range(members):
                other = table[m, p]
                src, dst = (p, other) if scatter else (other, p)
                slot = (n * micro + m) * members + p
                copy = pltpu.make_async_copy(sources[n].at[m, src], held.at[slot], in_sem.at[slot])
                copy.start()
                incoming.append(copy)
                outgoing.append(pltpu.make_async_copy(held.at[slot], targets[n].at[m, dst], out_sem.at[slot]))
    for one, two in zip(incoming, outgoing):
        one.wait()
        two.start()
    for two in outgoing:
        two.wait()


ANY = pl.BlockSpec(memory_space=pl.ANY)
VMEM = pl.BlockSpec(memory_space=pltpu.VMEM)


def reorder(scatter, table, *arrays):
    micro, members, piece, width = arrays[0].shape
    slots = len(arrays) * micro * members
    return pl.pallas_call(
        functools.partial(order_kernel, scatter),
        out_shape=tuple(jax.ShapeDtypeStruct(item.shape, item.dtype) for item in arrays),
        in_specs=[pl.BlockSpec(memory_space=pltpu.SMEM)] + [ANY] * len(arrays),
        out_specs=(ANY,) * len(arrays),
        scratch_shapes=[
            pltpu.VMEM((slots, piece, width), arrays[0].dtype),
            pltpu.SemaphoreType.DMA((slots,)),
            pltpu.SemaphoreType.DMA((slots,)),
        ],
        name="order_out" if scatter else "order_in",
    )(table, *arrays)


def gather_call(shard, tokens, grads, members, others):
    rows, columns = shard.shape
    high, wide = members // 2, others // 2
    sizes = (high, 2, wide, 2)
    micro = tokens.shape[0]
    third = 2048
    ranges = (
        (pl.ds(0, third), (0, 1, 2, 3)),
        (pl.ds(third, third), (0, 2, 1, 3)),
        (pl.ds(2 * third, columns - 2 * third), (0, 1, 2, 3)),
    )
    slots = high + 1 + wide
    return pl.pallas_call(
        functools.partial(gather_kernel, sizes, members, others, ranges),
        out_shape=(
            jax.ShapeDtypeStruct(sizes + (rows, columns), shard.dtype),
            jax.ShapeDtypeStruct(tokens.shape, tokens.dtype),
            jax.ShapeDtypeStruct(grads.shape, grads.dtype),
        ),
        in_specs=[VMEM, ANY, ANY],
        out_specs=(ANY,) * 3,
        scratch_shapes=[
            pltpu.SemaphoreType.DMA((len(ranges), slots)),
            pltpu.SemaphoreType.DMA((len(ranges), slots)),
            pltpu.SemaphoreType.DMA((2 * micro, members)),
            pltpu.SemaphoreType.DMA((2 * micro, members)),
            pltpu.SemaphoreType.DMA((2 * micro + len(ranges),)),
        ],
        compiler_params=pltpu.CompilerParams(collective_id=0, has_side_effects=True),
        name="gather_in",
    )(shard, tokens, grads)


def scatter_call(grads, extra, arrays, members, others, width, hidden):
    high = members // 2
    rows = grads.shape[4]
    scratch = []
    for columns in (hidden, hidden, 4 * width, 128):
        scratch += reduce_scratch(high, rows, columns)
    shapes = [(rows, 3 * width), (rows, width), (rows, hidden), (rows, hidden), (rows, 128)]
    return pl.pallas_call(
        functools.partial(scatter_kernel, high, members, others, (width, hidden)),
        out_shape=tuple(jax.ShapeDtypeStruct(shape, f32) for shape in shapes)
        + tuple(jax.ShapeDtypeStruct(item.shape, item.dtype) for item in arrays),
        in_specs=[VMEM, VMEM] + [ANY] * 4,
        out_specs=(VMEM,) * 5 + (ANY,) * 4,
        scratch_shapes=scratch + [
            pltpu.SemaphoreType.DMA((4, high + 2)),
            pltpu.SemaphoreType.DMA((4, high + 2)),
            pltpu.SemaphoreType.DMA((4, members)),
            pltpu.SemaphoreType.DMA((4, members)),
            pltpu.SemaphoreType.DMA((4,)),
        ],
        compiler_params=pltpu.CompilerParams(
            collective_id=1, has_side_effects=True, vmem_limit_bytes=67_043_328),
        name="scatter_out",
    )(grads, extra, *arrays)


def body(
    tokens, out_grad, seq_lengths, send_to, slot_of, first_gain, first_shift, joint_weight, query_bias,
    value_bias, mix_weight, mix_bias, second_gain, second_shift, up_weight, up_bias, down_weight, down_bias,
):
    members, others = lax.axis_size("dp"), lax.axis_size("fsdp")
    devices = members * others
    micro, rows, width = tokens.shape
    piece = rows // members
    own = first_gain.shape[0]
    hidden = down_weight.shape[0]
    per = hidden // width
    vectors = (first_gain, first_shift, query_bias, value_bias, mix_bias, second_gain, second_shift, down_bias)
    small = jnp.concatenate(
        [jnp.stack(vectors, axis=1), up_bias.reshape(own, per), jnp.zeros((own, 128 - 8 - per), bf16)], axis=1)
    shard = jnp.concatenate([joint_weight, mix_weight, up_weight, down_weight.T, small], axis=1)
    table = send_to[:, 0]
    pieces = (micro, members, piece, width)
    sent = reorder(True, table, tokens.reshape(pieces), out_grad.reshape(pieces))
    gathered, routed, routed_grad = gather_call(shard, *sent, members, others)
    whole = gathered.reshape(width, shard.shape[1])
    tail = whole[:, 4 * width + 2 * hidden :].astype(f32)
    vec = tail[:, :8].T
    upb = tail[:, 8 : 8 + per].reshape(1, hidden)
    spots = slot_of[:, 0, :, None] * piece + jnp.arange(piece, dtype=jnp.int32)
    live = (spots.reshape(micro, rows) < seq_lengths).astype(f32)[:, :, None]
    previous = None
    results = []
    for step in range(micro):
        final, token_grad, *previous = micro_call(
            routed[step].reshape(rows, width), routed_grad[step].reshape(rows, width), live[step], whole, vec, upb,
            previous and tuple(previous))
        results += [final.reshape(members, piece, width), token_grad.reshape(members, piece, width)]
    total, vsum, usum = previous
    sizes = (members // 2, 2, others // 2, 2, own)
    grads = total.reshape(sizes + (total.shape[1],))
    extra = jnp.concatenate(
        [vsum.T, usum.reshape(width, per), jnp.zeros((width, 128 - 8 - per), f32)], axis=1
    ).astype(bf16).reshape(sizes + (128,))
    joint, mix, up, down, tail, *returned = scatter_call(grads, extra, results, members, others, width, hidden)
    layer_output, input_grad = reorder(
        False, table, jnp.stack([returned[0], returned[2]]), jnp.stack([returned[1], returned[3]]))
    vec_grad = [tail[:, n] for n in range(8)]
    return (
        layer_output.reshape(tokens.shape), input_grad.reshape(tokens.shape),
        vec_grad[0], vec_grad[1], joint, vec_grad[2], vec_grad[3], mix, vec_grad[4], vec_grad[5], vec_grad[6],
        up, tail[:, 8 : 8 + per].reshape(up_bias.shape), down.T, vec_grad[7],
    )


SMALL = 256


class Layer:
    def __init__(self, x, g, live, weight, offsets, vec, upb, final, tg, put, vsum, usum, scratch):
        self.x, self.g, self.live, self.weight, self.offsets = x, g, live, weight, offsets
        self.vec, self.upb, self.final, self.tg, self.put, self.vsum, self.usum = vec, upb, final, tg, put, vsum, usum
        (self.q, self.k, self.v, self.att, self.qaug, self.first_t, self.second_t, self.down_t, self.att_t, self.mixin,
         self.mg, self.dout, self.hid, self.pre, self.kaug, self.vaug_a, self.vaug_b, self.dk, self.dv, self.acc_a,
         self.acc_b) = scratch
        self.rows, self.width = self.q.shape
        self.hidden = upb.shape[1]
        self.blocks = self.rows // BLK
        self.pairs = self.width // 128
        self.lane = lax.broadcasted_iota(jnp.int32, (1, 128), 1)
        self.low = self.lane < HEAD_DIM

    def at(self, i, size=BLK):
        return pl.ds(pl.multiple_of(i * size, size), size)

    def row(self, n):
        return self.vec[n : n + 1, :]

    def load(self, ref, i):
        per = BLK // ref.shape[1]
        return ref[pl.ds(i * per, per)].reshape(BLK, self.width)

    def save(self, ref, i, value):
        per = BLK // ref.shape[1]
        ref[pl.ds(i * per, per)] = value.reshape(per, ref.shape[1], self.width)

    def masks(self):
        rows, lane = self.rows, self.lane
        self.kaug[:, 128:] = jnp.where(
            lane == 0, (self.live[...] - 1.0) * (-masked_score), jnp.where(lane < 4, 1.0, 0.0)
        ).astype(bf16)
        self.vaug_a[:, 128:] = jnp.ones((rows, 128), bf16)
        self.vaug_b[:, 128:] = jnp.ones((rows, 128), bf16)

    def project(self):
        width = self.width

        def one(i, carry):
            rs = self.at(i)
            normed, _ = normalize(self.load(self.x, i).astype(f32))
            first_in = (normed * self.row(0) + self.row(1)).astype(bf16)
            self.first_t[:, rs] = first_in.T
            query = (nn(first_in, self.weight(0, width)) + self.row(2)).astype(bf16)
            self.q[rs, :] = query * jnp.array(HEAD_DIM ** (-0.5), bf16)
            self.k[rs, :] = nn(first_in, self.weight(width, width)).astype(bf16)
            self.v[rs, :] = (nn(first_in, self.weight(2 * width, width)) + self.row(3)).astype(bf16)
            return carry

        lax.fori_loop(0, self.blocks, one, 0)

    def attend(self, hook):
        lane, low = self.lane, self.low

        def pair(p, carry):
            ls = self.at(p, 128)
            self.kaug[:, :128] = self.k[:, ls]
            values = self.v[:, ls]
            zero = jnp.zeros_like(values)
            self.vaug_a[:, :128] = jnp.where(low, values, zero)
            self.vaug_b[:, :128] = jnp.where(low, zero, values)

            def one(i, carry):
                rs = self.at(i)
                query = self.q[rs, ls]
                qzero = jnp.zeros_like(query)
                lead = jnp.broadcast_to(jnp.where(lane == 0, 1.0, 0.0), (BLK, 128)).astype(bf16)
                out = None
                for half, vaug in ((0, self.vaug_a), (1, self.vaug_b)):
                    mine = jnp.where(low if half == 0 else jnp.logical_not(low), query, qzero)
                    scores = nt(jnp.concatenate([mine, lead], axis=1), self.kaug[...])
                    peak = jnp.max(scores, axis=-1, keepdims=True)
                    chances = jnp.exp(scores - peak).astype(bf16)
                    got = nn(chances, vaug[...])
                    total = got[:, 128:]
                    hi, mid, lo = three_parts(peak + jnp.log(total))
                    self.qaug[2 * p + half, rs, :] = jnp.where(
                        lane == 0, 1.0,
                        jnp.where(lane == 1, -hi, jnp.where(lane == 2, -mid, jnp.where(lane == 3, -lo, 0.0))),
                    ).astype(bf16)
                    part = got[:, :128] / total
                    out = part if out is None else out + part
                self.att[rs, ls] = out
                return carry

            lax.fori_loop(0, self.blocks, one, carry)
            hook(p)
            return carry

        lax.fori_loop(0, self.pairs, pair, 0)

    def feed(self):
        chunk = 512
        mix_at, up_at, down_at = self.offsets

        def one(i, carry):
            rs = self.at(i)
            live = self.live[rs, :]
            attended = self.att[rs, :].astype(bf16)
            self.att_t[:, rs] = attended.T
            mix_w = self.weight(mix_at, self.width)
            middle = self.load(self.x, i).astype(f32) + live * (nn(attended, mix_w) + self.row(4))
            second_norm, factor = normalize(middle)
            second_in = (second_norm * self.row(5) + self.row(6)).astype(bf16)
            self.second_t[:, rs] = second_in.T
            outer = self.load(self.g, i).astype(f32)
            down_in = (live * outer).astype(bf16)
            self.down_t[:, rs] = down_in.T
            self.vsum[7:8, :] += col_sum(down_in.astype(f32))
            self.acc_a[...] = jnp.zeros_like(self.acc_a)
            self.acc_b[...] = jnp.zeros_like(self.acc_b)

            def part(c, carry):
                cs = self.at(c, chunk)
                up = self.weight(pl.multiple_of(up_at + c * chunk, 128), chunk)
                down = self.weight(pl.multiple_of(down_at + c * chunk, 128), chunk)
                pre = nn(second_in, up) + self.upb[:, cs]
                phi = 0.5 * (1.0 + lax.erf(pre * root_half))
                hid = (pre * phi).astype(bf16)
                slope = phi + pre * jnp.exp(-0.5 * pre * pre) * gauss_norm
                self.hid[rs, cs] = hid
                self.acc_a[...] += nt(hid, down)
                pre_grad = (nn(down_in, down) * slope).astype(bf16)
                self.pre[rs, cs] = pre_grad
                self.usum[:, cs] += col_sum(pre_grad.astype(f32))
                self.acc_b[...] += nt(pre_grad, up)
                return carry

            lax.fori_loop(0, self.hidden // chunk, part, 0)
            self.save(self.final, i, (middle + live * (self.acc_a[...] + self.row(7))).astype(bf16))
            second_in_grad = self.acc_b[...]
            self.vsum[5:6, :] += col_sum(second_in_grad * second_norm)
            self.vsum[6:7, :] += col_sum(second_in_grad)
            middle_grad = outer + norm_back(second_in_grad * self.row(5), second_norm, factor)
            self.mg[rs, :] = middle_grad
            mix_in = (live * middle_grad).astype(bf16)
            self.mixin[rs, :] = mix_in
            self.vsum[4:5, :] += col_sum(mix_in.astype(f32))
            self.dout[rs, :] = nt(mix_in, mix_w).astype(bf16)
            return carry

        lax.fori_loop(0, self.blocks, one, 0)

    def wide(self, lhs_t, rhs, base, count):
        def one(c, carry):
            self.put(base + c, nn(lhs_t[...], rhs[:, self.at(c, 512)]))
            return carry

        lax.fori_loop(0, count, one, 0)

    def down_grad(self):
        self.wide(self.down_t, self.hid, 0, self.hidden // 512)

    def up_grad(self):
        self.wide(self.second_t, self.pre, self.hidden // 512, self.hidden // 512)

    def mix_grad(self):
        self.wide(self.att_t, self.mixin, 2 * self.hidden // 512, self.width // 512)

    def joint_grad(self):
        self.wide(self.first_t, self.hid, (2 * self.hidden + self.width) // 512, 3 * self.width // 512)

    def attend_back(self, hook):
        lane, low, width = self.lane, self.low, self.width
        joint = self.hid

        def pair(p, carry):
            ls = self.at(p, 128)
            keys = self.k[:, ls]
            self.kaug[:, :128] = keys
            self.vaug_a[:, :128] = self.v[:, ls]
            self.vaug_a[:, 128:] = self.kaug[:, 128:]
            zero = jnp.zeros_like(keys)
            self.vaug_b[:, :128] = jnp.where(low, keys, zero)
            self.vaug_b[:, 128:] = jnp.where(low, zero, keys)
            self.dk[...] = jnp.zeros_like(self.dk)
            self.dv[...] = jnp.zeros_like(self.dv)

            def one(i, carry):
                rs = self.at(i)
                query = self.q[rs, ls]
                grad = self.dout[rs, ls]
                both = grad.astype(f32) * self.att[rs, ls]
                dq = None
                for half in (0, 1):
                    keep = low if half == 0 else jnp.logical_not(low)
                    mine = jnp.where(keep, query, jnp.zeros_like(query))
                    grads = jnp.where(keep, grad, jnp.zeros_like(grad))
                    hi, mid, lo = three_parts(jnp.sum(jnp.where(keep, both, 0.0), axis=-1, keepdims=True))
                    gaug = jnp.where(
                        lane == 1, -hi, jnp.where(lane == 2, -mid, jnp.where(lane == 3, -lo, 0.0))
                    ).astype(bf16)
                    scores = nt(self.kaug[...], jnp.concatenate([mine, self.qaug[2 * p + half, rs, :]], axis=1))
                    chances = jnp.exp(scores)
                    centered = nt(self.vaug_a[...], jnp.concatenate([grads, gaug], axis=1))
                    score_grad = (chances * centered).astype(bf16)
                    self.dv[...] += nn(chances.astype(bf16), grads)
                    self.dk[...] += nn(score_grad, mine)
                    part = tn(score_grad, self.vaug_b[:, 128 * half : 128 * half + 128])
                    dq = part if dq is None else dq + part
                joint[rs, ls] = (dq * HEAD_DIM ** (-0.5)).astype(bf16)
                return carry

            lax.fori_loop(0, self.blocks, one, 0)
            joint[:, pl.ds(pl.multiple_of(width + p * 128, 128), 128)] = self.dk[...].astype(bf16)
            joint[:, pl.ds(pl.multiple_of(2 * width + p * 128, 128), 128)] = self.dv[...].astype(bf16)
            hook(p)
            return carry

        lax.fori_loop(0, self.pairs, pair, 0)

    def first_back(self, hook):
        width = self.width

        def one(i, carry):
            rs = self.at(i)
            grads = self.hid[rs, : 3 * width]
            self.vsum[2:3, :] += col_sum(grads[:, :width].astype(f32))
            self.vsum[3:4, :] += col_sum(grads[:, 2 * width :].astype(f32))
            first_in_grad = nt(grads, self.weight(0, 3 * width))
            normed, factor = normalize(self.load(self.x, i).astype(f32))
            self.vsum[0:1, :] += col_sum(first_in_grad * normed)
            self.vsum[1:2, :] += col_sum(first_in_grad)
            token_grad = self.load_mg(rs) + norm_back(first_in_grad * self.row(0), normed, factor)
            self.save(self.tg, i, token_grad.astype(bf16))
            hook(i)
            return carry

        lax.fori_loop(0, self.blocks, one, 0)

    def load_mg(self, rs):
        return self.mg[rs, :]


def layer_scratch(rows, width, hidden):
    return [
        pltpu.VMEM((rows, width), bf16),
        pltpu.VMEM((rows, width), bf16),
        pltpu.VMEM((rows, width), bf16),
        pltpu.VMEM((rows, width), f32),
        pltpu.VMEM((HEADS, rows, 128), bf16),
        pltpu.VMEM((width, rows), bf16),
        pltpu.VMEM((width, rows), bf16),
        pltpu.VMEM((width, rows), bf16),
        pltpu.VMEM((width, rows), bf16),
        pltpu.VMEM((rows, width), bf16),
        pltpu.VMEM((rows, width), f32),
        pltpu.VMEM((rows, width), bf16),
        pltpu.VMEM((rows, hidden), bf16),
        pltpu.VMEM((rows, hidden), bf16),
        pltpu.VMEM((rows, 256), bf16),
        pltpu.VMEM((rows, 256), bf16),
        pltpu.VMEM((rows, 256), bf16),
        pltpu.VMEM((rows, 128), f32),
        pltpu.VMEM((rows, 128), f32),
        pltpu.VMEM((BLK, width), f32),
        pltpu.VMEM((BLK, width), f32),
    ]


class Exchange:
    def __init__(self, grads, cs, wide_first, emit, scratch, send, recv, high):
        self.grads, self.cs, self.wide_first, self.emit, self.high = grads, cs, wide_first, emit, high
        self.from_core, self.after_core, self.from_one, self.after_one, self.from_two, self.after_two, self.last = scratch
        _, _, (a, b, c, e) = my_place()
        self.place = (a, b, c, e)
        across = {"fsdp": (1 - c) * 2 + e}, {"dp": a * 2 + 1 - b}

        def describe(source, target, slot, device):
            return pltpu.make_async_remote_copy(
                src_ref=source, dst_ref=target, send_sem=send.at[slot], recv_sem=recv.at[slot],
                device_id=device, device_id_type=MESH)

        stages = [[describe(grads.at[:, :, :, 1 - e, :, cs], self.from_core, 0, {"fsdp": c * 2 + 1 - e})]]
        if wide_first:
            stages.append([describe(self.after_core.at[:, :, 1 - c], self.from_one, 1, across[0])])
            stages.append([describe(self.after_one.at[:, 1 - b], self.from_two, 2, across[1])])
        else:
            stages.append([describe(self.after_core.at[:, 1 - b], self.from_one, 1, across[1])])
            stages.append([describe(self.after_one.at[:, 1 - c], self.from_two, 2, across[0])])
        copies = []
        for s in range(1, high):
            other = lax.rem(a + s, high)
            copies.append(describe(self.after_two.at[other], self.last.at[a], 2 + s, {"dp": other * 2 + b}))
        stages.append(copies)
        self.stages = stages

    def launch(self, number):
        for copy in self.stages[number]:
            copy.start()

    def start(self):
        self.launch(0)

    def step(self, number):
        a, b, c, e = self.place
        for copy in self.stages[number]:
            copy.wait_recv()
        if number == 0:
            def one(i, carry):
                mine = self.grads[i, :, :, e, :, self.cs]
                self.after_core[i] = (mine.astype(f32) + self.from_core[i].astype(f32)).astype(bf16)
                return carry
        elif number == 1:
            def one(i, carry):
                mine = self.after_core[i, :, c] if self.wide_first else self.after_core[i, b]
                self.after_one[i] = (mine.astype(f32) + self.from_one[i].astype(f32)).astype(bf16)
                return carry
        elif number == 2:
            def one(i, carry):
                mine = self.after_one[i, b] if self.wide_first else self.after_one[i, c]
                self.after_two[i] = (mine.astype(f32) + self.from_two[i].astype(f32)).astype(bf16)
                return carry
        if number < 3:
            lax.fori_loop(0, self.high, one, 0)
            self.launch(number + 1)
        else:
            total = self.after_two[a].astype(f32)
            for s in range(1, self.high):
                total = total + self.last[lax.rem(a + s, self.high)].astype(f32)
            self.emit(total)

    def wait_sent(self):
        for stage in self.stages:
            for copy in stage:
                copy.wait_send()


def when_at(index, value, action):
    @pl.when(index == value)
    def _():
        action()


def fill_vectors(small, vec, upb):
    devices, own, _ = small.shape
    turned = small[:, :, :128].reshape(devices * own, 128).astype(f32).T
    vec[...] = turned[:8]
    low = lax.broadcasted_iota(jnp.int32, (1, 128), 1) < 64
    for i in range(devices // 2):
        left, right = small[2 * i, :, 128:].astype(f32), small[2 * i + 1, :, 128:].astype(f32)
        upb[:, 128 * i : 128 * i + 128] = jnp.where(low, left[0:1], right[0:1])


def first_kernel(sizes, members, others, *refs):
    shard, live, tokens, grads = refs[:4]
    weights_out, final, tg, total, vsum, usum, next_x, next_g, vec, upb = refs[4:14]
    weights, x, g, wsend, wrecv, tsend, trecv, local = refs[14:22]
    scratch = refs[22:]
    own = shard.shape[0]
    width, hidden = vec.shape[1], upb.shape[1]
    devices = members * others
    greet(members, others)
    swaps = [
        Swap(src, dst, local.at[n], tsend.at[n], trecv.at[n], members)
        for n, (src, dst) in enumerate(
            ((tokens.at[0], x), (grads.at[0], g), (tokens.at[1], next_x), (grads.at[1], next_g)))
    ]
    mix_at = 3 * width + SMALL
    up_at = mix_at + width
    down_at = up_at + hidden
    ranges = (
        (pl.ds(0, 1024), (0, 1, 2, 3)),
        (pl.ds(1024, mix_at - 1024), (0, 2, 1, 3)),
        (pl.ds(up_at, hidden), (0, 1, 2, 3)),
        (pl.ds(down_at, hidden), (0, 2, 1, 3)),
        (pl.ds(mix_at, width), (0, 1, 2, 3)),
    )
    gathers = [
        Gather(shard, weights, cs, order, local.at[4 + n], wsend.at[n], wrecv.at[n], sizes)
        for n, (cs, order) in enumerate(ranges)
    ]
    early, late = gathers[:2], gathers[2:]
    for gather in early:
        gather.start(0)
    swaps[0].start()
    for number in range(1, 4):
        for gather in early:
            gather.wait(number - 1)
            gather.start(number)
    for gather in late:
        gather.start(0)
    swaps[1].start()

    def weight(start, size):
        return weights[:, :, :, :, :, pl.ds(start, size)].reshape(width, size)

    def put(k, value):
        total[:, pl.ds(pl.multiple_of(k * 512, 512), 512)] = value

    vsum[...] = jnp.zeros_like(vsum)
    usum[...] = jnp.zeros_like(usum)
    layer = Layer(x, g, live, weight, (mix_at, up_at, down_at), vec, upb, final, tg, put, vsum, usum, scratch)
    layer.masks()
    for gather in early:
        gather.wait(3)
    fill_vectors(weights[:, :, :, :, :, 3 * width : mix_at].reshape(devices, own, SMALL), vec, upb)
    swaps[0].wait()
    layer.project()

    def relay(number):
        def action():
            for gather in late:
                gather.wait(number - 1)
                gather.start(number)
        return action

    def hook(p):
        for number in (1, 2, 3):
            when_at(p, number - 1, relay(number))

    layer.attend(hook)
    for gather in late:
        gather.wait(3)
    swaps[1].wait()
    swaps[2].start()
    swaps[3].start()
    keep = pltpu.make_async_copy(weights, weights_out, local.at[4 + len(ranges)])
    keep.start()
    layer.feed()
    layer.down_grad()
    layer.up_grad()
    layer.mix_grad()
    layer.attend_back(lambda p: None)
    layer.joint_grad()
    layer.first_back(lambda i: None)
    keep.wait()
    for swap in swaps[2:]:
        swap.wait()
    for item in swaps + gathers:
        item.wait_sent()


def second_kernel(sizes, members, others, *refs):
    x, g, live, weights, vec, upb, previous, vprev, uprev, final0, tg0 = refs[:11]
    outs = refs[11:16]
    returned = refs[16:20]
    refs = refs[20:]
    final, tg, total, extra, vsum, usum, stage, wsend, wrecv, tsend, trecv, local, prior = refs[:13]
    pools = [refs[13 + 7 * n : 20 + 7 * n] for n in range(4)]
    scratch = refs[41:]
    high = sizes[0]
    width, hidden = vec.shape[1], upb.shape[1]
    devices = members * others
    own = width // devices
    greet(members, others)
    swaps = [
        Swap(src, dst, local.at[n], tsend.at[n], trecv.at[n], members)
        for n, (src, dst) in enumerate(zip((final0, tg0, final, tg), returned))
    ]
    swaps[0].start()
    swaps[1].start()

    def fetch(k):
        slot = lax.rem(k, 2)
        return pltpu.make_async_copy(
            previous.at[:, pl.ds(pl.multiple_of(k * 512, 512), 512)], stage.at[slot], prior.at[slot])

    chunks = (2 * hidden + 4 * width) // 512
    fetch(0).start()

    def put(k, value):
        fetch(k).wait()

        @pl.when(k + 1 < chunks)
        def _():
            fetch(k + 1).start()

        value = (value + stage[lax.rem(k, 2)]).astype(bf16)
        total[:, :, :, :, :, pl.ds(pl.multiple_of(k * 512, 512), 512)] = value.reshape(sizes + (own, 512))

    def weight(start, size):
        return weights[:, pl.ds(start, size)]

    mix_at = 3 * width + SMALL
    up_at = mix_at + width
    down_at = up_at + hidden
    vsum[...] = vprev[...]
    usum[...] = uprev[...]
    layer = Layer(x, g, live, weight, (mix_at, up_at, down_at), vec, upb, final, tg, put, vsum, usum, scratch)

    def emit_to(ref, lo=None, hi=None):
        def emit(value):
            ref[...] = value
        return emit

    joint_at = 2 * hidden + width
    down, up, rest, tail = (
        Exchange(grads, cs, wide_first, emit, pools[n], wsend.at[n], wrecv.at[n], high)
        for n, (grads, cs, wide_first, emit) in enumerate((
            (total, pl.ds(0, hidden), True, emit_to(outs[3])),
            (total, pl.ds(hidden, hidden + width), False, lambda v: emit_pair(v)),
            (total, pl.ds(joint_at, 3 * width), True, emit_to(outs[0])),
            (extra, pl.ds(0, SMALL), False, emit_to(outs[4])),
        ))
    )

    def emit_pair(value):
        outs[2][...] = value[:, :hidden]
        outs[1][...] = value[:, hidden:]

    layer.masks()
    layer.project()
    layer.attend(lambda p: None)
    layer.feed()
    layer.down_grad()
    layer.up_grad()
    down.start()
    layer.mix_grad()
    swaps[2].start()

    def hook(p):
        for number in range(4):
            when_at(p, number, lambda number=number: down.step(number))
        when_at(p, 0, up.start)
        for number in range(3):
            when_at(p, number + 1, lambda number=number: up.step(number))

    layer.attend_back(hook)
    layer.joint_grad()
    up.step(3)
    rest.start()
    first = swaps[3]
    per = BLK // tg.shape[1]
    me = lax.axis_index("dp")

    layer.first_back(lambda i: None)
    first.start()
    vectors = jnp.concatenate([vsum[...], jnp.zeros((120, width), f32)], axis=0).T
    extra[:, :, :, :, :, :128] = vectors.astype(bf16).reshape(sizes + (own, 128))
    for n in range(devices):
        a, b, c, e = n // (2 * others), (n // others) % 2, (n % others) // 2, n % 2
        piece = usum[:, 128 * (n // 2) : 128 * (n // 2) + 128]
        extra[a, b, c, e, :, 128:] = jnp.broadcast_to(piece, (own, 128)).astype(bf16)
    tail.start()
    for number in range(4):
        rest.step(number)
        tail.step(number)
    for swap in swaps:
        swap.wait()
    for item in swaps + [down, up, rest, tail]:
        item.wait_sent()


def first_call(shard, live, tokens, grads, members, others, hidden):
    own, columns = shard.shape
    micro, _, piece, width = tokens.shape
    rows = members * piece
    sizes = (members // 2, 2, others // 2, 2)
    slots = sizes[0] + 1 + sizes[2]
    block = jax.ShapeDtypeStruct((members, piece, width), bf16)
    dma = pltpu.SemaphoreType.DMA
    return pl.pallas_call(
        functools.partial(first_kernel, sizes, members, others),
        out_shape=(
            jax.ShapeDtypeStruct(sizes + (own, columns), bf16), block, block,
            jax.ShapeDtypeStruct((width, 2 * hidden + 4 * width), f32),
            jax.ShapeDtypeStruct((8, width), f32), jax.ShapeDtypeStruct((1, hidden), f32), block, block,
            jax.ShapeDtypeStruct((8, width), f32), jax.ShapeDtypeStruct((1, hidden), f32),
        ),
        in_specs=[VMEM, VMEM, ANY, ANY],
        out_specs=(ANY,) + (VMEM,) * 5 + (ANY,) * 2 + (VMEM,) * 2,
        scratch_shapes=[
            pltpu.VMEM(sizes + (own, columns), bf16),
            pltpu.VMEM((members, piece, width), bf16),
            pltpu.VMEM((members, piece, width), bf16),
            dma((5, slots)), dma((5, slots)), dma((4, members)), dma((4, members)), dma((10,)),
        ] + layer_scratch(rows, width, hidden),
        compiler_params=pltpu.CompilerParams(
            collective_id=2, has_side_effects=True, vmem_limit_bytes=67_043_328),
        name="first_sequence",
    )(shard, live, tokens, grads)


def second_call(x, g, live, weights, vec, upb, previous, vprev, uprev, final0, tg0, members, others):
    _, piece, width = x.shape
    rows, hidden = members * piece, upb.shape[1]
    sizes = (members // 2, 2, others // 2, 2)
    own = width // (members * others)
    dma = pltpu.SemaphoreType.DMA
    block = jax.ShapeDtypeStruct((members, piece, width), bf16)
    pools = []
    for columns in (hidden, hidden + width, 3 * width, SMALL):
        pools += reduce_scratch(sizes[0], own, columns)
    shapes = [(own, 3 * width), (own, width), (own, hidden), (own, hidden), (own, SMALL)]
    return pl.pallas_call(
        functools.partial(second_kernel, sizes, members, others),
        out_shape=tuple(jax.ShapeDtypeStruct(shape, f32) for shape in shapes) + (block,) * 4,
        in_specs=[VMEM] * 6 + [ANY] + [VMEM] * 2 + [ANY] * 2,
        out_specs=(VMEM,) * 5 + (ANY,) * 4,
        scratch_shapes=[
            pltpu.VMEM((members, piece, width), bf16),
            pltpu.VMEM((members, piece, width), bf16),
            pltpu.VMEM(sizes + (own, 2 * hidden + 4 * width), bf16),
            pltpu.VMEM(sizes + (own, SMALL), bf16),
            pltpu.VMEM((8, width), f32),
            pltpu.VMEM((1, hidden), f32),
            pltpu.VMEM((2, width, 512), f32),
            dma((4, sizes[0] + 2)), dma((4, sizes[0] + 2)), dma((4, members)), dma((4, members)), dma((4,)), dma((2,)),
        ] + pools + layer_scratch(rows, width, hidden),
        compiler_params=pltpu.CompilerParams(
            collective_id=3, has_side_effects=True, vmem_limit_bytes=67_043_328),
        name="second_sequence",
    )(x, g, live, weights, vec, upb, previous, vprev, uprev, final0, tg0)


def fused_body(
    tokens, out_grad, seq_lengths, send_to, slot_of, first_gain, first_shift, joint_weight, query_bias,
    value_bias, mix_weight, mix_bias, second_gain, second_shift, up_weight, up_bias, down_weight, down_bias,
):
    members, others = lax.axis_size("dp"), lax.axis_size("fsdp")
    micro, rows, width = tokens.shape
    piece = rows // members
    own = first_gain.shape[0]
    hidden = down_weight.shape[0]
    vectors = (first_gain, first_shift, query_bias, value_bias, mix_bias, second_gain, second_shift, down_bias)
    twice = jnp.broadcast_to(jnp.concatenate([up_bias, up_bias])[None], (own, 128))
    small = jnp.concatenate([jnp.stack(vectors, axis=1), jnp.zeros((own, 120), bf16), twice], axis=1)
    shard = jnp.concatenate([joint_weight, small, mix_weight, up_weight, down_weight.T], axis=1)
    table = send_to[:, 0]
    pieces = (micro, members, piece, width)
    sent, sent_grad = reorder(True, table, tokens.reshape(pieces), out_grad.reshape(pieces))
    spots = slot_of[:, 0, :, None] * piece + jnp.arange(piece, dtype=jnp.int32)
    live = (spots.reshape(micro, rows) < seq_lengths).astype(f32)[:, :, None]
    weights, final0, tg0, total, vsum, usum, x, g, vec, upb = first_call(
        shard, live[0], sent, sent_grad, members, others, hidden)
    whole = weights.reshape(width, shard.shape[1])
    joint, mix, up, down, tail, *returned = second_call(
        x, g, live[1], whole, vec, upb, total, vsum, usum, final0, tg0, members, others)
    layer_output, input_grad = reorder(
        False, table, jnp.stack([returned[0], returned[2]]), jnp.stack([returned[1], returned[3]]))
    vec_grad = [tail[:, n] for n in range(8)]
    odd = lax.rem(lax.axis_index("fsdp"), 2) == 1
    up_bias_grad = jnp.where(odd, tail[0, 192:256], tail[0, 128:192])
    return (
        layer_output.reshape(tokens.shape), input_grad.reshape(tokens.shape),
        vec_grad[0], vec_grad[1], joint, vec_grad[2], vec_grad[3], mix, vec_grad[4], vec_grad[5], vec_grad[6],
        up, up_bias_grad, down.T, vec_grad[7],
    )


def solution(mesh):
    both = ("dp", "fsdp")
    row3, row2, vector, matrix = P(None, both, None), P(None, both), P(both), P(both, None)
    turned = P(None, both)
    members, others = mesh.shape["dp"], mesh.shape["fsdp"]
    fits = members * others == 32 and others == 4
    return jax.shard_map(
        fused_body if fits else body,
        mesh=mesh,
        in_specs=(row3, row3, row2, row3, row3, vector, vector, matrix, vector, vector, matrix, vector, vector,
                  vector, matrix, vector, turned, vector),
        out_specs=(row3, row3, vector, vector, matrix, vector, vector, matrix, vector, vector, vector, matrix,
                   vector, turned, vector),
        check_vma=False,
    )
```

```python
import functools
import math

import jax
import jax.numpy as jnp
from jax import lax
from jax.experimental import pallas as pl
from jax.experimental.pallas import tpu as pltpu
from jax.sharding import PartitionSpec as P

HEADS = 8
HEAD_DIM = 64
BLK = 256

f32, bf16 = jnp.float32, jnp.bfloat16
epsilon = 1e-05
masked_score = -1e30
root_half = math.sqrt(0.5)
gauss_norm = 1.0 / math.sqrt(2.0 * math.pi)


def nn(a, b):
    return lax.dot_general(a, b, (((1,), (0,)), ((), ())), preferred_element_type=f32)


def nt(a, b):
    return lax.dot_general(a, b, (((1,), (1,)), ((), ())), preferred_element_type=f32)


def tn(a, b):
    return lax.dot_general(a, b, (((0,), (0,)), ((), ())), preferred_element_type=f32)


def normalize(rows):
    center = rows - jnp.mean(rows, axis=-1, keepdims=True)
    spread = jnp.mean(center * center, axis=-1, keepdims=True)
    factor = lax.rsqrt(spread + epsilon)
    return center * factor, factor


def norm_back(grad_norm, normed, factor):
    first_mean = jnp.mean(grad_norm, axis=-1, keepdims=True)
    second_mean = jnp.mean(grad_norm * normed, axis=-1, keepdims=True)
    return factor * (grad_norm - first_mean - normed * second_mean)


def three_parts(v):
    hi = v.astype(bf16).astype(f32)
    mid = (v - hi).astype(bf16).astype(f32)
    return hi, mid, v - hi - mid


def col_sum(v):
    return jnp.sum(v, axis=0, keepdims=True)


def micro_kernel(first, *refs):
    x_ref, g_ref, live_ref, w_ref, vec_ref, upb_ref = refs[:6]
    refs = refs[6:]
    if not first:
        prev_ref, vprev_ref, uprev_ref = refs[:3]
        refs = refs[3:]
    final_ref, tg_ref, grad_ref, vsum_ref, usum_ref = refs[:5]
    (q_ref, k_ref, v_ref, att_ref, qaug_ref, first_t, second_t, down_t, att_t, mixin_ref, mg_ref,
     dout_ref, hid_ref, pre_ref, kaug, vaug_a, vaug_b, dk_acc, dv_acc, acc_a, acc_b) = refs[5:]
    rows, width = x_ref.shape
    hidden = upb_ref.shape[1]
    blocks = rows // BLK
    pairs = width // 128
    mix_at = 3 * width
    up_at = mix_at + width
    down_at = up_at + hidden
    lane = lax.broadcasted_iota(jnp.int32, (1, 128), 1)
    low_half = lane < HEAD_DIM

    def at(i, size=BLK):
        return pl.ds(pl.multiple_of(i * size, size), size)

    if first:
        vsum_ref[...] = jnp.zeros_like(vsum_ref)
        usum_ref[...] = jnp.zeros_like(usum_ref)
    else:
        vsum_ref[...] = vprev_ref[...]
        usum_ref[...] = uprev_ref[...]

    def row(ref, n):
        return ref[n : n + 1, :]

    live_all = live_ref[...]
    mask_aug = jnp.where(
        lane == 0, (live_all - 1.0) * (-masked_score), jnp.where(lane < 4, 1.0, 0.0)
    ).astype(bf16)
    kaug[:, 128:] = mask_aug
    vaug_a[:, 128:] = jnp.ones((rows, 128), bf16)
    vaug_b[:, 128:] = jnp.ones((rows, 128), bf16)

    def project(i, carry):
        rs = at(i)
        normed, _ = normalize(x_ref[rs, :].astype(f32))
        first_in = (normed * row(vec_ref, 0) + row(vec_ref, 1)).astype(bf16)
        first_t[:, rs] = first_in.T
        query = (nn(first_in, w_ref[:, :width]) + row(vec_ref, 2)).astype(bf16)
        q_ref[rs, :] = query * jnp.array(HEAD_DIM ** (-0.5), bf16)
        k_ref[rs, :] = nn(first_in, w_ref[:, width : 2 * width]).astype(bf16)
        v_ref[rs, :] = (nn(first_in, w_ref[:, 2 * width : 3 * width]) + row(vec_ref, 3)).astype(bf16)
        return carry

    lax.fori_loop(0, blocks, project, 0)

    def attend_pair(p, carry):
        ls = at(p, 128)
        kaug[:, :128] = k_ref[:, ls]
        values = v_ref[:, ls]
        zero = jnp.zeros_like(values)
        vaug_a[:, :128] = jnp.where(low_half, values, zero)
        vaug_b[:, :128] = jnp.where(low_half, zero, values)

        def attend(i, carry):
            rs = at(i)
            query = q_ref[rs, ls]
            qzero = jnp.zeros_like(query)
            one = jnp.broadcast_to(jnp.where(lane == 0, 1.0, 0.0), (BLK, 128)).astype(bf16)
            out = None
            for half, vaug in ((0, vaug_a), (1, vaug_b)):
                mine = jnp.where(low_half if half == 0 else jnp.logical_not(low_half), query, qzero)
                scores = nt(jnp.concatenate([mine, one], axis=1), kaug[...])
                peak = jnp.max(scores, axis=-1, keepdims=True)
                chances = jnp.exp(scores - peak).astype(bf16)
                got = nn(chances, vaug[...])
                total = got[:, 128:]
                lse = peak + jnp.log(total)
                hi, mid, lo = three_parts(lse)
                qaug_ref[2 * p + half, rs, :] = jnp.where(
                    lane == 0, 1.0,
                    jnp.where(lane == 1, -hi, jnp.where(lane == 2, -mid, jnp.where(lane == 3, -lo, 0.0))),
                ).astype(bf16)
                part = got[:, :128] / total
                out = part if out is None else out + part
            att_ref[rs, ls] = out
            return carry

        return lax.fori_loop(0, blocks, attend, carry)

    lax.fori_loop(0, pairs, attend_pair, 0)

    chunk = 512
    mix_w = w_ref.at[:, mix_at:up_at]

    def feed(i, carry):
        rs = at(i)
        live = live_ref[rs, :]
        attended = att_ref[rs, :].astype(bf16)
        att_t[:, rs] = attended.T
        middle = x_ref[rs, :].astype(f32) + live * (nn(attended, mix_w[...]) + row(vec_ref, 4))
        second_norm, factor = normalize(middle)
        second_in = (second_norm * row(vec_ref, 5) + row(vec_ref, 6)).astype(bf16)
        second_t[:, rs] = second_in.T
        outer = g_ref[rs, :].astype(f32)
        down_in = (live * outer).astype(bf16)
        down_t[:, rs] = down_in.T
        vsum_ref[7:8, :] += col_sum(down_in.astype(f32))
        acc_a[...] = jnp.zeros_like(acc_a)
        acc_b[...] = jnp.zeros_like(acc_b)

        def part(c, carry):
            cs = at(c, chunk)
            up = w_ref[:, pl.ds(pl.multiple_of(up_at + c * chunk, chunk), chunk)]
            down = w_ref[:, pl.ds(pl.multiple_of(down_at + c * chunk, chunk), chunk)]
            pre = nn(second_in, up) + upb_ref[:, cs]
            phi = 0.5 * (1.0 + lax.erf(pre * root_half))
            hid = (pre * phi).astype(bf16)
            slope = phi + pre * jnp.exp(-0.5 * pre * pre) * gauss_norm
            hid_ref[rs, cs] = hid
            acc_a[...] += nt(hid, down)
            pre_grad = (nn(down_in, down) * slope).astype(bf16)
            pre_ref[rs, cs] = pre_grad
            usum_ref[:, cs] += col_sum(pre_grad.astype(f32))
            acc_b[...] += nt(pre_grad, up)
            return carry

        lax.fori_loop(0, hidden // chunk, part, 0)
        final_ref[rs, :] = (middle + live * (acc_a[...] + row(vec_ref, 7))).astype(bf16)
        second_in_grad = acc_b[...]
        vsum_ref[5:6, :] += col_sum(second_in_grad * second_norm)
        vsum_ref[6:7, :] += col_sum(second_in_grad)
        middle_grad = outer + norm_back(second_in_grad * row(vec_ref, 5), second_norm, factor)
        mg_ref[rs, :] = middle_grad
        mix_in = (live * middle_grad).astype(bf16)
        mixin_ref[rs, :] = mix_in
        vsum_ref[4:5, :] += col_sum(mix_in.astype(f32))
        dout_ref[rs, :] = nt(mix_in, mix_w[...]).astype(bf16)
        return carry

    lax.fori_loop(0, blocks, feed, 0)

    def put(value, cs):
        if not first:
            value = value + prev_ref[:, cs]
        grad_ref[:, cs] = value.astype(grad_ref.dtype)

    def wide(lhs_t, rhs_ref, base, count):
        def one(c, carry):
            put(nn(lhs_t[...], rhs_ref[:, at(c, chunk)]),
                pl.ds(pl.multiple_of(base + c * chunk, chunk), chunk))
            return carry
        lax.fori_loop(0, count, one, 0)

    wide(down_t, hid_ref, down_at, hidden // chunk)
    wide(second_t, pre_ref, up_at, hidden // chunk)
    wide(att_t, mixin_ref, mix_at, width // chunk)

    joint_grad = hid_ref

    def back_pair(p, carry):
        ls = at(p, 128)
        keys = k_ref[:, ls]
        kaug[:, :128] = keys
        vaug_a[:, :128] = v_ref[:, ls]
        vaug_a[:, 128:] = kaug[:, 128:]
        zero = jnp.zeros_like(keys)
        vaug_b[:, :128] = jnp.where(low_half, keys, zero)
        vaug_b[:, 128:] = jnp.where(low_half, zero, keys)
        dk_acc[...] = jnp.zeros_like(dk_acc)
        dv_acc[...] = jnp.zeros_like(dv_acc)

        def back(i, carry):
            rs = at(i)
            query = q_ref[rs, ls]
            grad = dout_ref[rs, ls]
            both = grad.astype(f32) * att_ref[rs, ls]
            dq = None
            for half in (0, 1):
                keep = low_half if half == 0 else jnp.logical_not(low_half)
                mine = jnp.where(keep, query, jnp.zeros_like(query))
                grads = jnp.where(keep, grad, jnp.zeros_like(grad))
                inner = jnp.sum(jnp.where(keep, both, 0.0), axis=-1, keepdims=True)
                hi, mid, lo = three_parts(inner)
                gaug = jnp.where(
                    lane == 1, -hi, jnp.where(lane == 2, -mid, jnp.where(lane == 3, -lo, 0.0))
                ).astype(bf16)
                scores = nt(kaug[...], jnp.concatenate([mine, qaug_ref[2 * p + half, rs, :]], axis=1))
                chances = jnp.exp(scores)
                centered = nt(vaug_a[...], jnp.concatenate([grads, gaug], axis=1))
                score_grad = (chances * centered).astype(bf16)
                dv_acc[...] += nn(chances.astype(bf16), grads)
                dk_acc[...] += nn(score_grad, mine)
                part = tn(score_grad, vaug_b[:, 128 * half : 128 * half + 128])
                dq = part if dq is None else dq + part
            joint_grad[rs, ls] = (dq * HEAD_DIM ** (-0.5)).astype(bf16)
            return carry

        lax.fori_loop(0, blocks, back, 0)
        joint_grad[:, pl.ds(pl.multiple_of(width + p * 128, 128), 128)] = dk_acc[...].astype(bf16)
        joint_grad[:, pl.ds(pl.multiple_of(2 * width + p * 128, 128), 128)] = dv_acc[...].astype(bf16)
        return carry

    lax.fori_loop(0, pairs, back_pair, 0)

    wide(first_t, joint_grad, 0, 3 * width // chunk)

    def back_first(i, carry):
        rs = at(i)
        grads = joint_grad[rs, : 3 * width]
        vsum_ref[2:3, :] += col_sum(grads[:, :width].astype(f32))
        vsum_ref[3:4, :] += col_sum(grads[:, 2 * width :].astype(f32))
        first_in_grad = nt(grads, w_ref[:, : 3 * width])
        normed, factor = normalize(x_ref[rs, :].astype(f32))
        vsum_ref[0:1, :] += col_sum(first_in_grad * normed)
        vsum_ref[1:2, :] += col_sum(first_in_grad)
        tg_ref[rs, :] = (
            mg_ref[rs, :] + norm_back(first_in_grad * row(vec_ref, 0), normed, factor)
        ).astype(bf16)
        return carry

    lax.fori_loop(0, blocks, back_first, 0)


def micro_call(x, g, live, weights, vec, upb, previous=None):
    rows, width = x.shape
    hidden = upb.shape[1]
    columns = weights.shape[1]
    first = previous is None
    vmem = pl.BlockSpec(memory_space=pltpu.VMEM)
    args = (x, g, live, weights, vec, upb) + (() if first else previous)
    scratch = [
        pltpu.VMEM((rows, width), bf16),
        pltpu.VMEM((rows, width), bf16),
        pltpu.VMEM((rows, width), bf16),
        pltpu.VMEM((rows, width), f32),
        pltpu.VMEM((HEADS, rows, 128), bf16),
        pltpu.VMEM((width, rows), bf16),
        pltpu.VMEM((width, rows), bf16),
        pltpu.VMEM((width, rows), bf16),
        pltpu.VMEM((width, rows), bf16),
        pltpu.VMEM((rows, width), bf16),
        pltpu.VMEM((rows, width), f32),
        pltpu.VMEM((rows, width), bf16),
        pltpu.VMEM((rows, hidden), bf16),
        pltpu.VMEM((rows, hidden), bf16),
        pltpu.VMEM((rows, 256), bf16),
        pltpu.VMEM((rows, 256), bf16),
        pltpu.VMEM((rows, 256), bf16),
        pltpu.VMEM((rows, 128), f32),
        pltpu.VMEM((rows, 128), f32),
        pltpu.VMEM((BLK, width), f32),
        pltpu.VMEM((BLK, width), f32),
    ]
    flops = 2 * rows * width * columns * 3 + 7 * 2 * rows * rows * width * 4
    return pl.pallas_call(
        functools.partial(micro_kernel, first),
        out_shape=(
            jax.ShapeDtypeStruct((rows, width), bf16),
            jax.ShapeDtypeStruct((rows, width), bf16),
            jax.ShapeDtypeStruct((width, 4 * width + 2 * hidden), f32 if first else bf16),
            jax.ShapeDtypeStruct((8, width), f32),
            jax.ShapeDtypeStruct((1, hidden), f32),
        ),
        in_specs=[vmem] * len(args),
        out_specs=(vmem,) * 5,
        scratch_shapes=scratch,
        compiler_params=pltpu.CompilerParams(vmem_limit_bytes=67_043_328),
        cost_estimate=pl.CostEstimate(flops=flops, bytes_accessed=30_000_000, transcendentals=3 * HEADS * rows * rows),
        name="micro_first" if first else "micro_second",
    )(*args)


MESH = pl.DeviceIdType.MESH


def split_axes():
    members, others = lax.axis_size("dp"), lax.axis_size("fsdp")
    return members // 2, 2, others // 2, 2


def my_place():
    d, f = lax.axis_index("dp"), lax.axis_index("fsdp")
    return d, f, (d // 2, lax.rem(d, 2), f // 2, lax.rem(f, 2))


def greet(members, others):
    d, f = lax.axis_index("dp"), lax.axis_index("fsdp")
    barrier = pltpu.get_barrier_semaphore()
    for s in range(1, members):
        pl.semaphore_signal(barrier, inc=1, device_id={"dp": lax.rem(d + s, members)}, device_id_type=MESH)
    for s in range(1, others):
        pl.semaphore_signal(barrier, inc=1, device_id={"fsdp": lax.rem(f + s, others)}, device_id_type=MESH)
    pl.semaphore_wait(barrier, members + others - 2)


class Swap:
    def __init__(self, src, dst, local, send, recv, members):
        d = lax.axis_index("dp")
        self.copies = []
        for s in range(1, members):
            to = lax.rem(d + s, members)
            self.copies.append(pltpu.make_async_remote_copy(
                src_ref=src.at[to], dst_ref=dst.at[d], send_sem=send.at[s], recv_sem=recv.at[s],
                device_id={"dp": to}, device_id_type=MESH))
        self.own = pltpu.make_async_copy(src.at[d], dst.at[d], local)

    def start(self):
        for copy in self.copies:
            copy.start()
        self.own.start()

    def wait(self):
        for copy in self.copies:
            copy.wait_recv()
        self.own.wait()

    def wait_sent(self):
        for copy in self.copies:
            copy.wait_send()


class Gather:
    def __init__(self, src, out, cs, order, local, send, recv, sizes):
        a, b, c, e = my_place()[2]
        d, f = lax.axis_index("dp"), lax.axis_index("fsdp")
        high, _, wide, _ = sizes
        every = slice(None)
        place = [a, b, c, e]
        self.own = pltpu.make_async_copy(src.at[:, cs], out.at[a, b, c, e, :, cs], local)
        self.stages = []
        done = [False] * 4
        slot = 0
        for number, axis in enumerate(order):
            copies = []
            size = (high, 2, wide, 2)[axis]
            for s in range(1, size):
                other = lax.rem(place[axis] + s, size)
                if axis == 0:
                    target = {"dp": other * 2 + b}
                elif axis == 1:
                    target = {"dp": a * 2 + other}
                elif axis == 2:
                    target = {"fsdp": other * 2 + e}
                else:
                    target = {"fsdp": c * 2 + other}
                where = tuple(every if done[k] else place[k] for k in range(4)) + (every, cs)
                source = src.at[:, cs] if number == 0 else out.at[where]
                copies.append(pltpu.make_async_remote_copy(
                    src_ref=source, dst_ref=out.at[where], send_sem=send.at[slot], recv_sem=recv.at[slot],
                    device_id=target, device_id_type=MESH))
                slot += 1
            self.stages.append(copies)
            done[axis] = True

    def start(self, number):
        if number == 0:
            self.own.start()
        for copy in self.stages[number]:
            copy.start()

    def wait(self, number):
        for copy in self.stages[number]:
            copy.wait_recv()
        if number == 0:
            self.own.wait()

    def wait_sent(self):
        for stage in self.stages:
            for copy in stage:
                copy.wait_send()


class Reduce:
    def __init__(self, grads, cs, wide_first, emit, scratch, send, recv, high):
        self.grads, self.cs, self.wide_first, self.emit, self.high = grads, cs, wide_first, emit, high
        self.from_core, self.after_core, self.from_one, self.after_one, self.from_two, self.after_two, self.last = scratch
        self.send, self.recv = send, recv
        self.sent = []

    def push(self, source, target, slot, device):
        copy = pltpu.make_async_remote_copy(
            src_ref=source, dst_ref=target, send_sem=self.send.at[slot], recv_sem=self.recv.at[slot],
            device_id=device, device_id_type=MESH)
        copy.start()
        self.sent.append(copy)
        self.copy = copy

    def start(self):
        _, _, (a, b, c, e) = my_place()
        self.push(self.grads.at[:, :, :, 1 - e, :, self.cs], self.from_core, 0, {"fsdp": c * 2 + 1 - e})

    def step(self, number):
        d, f, (a, b, c, e) = my_place()
        across = {"fsdp": (1 - c) * 2 + e}, {"dp": a * 2 + 1 - b}
        if number == 0:
            self.copy.wait_recv()

            def one(i, carry):
                mine = self.grads[i, :, :, e, :, self.cs]
                self.after_core[i] = (mine.astype(f32) + self.from_core[i].astype(f32)).astype(bf16)
                return carry

            lax.fori_loop(0, self.high, one, 0)
            if self.wide_first:
                self.push(self.after_core.at[:, :, 1 - c], self.from_one, 1, across[0])
            else:
                self.push(self.after_core.at[:, 1 - b], self.from_one, 1, across[1])
        elif number == 1:
            self.copy.wait_recv()

            def two(i, carry):
                mine = self.after_core[i, :, c] if self.wide_first else self.after_core[i, b]
                self.after_one[i] = (mine.astype(f32) + self.from_one[i].astype(f32)).astype(bf16)
                return carry

            lax.fori_loop(0, self.high, two, 0)
            if self.wide_first:
                self.push(self.after_one.at[:, 1 - b], self.from_two, 2, across[1])
            else:
                self.push(self.after_one.at[:, 1 - c], self.from_two, 2, across[0])
        elif number == 2:
            self.copy.wait_recv()

            def three(i, carry):
                mine = self.after_one[i, b] if self.wide_first else self.after_one[i, c]
                self.after_two[i] = (mine.astype(f32) + self.from_two[i].astype(f32)).astype(bf16)
                return carry

            lax.fori_loop(0, self.high, three, 0)
            self.copies = []
            for s in range(1, self.high):
                other = lax.rem(a + s, self.high)
                self.push(self.after_two.at[other], self.last.at[a], 2 + s, {"dp": other * 2 + b})
                self.copies.append(self.copy)
        else:
            for copy in self.copies:
                copy.wait_recv()
            total = self.after_two[a].astype(f32)
            for s in range(1, self.high):
                total = total + self.last[lax.rem(a + s, self.high)].astype(f32)
            self.emit(total)

    def wait_sent(self):
        for copy in self.sent:
            copy.wait_send()


def reduce_scratch(high, rows, columns):
    shapes = [(high, 2, 2), (high, 2, 2), (high, 2), (high, 2), (high,), (high,), (high,)]
    return [pltpu.VMEM(lead + (rows, columns), bf16) for lead in shapes]


def gather_kernel(sizes, members, others, ranges, shard, tokens, grads, out, tokens_out, grads_out, wsend, wrecv, tsend, trecv, local):
    greet(members, others)
    micro = tokens.shape[0]
    swaps = []
    for step in range(micro):
        for kind, (src, dst) in enumerate(((tokens, tokens_out), (grads, grads_out))):
            n = step * 2 + kind
            swaps.append(Swap(src.at[step], dst.at[step], local.at[n], tsend.at[n], trecv.at[n], members))
    gathers = [
        Gather(shard, out, cs, order, local.at[2 * micro + n], wsend.at[n], wrecv.at[n], sizes)
        for n, (cs, order) in enumerate(ranges)
    ]
    swaps[0].start()
    for gather in gathers:
        gather.start(0)
    for number in range(1, 4):
        for gather in gathers:
            gather.wait(number - 1)
            gather.start(number)
        if number == 1:
            for swap in swaps[1:]:
                swap.start()
    for gather in gathers:
        gather.wait(3)
    for swap in swaps:
        swap.wait()
    for item in swaps + gathers:
        item.wait_sent()


def scatter_kernel(high, members, others, widths, grads, extra, *refs):
    sources, refs = refs[:4], refs[4:]
    outs, refs = refs[:5], refs[5:]
    returned, refs = refs[:4], refs[4:]
    wsend, wrecv, tsend, trecv, local = refs[-5:]
    scratch = refs[:-5]
    greet(members, others)
    width, hidden = widths
    swaps = [
        Swap(src, dst, local.at[n], tsend.at[n], trecv.at[n], members)
        for n, (src, dst) in enumerate(zip(sources, returned))
    ]

    def emit_first(total):
        outs[0][...] = total[:, : 3 * width]
        outs[1][...] = total[:, 3 * width :]

    def emit_to(ref):
        def emit(total):
            ref[...] = total
        return emit

    up_at, down_at = 4 * width, 4 * width + hidden
    items = [
        Reduce(grads, pl.ds(down_at, hidden), True, emit_to(outs[3]), scratch[0:7], wsend.at[0], wrecv.at[0], high),
        Reduce(grads, pl.ds(up_at, hidden), False, emit_to(outs[2]), scratch[7:14], wsend.at[1], wrecv.at[1], high),
        Reduce(grads, pl.ds(0, up_at), True, emit_first, scratch[14:21], wsend.at[2], wrecv.at[2], high),
        Reduce(extra, pl.ds(0, 128), False, emit_to(outs[4]), scratch[21:28], wsend.at[3], wrecv.at[3], high),
    ]
    for item in items:
        item.start()
    for swap in swaps:
        swap.start()
    for number in range(4):
        for item in items:
            item.step(number)
    for swap in swaps:
        swap.wait()
    for item in items + swaps:
        item.wait_sent()


def order_kernel(scatter, table, *refs):
    count = (len(refs) - 3) // 2
    sources, targets = refs[:count], refs[count : 2 * count]
    held, in_sem, out_sem = refs[2 * count :]
    micro, members = sources[0].shape[:2]
    incoming, outgoing = [], []
    for n in range(count):
        for m in range(micro):
            for p in range(members):
                other = table[m, p]
                src, dst = (p, other) if scatter else (other, p)
                slot = (n * micro + m) * members + p
                copy = pltpu.make_async_copy(sources[n].at[m, src], held.at[slot], in_sem.at[slot])
                copy.start()
                incoming.append(copy)
                outgoing.append(pltpu.make_async_copy(held.at[slot], targets[n].at[m, dst], out_sem.at[slot]))
    for one, two in zip(incoming, outgoing):
        one.wait()
        two.start()
    for two in outgoing:
        two.wait()


ANY = pl.BlockSpec(memory_space=pl.ANY)
VMEM = pl.BlockSpec(memory_space=pltpu.VMEM)


def reorder(scatter, table, *arrays):
    micro, members, piece, width = arrays[0].shape
    slots = len(arrays) * micro * members
    return pl.pallas_call(
        functools.partial(order_kernel, scatter),
        out_shape=tuple(jax.ShapeDtypeStruct(item.shape, item.dtype) for item in arrays),
        in_specs=[pl.BlockSpec(memory_space=pltpu.SMEM)] + [ANY] * len(arrays),
        out_specs=(ANY,) * len(arrays),
        scratch_shapes=[
            pltpu.VMEM((slots, piece, width), arrays[0].dtype),
            pltpu.SemaphoreType.DMA((slots,)),
            pltpu.SemaphoreType.DMA((slots,)),
        ],
        name="order_out" if scatter else "order_in",
    )(table, *arrays)


def gather_call(shard, tokens, grads, members, others):
    rows, columns = shard.shape
    high, wide = members // 2, others // 2
    sizes = (high, 2, wide, 2)
    micro = tokens.shape[0]
    third = 2048
    ranges = (
        (pl.ds(0, third), (0, 1, 2, 3)),
        (pl.ds(third, third), (0, 2, 1, 3)),
        (pl.ds(2 * third, columns - 2 * third), (0, 1, 2, 3)),
    )
    slots = high + 1 + wide
    return pl.pallas_call(
        functools.partial(gather_kernel, sizes, members, others, ranges),
        out_shape=(
            jax.ShapeDtypeStruct(sizes + (rows, columns), shard.dtype),
            jax.ShapeDtypeStruct(tokens.shape, tokens.dtype),
            jax.ShapeDtypeStruct(grads.shape, grads.dtype),
        ),
        in_specs=[VMEM, ANY, ANY],
        out_specs=(ANY,) * 3,
        scratch_shapes=[
            pltpu.SemaphoreType.DMA((len(ranges), slots)),
            pltpu.SemaphoreType.DMA((len(ranges), slots)),
            pltpu.SemaphoreType.DMA((2 * micro, members)),
            pltpu.SemaphoreType.DMA((2 * micro, members)),
            pltpu.SemaphoreType.DMA((2 * micro + len(ranges),)),
        ],
        compiler_params=pltpu.CompilerParams(collective_id=0, has_side_effects=True),
        name="gather_in",
    )(shard, tokens, grads)


def scatter_call(grads, extra, arrays, members, others, width, hidden):
    high = members // 2
    rows = grads.shape[4]
    scratch = []
    for columns in (hidden, hidden, 4 * width, 128):
        scratch += reduce_scratch(high, rows, columns)
    shapes = [(rows, 3 * width), (rows, width), (rows, hidden), (rows, hidden), (rows, 128)]
    return pl.pallas_call(
        functools.partial(scatter_kernel, high, members, others, (width, hidden)),
        out_shape=tuple(jax.ShapeDtypeStruct(shape, f32) for shape in shapes)
        + tuple(jax.ShapeDtypeStruct(item.shape, item.dtype) for item in arrays),
        in_specs=[VMEM, VMEM] + [ANY] * 4,
        out_specs=(VMEM,) * 5 + (ANY,) * 4,
        scratch_shapes=scratch + [
            pltpu.SemaphoreType.DMA((4, high + 2)),
            pltpu.SemaphoreType.DMA((4, high + 2)),
            pltpu.SemaphoreType.DMA((4, members)),
            pltpu.SemaphoreType.DMA((4, members)),
            pltpu.SemaphoreType.DMA((4,)),
        ],
        compiler_params=pltpu.CompilerParams(
            collective_id=1, has_side_effects=True, vmem_limit_bytes=67_043_328),
        name="scatter_out",
    )(grads, extra, *arrays)


def body(
    tokens, out_grad, seq_lengths, send_to, slot_of, first_gain, first_shift, joint_weight, query_bias,
    value_bias, mix_weight, mix_bias, second_gain, second_shift, up_weight, up_bias, down_weight, down_bias,
):
    members, others = lax.axis_size("dp"), lax.axis_size("fsdp")
    devices = members * others
    micro, rows, width = tokens.shape
    piece = rows // members
    own = first_gain.shape[0]
    hidden = down_weight.shape[0]
    per = hidden // width
    vectors = (first_gain, first_shift, query_bias, value_bias, mix_bias, second_gain, second_shift, down_bias)
    small = jnp.concatenate(
        [jnp.stack(vectors, axis=1), up_bias.reshape(own, per), jnp.zeros((own, 128 - 8 - per), bf16)], axis=1)
    shard = jnp.concatenate([joint_weight, mix_weight, up_weight, down_weight.T, small], axis=1)
    table = send_to[:, 0]
    pieces = (micro, members, piece, width)
    sent = reorder(True, table, tokens.reshape(pieces), out_grad.reshape(pieces))
    gathered, routed, routed_grad = gather_call(shard, *sent, members, others)
    whole = gathered.reshape(width, shard.shape[1])
    tail = whole[:, 4 * width + 2 * hidden :].astype(f32)
    vec = tail[:, :8].T
    upb = tail[:, 8 : 8 + per].reshape(1, hidden)
    spots = slot_of[:, 0, :, None] * piece + jnp.arange(piece, dtype=jnp.int32)
    live = (spots.reshape(micro, rows) < seq_lengths).astype(f32)[:, :, None]
    previous = None
    results = []
    for step in range(micro):
        final, token_grad, *previous = micro_call(
            routed[step].reshape(rows, width), routed_grad[step].reshape(rows, width), live[step], whole, vec, upb,
            previous and tuple(previous))
        results += [final.reshape(members, piece, width), token_grad.reshape(members, piece, width)]
    total, vsum, usum = previous
    sizes = (members // 2, 2, others // 2, 2, own)
    grads = total.reshape(sizes + (total.shape[1],))
    extra = jnp.concatenate(
        [vsum.T, usum.reshape(width, per), jnp.zeros((width, 128 - 8 - per), f32)], axis=1
    ).astype(bf16).reshape(sizes + (128,))
    joint, mix, up, down, tail, *returned = scatter_call(grads, extra, results, members, others, width, hidden)
    layer_output, input_grad = reorder(
        False, table, jnp.stack([returned[0], returned[2]]), jnp.stack([returned[1], returned[3]]))
    vec_grad = [tail[:, n] for n in range(8)]
    return (
        layer_output.reshape(tokens.shape), input_grad.reshape(tokens.shape),
        vec_grad[0], vec_grad[1], joint, vec_grad[2], vec_grad[3], mix, vec_grad[4], vec_grad[5], vec_grad[6],
        up, tail[:, 8 : 8 + per].reshape(up_bias.shape), down.T, vec_grad[7],
    )


SMALL = 256


class Layer:
    def __init__(self, x, g, live, weight, offsets, vec, upb, final, tg, put, vsum, usum, scratch):
        self.x, self.g, self.live, self.weight, self.offsets = x, g, live, weight, offsets
        self.vec, self.upb, self.final, self.tg, self.put, self.vsum, self.usum = vec, upb, final, tg, put, vsum, usum
        (self.q, self.k, self.v, self.att, self.qaug, self.first_t, self.second_t, self.down_t, self.att_t, self.mixin,
         self.mg, self.dout, self.hid, self.pre, self.kaug, self.vaug_a, self.vaug_b, self.dk, self.dv, self.acc_a,
         self.acc_b) = scratch
        self.rows, self.width = self.q.shape
        self.hidden = upb.shape[1]
        self.blocks = self.rows // BLK
        self.pairs = self.width // 128
        self.lane = lax.broadcasted_iota(jnp.int32, (1, 128), 1)
        self.low = self.lane < HEAD_DIM

    def at(self, i, size=BLK):
        return pl.ds(pl.multiple_of(i * size, size), size)

    def row(self, n):
        return self.vec[n : n + 1, :]

    def load(self, ref, i):
        per = BLK // ref.shape[1]
        return ref[pl.ds(i * per, per)].reshape(BLK, self.width)

    def save(self, ref, i, value):
        per = BLK // ref.shape[1]
        ref[pl.ds(i * per, per)] = value.reshape(per, ref.shape[1], self.width)

    def masks(self):
        rows, lane = self.rows, self.lane
        self.kaug[:, 128:] = jnp.where(
            lane == 0, (self.live[...] - 1.0) * (-masked_score), jnp.where(lane < 4, 1.0, 0.0)
        ).astype(bf16)
        self.vaug_a[:, 128:] = jnp.ones((rows, 128), bf16)
        self.vaug_b[:, 128:] = jnp.ones((rows, 128), bf16)

    def project(self, turn, arrive):
        width = self.width

        def one(s, carry):
            arrive(s)
            i = turn(s)
            rs = self.at(i)
            normed, _ = normalize(self.load(self.x, i).astype(f32))
            first_in = (normed * self.row(0) + self.row(1)).astype(bf16)
            self.first_t[:, rs] = first_in.T
            query = (nn(first_in, self.weight(0, width)) + self.row(2)).astype(bf16)
            self.q[rs, :] = query * jnp.array(HEAD_DIM ** (-0.5), bf16)
            self.k[rs, :] = nn(first_in, self.weight(width, width)).astype(bf16)
            self.v[rs, :] = (nn(first_in, self.weight(2 * width, width)) + self.row(3)).astype(bf16)
            return carry

        lax.fori_loop(0, self.blocks, one, 0)

    def attend(self, hook):
        lane, low = self.lane, self.low

        def pair(p, carry):
            ls = self.at(p, 128)
            self.kaug[:, :128] = self.k[:, ls]
            values = self.v[:, ls]
            zero = jnp.zeros_like(values)
            self.vaug_a[:, :128] = jnp.where(low, values, zero)
            self.vaug_b[:, :128] = jnp.where(low, zero, values)

            def one(i, carry):
                rs = self.at(i)
                query = self.q[rs, ls]
                qzero = jnp.zeros_like(query)
                lead = jnp.broadcast_to(jnp.where(lane == 0, 1.0, 0.0), (BLK, 128)).astype(bf16)
                out = None
                for half, vaug in ((0, self.vaug_a), (1, self.vaug_b)):
                    mine = jnp.where(low if half == 0 else jnp.logical_not(low), query, qzero)
                    scores = nt(jnp.concatenate([mine, lead], axis=1), self.kaug[...])
                    peak = jnp.max(scores, axis=-1, keepdims=True)
                    chances = jnp.exp(scores - peak).astype(bf16)
                    got = nn(chances, vaug[...])
                    total = got[:, 128:]
                    hi, mid, lo = three_parts(peak + jnp.log(total))
                    self.qaug[2 * p + half, rs, :] = jnp.where(
                        lane == 0, 1.0,
                        jnp.where(lane == 1, -hi, jnp.where(lane == 2, -mid, jnp.where(lane == 3, -lo, 0.0))),
                    ).astype(bf16)
                    part = got[:, :128] / total
                    out = part if out is None else out + part
                self.att[rs, ls] = out
                hook(p * self.blocks + i)
                return carry

            return lax.fori_loop(0, self.blocks, one, carry)

        lax.fori_loop(0, self.pairs, pair, 0)

    def feed(self, turn, arrive):
        chunk = 512
        mix_at, up_at, down_at = self.offsets

        def one(s, carry):
            arrive(s)
            i = turn(s)
            rs = self.at(i)
            live = self.live[rs, :]
            attended = self.att[rs, :].astype(bf16)
            self.att_t[:, rs] = attended.T
            mix_w = self.weight(mix_at, self.width)
            middle = self.load(self.x, i).astype(f32) + live * (nn(attended, mix_w) + self.row(4))
            second_norm, factor = normalize(middle)
            second_in = (second_norm * self.row(5) + self.row(6)).astype(bf16)
            self.second_t[:, rs] = second_in.T
            outer = self.load(self.g, i).astype(f32)
            down_in = (live * outer).astype(bf16)
            self.down_t[:, rs] = down_in.T
            self.vsum[7:8, :] += col_sum(down_in.astype(f32))
            self.acc_a[...] = jnp.zeros_like(self.acc_a)
            self.acc_b[...] = jnp.zeros_like(self.acc_b)

            def part(c, carry):
                cs = self.at(c, chunk)
                up = self.weight(pl.multiple_of(up_at + c * chunk, 128), chunk)
                down = self.weight(pl.multiple_of(down_at + c * chunk, 128), chunk)
                pre = nn(second_in, up) + self.upb[:, cs]
                phi = 0.5 * (1.0 + lax.erf(pre * root_half))
                hid = (pre * phi).astype(bf16)
                slope = phi + pre * jnp.exp(-0.5 * pre * pre) * gauss_norm
                self.hid[c, rs, :] = hid
                self.acc_a[...] += nt(hid, down)
                pre_grad = (nn(down_in, down) * slope).astype(bf16)
                self.pre[c, rs, :] = pre_grad
                self.usum[:, cs] += col_sum(pre_grad.astype(f32))
                self.acc_b[...] += nt(pre_grad, up)
                return carry

            lax.fori_loop(0, self.hidden // chunk, part, 0)
            self.save(self.final, i, (middle + live * (self.acc_a[...] + self.row(7))).astype(bf16))
            second_in_grad = self.acc_b[...]
            self.vsum[5:6, :] += col_sum(second_in_grad * second_norm)
            self.vsum[6:7, :] += col_sum(second_in_grad)
            middle_grad = outer + norm_back(second_in_grad * self.row(5), second_norm, factor)
            self.mg[rs, :] = middle_grad
            mix_in = (live * middle_grad).astype(bf16)
            self.mixin[rs, :] = mix_in
            self.vsum[4:5, :] += col_sum(mix_in.astype(f32))
            self.dout[rs, :] = nt(mix_in, mix_w).astype(bf16)
            return carry

        lax.fori_loop(0, self.blocks, one, 0)

    def wide(self, lhs_t, rhs, base, count):
        def one(c, carry):
            self.put(base + c, nn(lhs_t[...], rhs[c]))
            return carry

        lax.fori_loop(0, count, one, 0)

    def down_grad(self):
        self.wide(self.down_t, self.hid, 0, self.hidden // 512)

    def up_grad(self):
        self.wide(self.second_t, self.pre, self.hidden // 512, self.hidden // 512)

    def mix_grad(self):
        self.put(2 * self.hidden // 512, nn(self.att_t[...], self.mixin[...]))

    def joint_grad(self):
        self.wide(self.first_t, self.hid, (2 * self.hidden + self.width) // 512, 3 * self.width // 512)

    def attend_back(self, hook):
        lane, low = self.lane, self.low
        joint = self.hid

        def pair(p, carry):
            ls = self.at(p, 128)
            keys = self.k[:, ls]
            self.kaug[:, :128] = keys
            self.vaug_a[:, :128] = self.v[:, ls]
            self.vaug_a[:, 128:] = self.kaug[:, 128:]
            zero = jnp.zeros_like(keys)
            self.vaug_b[:, :128] = jnp.where(low, keys, zero)
            self.vaug_b[:, 128:] = jnp.where(low, zero, keys)
            self.dk[...] = jnp.zeros_like(self.dk)
            self.dv[...] = jnp.zeros_like(self.dv)

            def one(i, carry):
                rs = self.at(i)
                query = self.q[rs, ls]
                grad = self.dout[rs, ls]
                both = grad.astype(f32) * self.att[rs, ls]
                dq = None
                for half in (0, 1):
                    keep = low if half == 0 else jnp.logical_not(low)
                    mine = jnp.where(keep, query, jnp.zeros_like(query))
                    grads = jnp.where(keep, grad, jnp.zeros_like(grad))
                    hi, mid, lo = three_parts(jnp.sum(jnp.where(keep, both, 0.0), axis=-1, keepdims=True))
                    gaug = jnp.where(
                        lane == 1, -hi, jnp.where(lane == 2, -mid, jnp.where(lane == 3, -lo, 0.0))
                    ).astype(bf16)
                    scores = nt(self.kaug[...], jnp.concatenate([mine, self.qaug[2 * p + half, rs, :]], axis=1))
                    chances = jnp.exp(scores)
                    centered = nt(self.vaug_a[...], jnp.concatenate([grads, gaug], axis=1))
                    score_grad = (chances * centered).astype(bf16)
                    self.dv[...] += nn(chances.astype(bf16), grads)
                    self.dk[...] += nn(score_grad, mine)
                    part = tn(score_grad, self.vaug_b[:, 128 * half : 128 * half + 128])
                    dq = part if dq is None else dq + part
                joint[0, rs, ls] = (dq * HEAD_DIM ** (-0.5)).astype(bf16)
                hook(p * self.blocks + i)
                return carry

            lax.fori_loop(0, self.blocks, one, 0)
            joint[1, :, ls] = self.dk[...].astype(bf16)
            joint[2, :, ls] = self.dv[...].astype(bf16)
            return carry

        lax.fori_loop(0, self.pairs, pair, 0)

    def first_back(self, turn, done):
        width = self.width

        def one(s, carry):
            i = turn(s)
            rs = self.at(i)
            grads = jnp.concatenate([self.hid[0, rs, :], self.hid[1, rs, :], self.hid[2, rs, :]], axis=1)
            self.vsum[2:3, :] += col_sum(grads[:, :width].astype(f32))
            self.vsum[3:4, :] += col_sum(grads[:, 2 * width :].astype(f32))
            first_in_grad = nt(grads, self.weight(0, 3 * width))
            normed, factor = normalize(self.load(self.x, i).astype(f32))
            self.vsum[0:1, :] += col_sum(first_in_grad * normed)
            self.vsum[1:2, :] += col_sum(first_in_grad)
            token_grad = self.mg[rs, :] + norm_back(first_in_grad * self.row(0), normed, factor)
            self.save(self.tg, i, token_grad.astype(bf16))
            done(s)
            return carry

        lax.fori_loop(0, self.blocks, one, 0)


def layer_scratch(rows, width, hidden):
    return [
        pltpu.VMEM((rows, width), bf16),
        pltpu.VMEM((rows, width), bf16),
        pltpu.VMEM((rows, width), bf16),
        pltpu.VMEM((rows, width), f32),
        pltpu.VMEM((HEADS, rows, 128), bf16),
        pltpu.VMEM((width, rows), bf16),
        pltpu.VMEM((width, rows), bf16),
        pltpu.VMEM((width, rows), bf16),
        pltpu.VMEM((width, rows), bf16),
        pltpu.VMEM((rows, width), bf16),
        pltpu.VMEM((rows, width), f32),
        pltpu.VMEM((rows, width), bf16),
        pltpu.VMEM((hidden // 512, rows, 512), bf16),
        pltpu.VMEM((hidden // 512, rows, 512), bf16),
        pltpu.VMEM((rows, 256), bf16),
        pltpu.VMEM((rows, 256), bf16),
        pltpu.VMEM((rows, 256), bf16),
        pltpu.VMEM((rows, 128), f32),
        pltpu.VMEM((rows, 128), f32),
        pltpu.VMEM((BLK, width), f32),
        pltpu.VMEM((BLK, width), f32),
    ]


class Route:
    def __init__(self, src, dst, local, send, recv, members):
        self.src, self.dst, self.send, self.recv, self.members = src, dst, send, recv, members
        self.me = lax.axis_index("dp")
        self.own = pltpu.make_async_copy(src.at[self.me], dst.at[self.me], local)

    def outgoing(self, to):
        slot = lax.rem(to - self.me + self.members, self.members)
        return pltpu.make_async_remote_copy(
            src_ref=self.src.at[to], dst_ref=self.dst.at[self.me], send_sem=self.send.at[slot],
            recv_sem=self.recv.at[slot], device_id={"dp": to}, device_id_type=MESH)

    def incoming(self, source):
        slot = lax.rem(self.me - source + self.members, self.members)
        return pltpu.make_async_remote_copy(
            src_ref=self.src.at[source], dst_ref=self.dst.at[source], send_sem=self.send.at[slot],
            recv_sem=self.recv.at[slot], device_id={"dp": source}, device_id_type=MESH)

    def beside(self):
        return self.me + 1 - 2 * lax.rem(self.me, 2)

    def pair(self, s):
        block = lax.rem(self.me // 2 + s, self.members // 2)
        return 2 * block, 2 * block + 1

    def start(self):
        for s in range(1, self.members):
            self.outgoing(lax.rem(self.me + s, self.members)).start()
        self.own.start()

    def give(self, s):
        @pl.when(s > 0)
        def _():
            for to in self.pair(s):
                self.outgoing(to).start()

        @pl.when(s == 0)
        def _():
            self.outgoing(self.beside()).start()
            self.own.start()

    def take(self, s):
        @pl.when(s > 0)
        def _():
            for source in self.pair(s):
                self.incoming(source).wait_recv()

        @pl.when(s == 0)
        def _():
            self.own.wait()
            self.incoming(self.beside()).wait_recv()

    def wait(self):
        for s in range(1, self.members):
            self.incoming(lax.rem(self.me + s, self.members)).wait_recv()
        self.own.wait()

    def wait_sent(self):
        for s in range(1, self.members):
            self.outgoing(lax.rem(self.me + s, self.members)).wait_send()


class Exchange:
    def __init__(self, grads, cs, wide_first, emit, scratch, send, recv, high):
        self.grads, self.cs, self.wide_first, self.emit, self.high = grads, cs, wide_first, emit, high
        self.from_core, self.from_one, self.from_two, self.last = scratch
        _, _, (a, b, c, e) = my_place()
        self.place = (a, b, c, e)
        across = {"fsdp": (1 - c) * 2 + e}, {"dp": a * 2 + 1 - b}

        def describe(source, target, slot, device):
            return pltpu.make_async_remote_copy(
                src_ref=source, dst_ref=target, send_sem=send.at[slot], recv_sem=recv.at[slot],
                device_id=device, device_id_type=MESH)

        stages = [[describe(grads.at[:, :, :, 1 - e, :, cs], self.from_core, 0, {"fsdp": c * 2 + 1 - e})]]
        if wide_first:
            stages.append([describe(grads.at[:, :, 1 - c, e, :, cs], self.from_one, 1, across[0])])
            stages.append([describe(grads.at[:, 1 - b, c, e, :, cs], self.from_two, 2, across[1])])
        else:
            stages.append([describe(grads.at[:, 1 - b, :, e, :, cs], self.from_one, 1, across[1])])
            stages.append([describe(grads.at[:, b, 1 - c, e, :, cs], self.from_two, 2, across[0])])
        copies = []
        for s in range(1, high):
            other = lax.rem(a + s, high)
            copies.append(describe(
                grads.at[other, b, c, e, :, cs], self.last.at[a], 2 + s, {"dp": other * 2 + b}))
        stages.append(copies)
        self.stages = stages

    def launch(self, number):
        for copy in self.stages[number]:
            copy.start()

    def start(self):
        self.launch(0)

    def step(self, number):
        a, b, c, e = self.place
        grads, cs = self.grads, self.cs
        for copy in self.stages[number]:
            copy.wait_recv()
        if number == 0:
            def one(i, carry):
                mine = grads[i, :, :, e, :, cs].astype(f32)
                grads[i, :, :, e, :, cs] = (mine + self.from_core[i].astype(f32)).astype(bf16)
                return carry
        elif number == 1 and self.wide_first:
            def one(i, carry):
                mine = grads[i, :, c, e, :, cs].astype(f32)
                grads[i, :, c, e, :, cs] = (mine + self.from_one[i].astype(f32)).astype(bf16)
                return carry
        elif number == 1:
            def one(i, carry):
                mine = grads[i, b, :, e, :, cs].astype(f32)
                grads[i, b, :, e, :, cs] = (mine + self.from_one[i].astype(f32)).astype(bf16)
                return carry
        elif number == 2:
            def one(i, carry):
                mine = grads[i, b, c, e, :, cs].astype(f32)
                grads[i, b, c, e, :, cs] = (mine + self.from_two[i].astype(f32)).astype(bf16)
                return carry
        if number < 3:
            lax.fori_loop(0, self.high, one, 0)
            self.launch(number + 1)
        else:
            total = grads[a, b, c, e, :, cs].astype(f32)
            for s in range(1, self.high):
                total = total + self.last[lax.rem(a + s, self.high)].astype(f32)
            self.emit(total)

    def wait_sent(self):
        for stage in self.stages:
            for copy in stage:
                copy.wait_send()


def exchange_scratch(high, rows, columns):
    return [pltpu.VMEM(lead + (rows, columns), bf16) for lead in ((high, 2, 2), (high, 2), (high,), (high,))]


def fill_vectors(small, vec, upb):
    devices, own, _ = small.shape
    rows = small[:, :, :128].reshape(devices * own, 128).astype(f32)
    spot = lax.broadcasted_iota(jnp.int32, rows.shape, 1)
    turn = lax.broadcasted_iota(jnp.int32, rows.shape, 0)
    mine = jnp.where(lax.rem(spot, own) == lax.rem(turn, own), rows, 0.0).astype(bf16)
    lanes = lax.broadcasted_iota(jnp.int32, (16, 128), 1)
    picks = lax.broadcasted_iota(jnp.int32, (16, 128), 0)
    choose = jnp.where(lanes - picks * own == lax.rem(lanes, own), 1.0, 0.0).astype(bf16)
    vec[...] = nt(choose, mine)[:8]
    low = lax.broadcasted_iota(jnp.int32, (1, 128), 1) < 64
    for i in range(devices // 2):
        left, right = small[2 * i, :, 128:].astype(f32), small[2 * i + 1, :, 128:].astype(f32)
        upb[:, 128 * i : 128 * i + 128] = jnp.where(low, left[0:1], right[0:1])


def at_points(index, plan):
    for point, action in plan:
        @pl.when(index == point)
        def _(action=action):
            action()


def permute(target, source, table, m):
    def one(n, carry):
        target[n] = source[table[m, n]]
        return carry

    lax.fori_loop(0, target.shape[0], one, 0)


def layer_kernel(sizes, members, others, *refs):
    came_from, goes_to, slot, length, joint, small, mix, up, down, tokens, grads = refs[:11]
    joint_out, mix_out, up_out, down_out, tail_out, layer_out, input_out = refs[11:18]
    (shard, weights, held, taken, back_0, back_1, back_2, back_3, total, extra, live, vec, upb, vsum, usum,
     wsend, wrecv, tsend, trecv, rsend, rrecv, local) = refs[18:40]
    back = (back_0, back_1, back_2, back_3)
    pools = [refs[40 + 4 * n : 44 + 4 * n] for n in range(4)]
    scratch = refs[56:]
    high = sizes[0]
    own, hidden = up.shape
    width = mix.shape[1]
    piece = tokens.shape[2]
    devices = members * others
    z = lax.axis_index("dp") // 2

    loads = [
        pltpu.make_async_copy((grads if n % 2 else tokens).at[n // 2], back[n], local.at[n]) for n in range(4)
    ]
    for load in loads:
        load.start()
    mix_at = 3 * width + SMALL
    up_at = mix_at + width
    down_at = up_at + hidden
    shard[:, : 3 * width] = joint[...]
    shard[:, 3 * width : mix_at] = small[...]
    shard[:, mix_at:up_at] = mix[...]
    shard[:, up_at:down_at] = up[...]
    shard[:, down_at:] = down[...]
    loads[0].wait()
    permute(held.at[0], back[0], came_from, 0)
    greet(members, others)

    into = [
        Route(held.at[n], taken.at[n], local.at[4 + n], tsend.at[n], trecv.at[n], members) for n in range(4)
    ]
    returns = [
        Route(held.at[n], back[n], local.at[8 + n], tsend.at[4 + n], trecv.at[4 + n], members) for n in range(4)
    ]
    results = [
        pltpu.make_async_copy(taken.at[n], (input_out if n % 2 else layer_out).at[n // 2], local.at[12 + n])
        for n in range(4)
    ]
    ranges = (
        (pl.ds(0, 1024), (0, 1, 2, 3)),
        (pl.ds(1024, mix_at - 1024), (0, 2, 1, 3)),
        (pl.ds(mix_at, width), (0, 1, 2, 3)),
        (pl.ds(up_at, hidden), (0, 1, 2, 3)),
        (pl.ds(down_at, hidden), (0, 2, 1, 3)),
    )
    gathers = [
        Gather(shard, weights, cs, order, local.at[16 + n], wsend.at[n], wrecv.at[n], sizes)
        for n, (cs, order) in enumerate(ranges)
    ]
    early, late = gathers[:2], gathers[2:]
    for gather in early:
        gather.start(0)
    into[0].start()
    for n in range(1, 4):
        loads[n].wait()
        permute(held.at[n], back[n], came_from, n // 2)
    for number in range(1, 4):
        for gather in early:
            gather.wait(number - 1)
            gather.start(number)
    vsum[...] = jnp.zeros_like(vsum)
    usum[...] = jnp.zeros_like(usum)

    def mark(m):
        places = lax.broadcasted_iota(jnp.int32, (piece, 1), 0)
        for n in range(members):
            live[n * piece : (n + 1) * piece, :] = jnp.where(
                places + slot[m, n] * piece < length[m, 0], 1.0, 0.0)

    def weight(start, size):
        return weights[:, :, :, :, :, pl.ds(start, size)].reshape(width, size)

    def columns(k):
        return pl.ds(pl.multiple_of(k * 512, 512), 512)

    def put_first(k, value):
        total[:, :, :, :, :, columns(k)] = value.astype(bf16).reshape(sizes + (own, 512))

    def put_second(k, value):
        value = value + total[:, :, :, :, :, columns(k)].reshape(width, 512).astype(f32)
        total[:, :, :, :, :, columns(k)] = value.astype(bf16).reshape(sizes + (own, 512))

    def turn(s):
        return lax.rem(z + s, high)

    def turn_last(s):
        return lax.rem(z + 1 + s, high)

    def nothing(s):
        pass

    first, second = (
        Layer(taken.at[2 * m], taken.at[2 * m + 1], live, weight, (mix_at, up_at, down_at), vec, upb,
              held.at[2 * m], held.at[2 * m + 1], put, vsum, usum, scratch)
        for m, put in enumerate((put_first, put_second))
    )

    mark(0)
    first.masks()
    for gather in early:
        gather.wait(3)
    fill_vectors(weights[:, :, :, :, :, 3 * width : mix_at].reshape(devices, own, SMALL), vec, upb)

    def arrive_tokens(s):
        @pl.when(s == high - 1)
        def _():
            for gather in late:
                gather.start(0)
            into[1].start()

        into[0].take(s)

    first.project(turn, arrive_tokens)

    def relay(gather, number):
        def action():
            gather.wait(number - 1)
            gather.start(number)
        return action

    points = ((0, 2, 4), (4, 8, 13), (8, 12, 15))
    plan = [
        (point, relay(gather, number + 1))
        for gather, when in zip(late, points) for number, point in enumerate(when)
    ]
    plan.sort(key=lambda item: item[0])
    first.attend(lambda h: at_points(h, plan))
    for gather in late:
        gather.wait(3)
    into[0].wait_sent()

    def arrive_grads(s):
        into[1].take(s)

        @pl.when(s == high - 1)
        def _():
            into[2].start()
            into[3].start()

    first.feed(turn, arrive_grads)
    returns[0].start()
    into[1].wait_sent()
    first.down_grad()
    first.up_grad()
    first.mix_grad()
    first.attend_back(nothing)
    first.joint_grad()
    first.first_back(turn, nothing)
    returns[1].start()

    def emit_to(ref):
        def emit(value):
            ref[...] = value
        return emit

    def emit_pair(value):
        up_out[...] = value[:, :hidden]
        mix_out[...] = value[:, hidden:]

    downs, ups, rest, last = (
        Exchange(source, cs, wide_first, emit, pools[n], rsend.at[n], rrecv.at[n], high)
        for n, (source, cs, wide_first, emit) in enumerate((
            (total, pl.ds(0, hidden), True, emit_to(down_out)),
            (total, pl.ds(hidden, hidden + width), False, emit_pair),
            (total, pl.ds(2 * hidden + width, 3 * width), True, emit_to(joint_out)),
            (extra, pl.ds(0, SMALL), False, emit_to(tail_out)),
        ))
    )
    mark(1)
    second.masks()
    into[2].wait()
    second.project(turn, nothing)
    second.attend(nothing)
    into[2].wait_sent()
    into[3].wait()
    second.feed(turn, nothing)
    returns[2].start()
    into[3].wait_sent()
    second.down_grad()
    downs.start()
    second.up_grad()
    second.mix_grad()
    ups.start()

    def result(n):
        def action():
            returns[n].wait()
            permute(taken.at[n], back[n], goes_to, n // 2)
            results[n].start()
        return action

    def step(exchange, number):
        return lambda: exchange.step(number)

    plan_back = [
        (0, step(downs, 0)), (1, step(ups, 0)), (3, result(0)), (6, step(downs, 1)), (8, step(ups, 1)),
        (9, result(1)), (10, step(downs, 2)), (12, step(ups, 2)), (15, step(downs, 3)),
    ]
    second.attend_back(lambda h: at_points(h, plan_back))

    def send_grads(s):
        returns[3].give(lax.rem(s + 1, high))

    second.first_back(turn_last, send_grads)
    second.joint_grad()
    rest.start()
    turned = jnp.concatenate([vsum[...], jnp.zeros((120, width), f32)], axis=0).T
    extra[:, :, :, :, :, :128] = turned.astype(bf16).reshape(sizes + (own, 128))
    for n in range(devices):
        a, b, c, e = n // (2 * others), (n // others) % 2, (n % others) // 2, n % 2
        part = usum[:, 128 * (n // 2) : 128 * (n // 2) + 128]
        extra[a, b, c, e, :, 128:] = jnp.broadcast_to(part, (own, 128)).astype(bf16)
    last.start()
    ups.step(3)
    rest.step(0)
    last.step(0)
    result(2)()
    for number in range(1, 4):
        rest.step(number)
        last.step(number)
    result(3)()
    for item in gathers + returns + [downs, ups, rest, last]:
        item.wait_sent()
    for item in results:
        item.wait()


def layer_call(tables, shards, tokens, grads, members, others):
    joint, small, mix, up, down = shards
    own, hidden = up.shape
    _, _, piece, width = tokens.shape
    rows = members * piece
    sizes = (members // 2, 2, others // 2, 2)
    high = sizes[0]
    slots = high + 1 + sizes[2]
    columns = 4 * width + 2 * hidden
    dma = pltpu.SemaphoreType.DMA
    smem = pl.BlockSpec(memory_space=pltpu.SMEM)
    pools = []
    for count in (hidden, hidden + width, 3 * width, SMALL):
        pools += exchange_scratch(high, own, count)
    shapes = [(own, 3 * width), (own, width), (own, hidden), (own, hidden), (own, SMALL)]
    blocks = pltpu.VMEM((4, members, piece, width), bf16)
    return pl.pallas_call(
        functools.partial(layer_kernel, sizes, members, others),
        out_shape=tuple(jax.ShapeDtypeStruct(shape, f32) for shape in shapes)
        + (jax.ShapeDtypeStruct(tokens.shape, bf16),) * 2,
        in_specs=[smem] * 4 + [VMEM] * 5 + [ANY] * 2,
        out_specs=(VMEM,) * 5 + (ANY,) * 2,
        scratch_shapes=[
            pltpu.VMEM((own, columns + SMALL), bf16),
            pltpu.VMEM(sizes + (own, columns + SMALL), bf16),
            blocks, blocks,
        ] + [pltpu.VMEM((members, piece, width), bf16)] * 4 + [
            pltpu.VMEM(sizes + (own, columns), bf16),
            pltpu.VMEM(sizes + (own, SMALL), bf16),
            pltpu.VMEM((rows, 1), f32),
            pltpu.VMEM((8, width), f32), pltpu.VMEM((1, hidden), f32),
            pltpu.VMEM((8, width), f32), pltpu.VMEM((1, hidden), f32),
            dma((5, slots)), dma((5, slots)), dma((8, members)), dma((8, members)),
            dma((4, high + 2)), dma((4, high + 2)), dma((21,)),
        ] + pools + layer_scratch(rows, width, hidden),
        compiler_params=pltpu.CompilerParams(
            collective_id=2, has_side_effects=True, vmem_limit_bytes=67_043_328),
        name="layer",
    )(*tables, *shards, tokens, grads)


def fused_body(
    tokens, out_grad, seq_lengths, send_to, slot_of, first_gain, first_shift, joint_weight, query_bias,
    value_bias, mix_weight, mix_bias, second_gain, second_shift, up_weight, up_bias, down_weight, down_bias,
):
    members, others = lax.axis_size("dp"), lax.axis_size("fsdp")
    micro, rows, width = tokens.shape
    own = first_gain.shape[0]
    parts = (first_gain, first_shift, query_bias, value_bias, mix_bias, second_gain, second_shift, down_bias,
             up_bias, up_bias)
    small = jnp.broadcast_to(jnp.concatenate(parts)[None], (own, SMALL))
    goes_to = send_to[:, 0]
    order = jnp.arange(members, dtype=jnp.int32)
    came_from = jnp.sum(jnp.where(goes_to[:, :, None] == order, order[None, :, None], 0), axis=1).astype(jnp.int32)
    pieces = (micro, members, rows // members, width)
    joint, mix, up, down, tail, layer_output, input_grad = layer_call(
        (came_from, goes_to, slot_of[:, 0], seq_lengths), (joint_weight, small, mix_weight, up_weight, down_weight.T),
        tokens.reshape(pieces), out_grad.reshape(pieces), members, others)
    vec_grad = [tail[:, n] for n in range(8)]
    odd = lax.rem(lax.axis_index("fsdp"), 2) == 1
    up_bias_grad = jnp.where(odd, tail[0, 192:256], tail[0, 128:192])
    return (
        layer_output.reshape(tokens.shape), input_grad.reshape(tokens.shape),
        vec_grad[0], vec_grad[1], joint, vec_grad[2], vec_grad[3], mix, vec_grad[4], vec_grad[5], vec_grad[6],
        up, up_bias_grad, down.T, vec_grad[7],
    )


def solution(mesh):
    both = ("dp", "fsdp")
    row3, row2, vector, matrix = P(None, both, None), P(None, both), P(both), P(both, None)
    turned = P(None, both)
    members, others = mesh.shape["dp"], mesh.shape["fsdp"]
    fits = members * others == 32 and others == 4
    return jax.shard_map(
        fused_body if fits else body,
        mesh=mesh,
        in_specs=(row3, row3, row2, row3, row3, vector, vector, matrix, vector, vector, matrix, vector, vector,
                  vector, matrix, vector, turned, vector),
        out_specs=(row3, row3, vector, vector, matrix, vector, vector, matrix, vector, vector, vector, matrix,
                   vector, turned, vector),
        check_vma=False,
    )
```

```python
import functools
import math

import jax
import jax.numpy as jnp
from jax import lax
from jax.experimental import pallas as pl
from jax.experimental.pallas import tpu as pltpu
from jax.sharding import PartitionSpec as P

HEADS = 8
HEAD_DIM = 64
BLK = 256

f32, bf16 = jnp.float32, jnp.bfloat16
epsilon = 1e-05
masked_score = -1e30
root_half = math.sqrt(0.5)
gauss_norm = 1.0 / math.sqrt(2.0 * math.pi)


def nn(a, b):
    return lax.dot_general(a, b, (((1,), (0,)), ((), ())), preferred_element_type=f32)


def nt(a, b):
    return lax.dot_general(a, b, (((1,), (1,)), ((), ())), preferred_element_type=f32)


def tn(a, b):
    return lax.dot_general(a, b, (((0,), (0,)), ((), ())), preferred_element_type=f32)


def normalize(rows):
    center = rows - jnp.mean(rows, axis=-1, keepdims=True)
    spread = jnp.mean(center * center, axis=-1, keepdims=True)
    factor = lax.rsqrt(spread + epsilon)
    return center * factor, factor


def norm_back(grad_norm, normed, factor):
    first_mean = jnp.mean(grad_norm, axis=-1, keepdims=True)
    second_mean = jnp.mean(grad_norm * normed, axis=-1, keepdims=True)
    return factor * (grad_norm - first_mean - normed * second_mean)


def three_parts(v):
    hi = v.astype(bf16).astype(f32)
    mid = (v - hi).astype(bf16).astype(f32)
    return hi, mid, v - hi - mid


def col_sum(v):
    return jnp.sum(v, axis=0, keepdims=True)


def micro_kernel(first, *refs):
    x_ref, g_ref, live_ref, w_ref, vec_ref, upb_ref = refs[:6]
    refs = refs[6:]
    if not first:
        prev_ref, vprev_ref, uprev_ref = refs[:3]
        refs = refs[3:]
    final_ref, tg_ref, grad_ref, vsum_ref, usum_ref = refs[:5]
    (q_ref, k_ref, v_ref, att_ref, qaug_ref, first_t, second_t, down_t, att_t, mixin_ref, mg_ref,
     dout_ref, hid_ref, pre_ref, kaug, vaug_a, vaug_b, dk_acc, dv_acc, acc_a, acc_b) = refs[5:]
    rows, width = x_ref.shape
    hidden = upb_ref.shape[1]
    blocks = rows // BLK
    pairs = width // 128
    mix_at = 3 * width
    up_at = mix_at + width
    down_at = up_at + hidden
    lane = lax.broadcasted_iota(jnp.int32, (1, 128), 1)
    low_half = lane < HEAD_DIM

    def at(i, size=BLK):
        return pl.ds(pl.multiple_of(i * size, size), size)

    if first:
        vsum_ref[...] = jnp.zeros_like(vsum_ref)
        usum_ref[...] = jnp.zeros_like(usum_ref)
    else:
        vsum_ref[...] = vprev_ref[...]
        usum_ref[...] = uprev_ref[...]

    def row(ref, n):
        return ref[n : n + 1, :]

    live_all = live_ref[...]
    mask_aug = jnp.where(
        lane == 0, (live_all - 1.0) * (-masked_score), jnp.where(lane < 4, 1.0, 0.0)
    ).astype(bf16)
    kaug[:, 128:] = mask_aug
    vaug_a[:, 128:] = jnp.ones((rows, 128), bf16)
    vaug_b[:, 128:] = jnp.ones((rows, 128), bf16)

    def project(i, carry):
        rs = at(i)
        normed, _ = normalize(x_ref[rs, :].astype(f32))
        first_in = (normed * row(vec_ref, 0) + row(vec_ref, 1)).astype(bf16)
        first_t[:, rs] = first_in.T
        query = (nn(first_in, w_ref[:, :width]) + row(vec_ref, 2)).astype(bf16)
        q_ref[rs, :] = query * jnp.array(HEAD_DIM ** (-0.5), bf16)
        k_ref[rs, :] = nn(first_in, w_ref[:, width : 2 * width]).astype(bf16)
        v_ref[rs, :] = (nn(first_in, w_ref[:, 2 * width : 3 * width]) + row(vec_ref, 3)).astype(bf16)
        return carry

    lax.fori_loop(0, blocks, project, 0)

    def attend_pair(p, carry):
        ls = at(p, 128)
        kaug[:, :128] = k_ref[:, ls]
        values = v_ref[:, ls]
        zero = jnp.zeros_like(values)
        vaug_a[:, :128] = jnp.where(low_half, values, zero)
        vaug_b[:, :128] = jnp.where(low_half, zero, values)

        def attend(i, carry):
            rs = at(i)
            query = q_ref[rs, ls]
            qzero = jnp.zeros_like(query)
            one = jnp.broadcast_to(jnp.where(lane == 0, 1.0, 0.0), (BLK, 128)).astype(bf16)
            out = None
            for half, vaug in ((0, vaug_a), (1, vaug_b)):
                mine = jnp.where(low_half if half == 0 else jnp.logical_not(low_half), query, qzero)
                scores = nt(jnp.concatenate([mine, one], axis=1), kaug[...])
                peak = jnp.max(scores, axis=-1, keepdims=True)
                chances = jnp.exp(scores - peak).astype(bf16)
                got = nn(chances, vaug[...])
                total = got[:, 128:]
                lse = peak + jnp.log(total)
                hi, mid, lo = three_parts(lse)
                qaug_ref[2 * p + half, rs, :] = jnp.where(
                    lane == 0, 1.0,
                    jnp.where(lane == 1, -hi, jnp.where(lane == 2, -mid, jnp.where(lane == 3, -lo, 0.0))),
                ).astype(bf16)
                part = got[:, :128] / total
                out = part if out is None else out + part
            att_ref[rs, ls] = out
            return carry

        return lax.fori_loop(0, blocks, attend, carry)

    lax.fori_loop(0, pairs, attend_pair, 0)

    chunk = 512
    mix_w = w_ref.at[:, mix_at:up_at]

    def feed(i, carry):
        rs = at(i)
        live = live_ref[rs, :]
        attended = att_ref[rs, :].astype(bf16)
        att_t[:, rs] = attended.T
        middle = x_ref[rs, :].astype(f32) + live * (nn(attended, mix_w[...]) + row(vec_ref, 4))
        second_norm, factor = normalize(middle)
        second_in = (second_norm * row(vec_ref, 5) + row(vec_ref, 6)).astype(bf16)
        second_t[:, rs] = second_in.T
        outer = g_ref[rs, :].astype(f32)
        down_in = (live * outer).astype(bf16)
        down_t[:, rs] = down_in.T
        vsum_ref[7:8, :] += col_sum(down_in.astype(f32))
        acc_a[...] = jnp.zeros_like(acc_a)
        acc_b[...] = jnp.zeros_like(acc_b)

        def part(c, carry):
            cs = at(c, chunk)
            up = w_ref[:, pl.ds(pl.multiple_of(up_at + c * chunk, chunk), chunk)]
            down = w_ref[:, pl.ds(pl.multiple_of(down_at + c * chunk, chunk), chunk)]
            pre = nn(second_in, up) + upb_ref[:, cs]
            phi = 0.5 * (1.0 + lax.erf(pre * root_half))
            hid = (pre * phi).astype(bf16)
            slope = phi + pre * jnp.exp(-0.5 * pre * pre) * gauss_norm
            hid_ref[rs, cs] = hid
            acc_a[...] += nt(hid, down)
            pre_grad = (nn(down_in, down) * slope).astype(bf16)
            pre_ref[rs, cs] = pre_grad
            usum_ref[:, cs] += col_sum(pre_grad.astype(f32))
            acc_b[...] += nt(pre_grad, up)
            return carry

        lax.fori_loop(0, hidden // chunk, part, 0)
        final_ref[rs, :] = (middle + live * (acc_a[...] + row(vec_ref, 7))).astype(bf16)
        second_in_grad = acc_b[...]
        vsum_ref[5:6, :] += col_sum(second_in_grad * second_norm)
        vsum_ref[6:7, :] += col_sum(second_in_grad)
        middle_grad = outer + norm_back(second_in_grad * row(vec_ref, 5), second_norm, factor)
        mg_ref[rs, :] = middle_grad
        mix_in = (live * middle_grad).astype(bf16)
        mixin_ref[rs, :] = mix_in
        vsum_ref[4:5, :] += col_sum(mix_in.astype(f32))
        dout_ref[rs, :] = nt(mix_in, mix_w[...]).astype(bf16)
        return carry

    lax.fori_loop(0, blocks, feed, 0)

    def put(value, cs):
        if not first:
            value = value + prev_ref[:, cs]
        grad_ref[:, cs] = value.astype(grad_ref.dtype)

    def wide(lhs_t, rhs_ref, base, count):
        def one(c, carry):
            put(nn(lhs_t[...], rhs_ref[:, at(c, chunk)]),
                pl.ds(pl.multiple_of(base + c * chunk, chunk), chunk))
            return carry
        lax.fori_loop(0, count, one, 0)

    wide(down_t, hid_ref, down_at, hidden // chunk)
    wide(second_t, pre_ref, up_at, hidden // chunk)
    wide(att_t, mixin_ref, mix_at, width // chunk)

    joint_grad = hid_ref

    def back_pair(p, carry):
        ls = at(p, 128)
        keys = k_ref[:, ls]
        kaug[:, :128] = keys
        vaug_a[:, :128] = v_ref[:, ls]
        vaug_a[:, 128:] = kaug[:, 128:]
        zero = jnp.zeros_like(keys)
        vaug_b[:, :128] = jnp.where(low_half, keys, zero)
        vaug_b[:, 128:] = jnp.where(low_half, zero, keys)
        dk_acc[...] = jnp.zeros_like(dk_acc)
        dv_acc[...] = jnp.zeros_like(dv_acc)

        def back(i, carry):
            rs = at(i)
            query = q_ref[rs, ls]
            grad = dout_ref[rs, ls]
            both = grad.astype(f32) * att_ref[rs, ls]
            dq = None
            for half in (0, 1):
                keep = low_half if half == 0 else jnp.logical_not(low_half)
                mine = jnp.where(keep, query, jnp.zeros_like(query))
                grads = jnp.where(keep, grad, jnp.zeros_like(grad))
                inner = jnp.sum(jnp.where(keep, both, 0.0), axis=-1, keepdims=True)
                hi, mid, lo = three_parts(inner)
                gaug = jnp.where(
                    lane == 1, -hi, jnp.where(lane == 2, -mid, jnp.where(lane == 3, -lo, 0.0))
                ).astype(bf16)
                scores = nt(kaug[...], jnp.concatenate([mine, qaug_ref[2 * p + half, rs, :]], axis=1))
                chances = jnp.exp(scores)
                centered = nt(vaug_a[...], jnp.concatenate([grads, gaug], axis=1))
                score_grad = (chances * centered).astype(bf16)
                dv_acc[...] += nn(chances.astype(bf16), grads)
                dk_acc[...] += nn(score_grad, mine)
                part = tn(score_grad, vaug_b[:, 128 * half : 128 * half + 128])
                dq = part if dq is None else dq + part
            joint_grad[rs, ls] = (dq * HEAD_DIM ** (-0.5)).astype(bf16)
            return carry

        lax.fori_loop(0, blocks, back, 0)
        joint_grad[:, pl.ds(pl.multiple_of(width + p * 128, 128), 128)] = dk_acc[...].astype(bf16)
        joint_grad[:, pl.ds(pl.multiple_of(2 * width + p * 128, 128), 128)] = dv_acc[...].astype(bf16)
        return carry

    lax.fori_loop(0, pairs, back_pair, 0)

    wide(first_t, joint_grad, 0, 3 * width // chunk)

    def back_first(i, carry):
        rs = at(i)
        grads = joint_grad[rs, : 3 * width]
        vsum_ref[2:3, :] += col_sum(grads[:, :width].astype(f32))
        vsum_ref[3:4, :] += col_sum(grads[:, 2 * width :].astype(f32))
        first_in_grad = nt(grads, w_ref[:, : 3 * width])
        normed, factor = normalize(x_ref[rs, :].astype(f32))
        vsum_ref[0:1, :] += col_sum(first_in_grad * normed)
        vsum_ref[1:2, :] += col_sum(first_in_grad)
        tg_ref[rs, :] = (
            mg_ref[rs, :] + norm_back(first_in_grad * row(vec_ref, 0), normed, factor)
        ).astype(bf16)
        return carry

    lax.fori_loop(0, blocks, back_first, 0)


def micro_call(x, g, live, weights, vec, upb, previous=None):
    rows, width = x.shape
    hidden = upb.shape[1]
    columns = weights.shape[1]
    first = previous is None
    vmem = pl.BlockSpec(memory_space=pltpu.VMEM)
    args = (x, g, live, weights, vec, upb) + (() if first else previous)
    scratch = [
        pltpu.VMEM((rows, width), bf16),
        pltpu.VMEM((rows, width), bf16),
        pltpu.VMEM((rows, width), bf16),
        pltpu.VMEM((rows, width), f32),
        pltpu.VMEM((HEADS, rows, 128), bf16),
        pltpu.VMEM((width, rows), bf16),
        pltpu.VMEM((width, rows), bf16),
        pltpu.VMEM((width, rows), bf16),
        pltpu.VMEM((width, rows), bf16),
        pltpu.VMEM((rows, width), bf16),
        pltpu.VMEM((rows, width), f32),
        pltpu.VMEM((rows, width), bf16),
        pltpu.VMEM((rows, hidden), bf16),
        pltpu.VMEM((rows, hidden), bf16),
        pltpu.VMEM((rows, 256), bf16),
        pltpu.VMEM((rows, 256), bf16),
        pltpu.VMEM((rows, 256), bf16),
        pltpu.VMEM((rows, 128), f32),
        pltpu.VMEM((rows, 128), f32),
        pltpu.VMEM((BLK, width), f32),
        pltpu.VMEM((BLK, width), f32),
    ]
    flops = 2 * rows * width * columns * 3 + 7 * 2 * rows * rows * width * 4
    return pl.pallas_call(
        functools.partial(micro_kernel, first),
        out_shape=(
            jax.ShapeDtypeStruct((rows, width), bf16),
            jax.ShapeDtypeStruct((rows, width), bf16),
            jax.ShapeDtypeStruct((width, 4 * width + 2 * hidden), f32 if first else bf16),
            jax.ShapeDtypeStruct((8, width), f32),
            jax.ShapeDtypeStruct((1, hidden), f32),
        ),
        in_specs=[vmem] * len(args),
        out_specs=(vmem,) * 5,
        scratch_shapes=scratch,
        compiler_params=pltpu.CompilerParams(vmem_limit_bytes=67_043_328),
        cost_estimate=pl.CostEstimate(flops=flops, bytes_accessed=30_000_000, transcendentals=3 * HEADS * rows * rows),
        name="micro_first" if first else "micro_second",
    )(*args)


MESH = pl.DeviceIdType.MESH


def split_axes():
    members, others = lax.axis_size("dp"), lax.axis_size("fsdp")
    return members // 2, 2, others // 2, 2


def my_place():
    d, f = lax.axis_index("dp"), lax.axis_index("fsdp")
    return d, f, (d // 2, lax.rem(d, 2), f // 2, lax.rem(f, 2))


def greet(members, others):
    d, f = lax.axis_index("dp"), lax.axis_index("fsdp")
    barrier = pltpu.get_barrier_semaphore()
    for s in range(1, members):
        pl.semaphore_signal(barrier, inc=1, device_id={"dp": lax.rem(d + s, members)}, device_id_type=MESH)
    for s in range(1, others):
        pl.semaphore_signal(barrier, inc=1, device_id={"fsdp": lax.rem(f + s, others)}, device_id_type=MESH)
    pl.semaphore_wait(barrier, members + others - 2)


class Swap:
    def __init__(self, src, dst, local, send, recv, members):
        d = lax.axis_index("dp")
        self.copies = []
        for s in range(1, members):
            to = lax.rem(d + s, members)
            self.copies.append(pltpu.make_async_remote_copy(
                src_ref=src.at[to], dst_ref=dst.at[d], send_sem=send.at[s], recv_sem=recv.at[s],
                device_id={"dp": to}, device_id_type=MESH))
        self.own = pltpu.make_async_copy(src.at[d], dst.at[d], local)

    def start(self):
        for copy in self.copies:
            copy.start()
        self.own.start()

    def wait(self):
        for copy in self.copies:
            copy.wait_recv()
        self.own.wait()

    def wait_sent(self):
        for copy in self.copies:
            copy.wait_send()


class Gather:
    def __init__(self, src, out, cs, order, local, send, recv, sizes):
        a, b, c, e = my_place()[2]
        d, f = lax.axis_index("dp"), lax.axis_index("fsdp")
        high, _, wide, _ = sizes
        every = slice(None)
        place = [a, b, c, e]
        self.own = pltpu.make_async_copy(src.at[:, cs], out.at[a, b, c, e, :, cs], local)
        self.stages = []
        done = [False] * 4
        slot = 0
        for number, axis in enumerate(order):
            copies = []
            size = (high, 2, wide, 2)[axis]
            for s in range(1, size):
                other = lax.rem(place[axis] + s, size)
                if axis == 0:
                    target = {"dp": other * 2 + b}
                elif axis == 1:
                    target = {"dp": a * 2 + other}
                elif axis == 2:
                    target = {"fsdp": other * 2 + e}
                else:
                    target = {"fsdp": c * 2 + other}
                where = tuple(every if done[k] else place[k] for k in range(4)) + (every, cs)
                source = src.at[:, cs] if number == 0 else out.at[where]
                copies.append(pltpu.make_async_remote_copy(
                    src_ref=source, dst_ref=out.at[where], send_sem=send.at[slot], recv_sem=recv.at[slot],
                    device_id=target, device_id_type=MESH))
                slot += 1
            self.stages.append(copies)
            done[axis] = True

    def start(self, number):
        if number == 0:
            self.own.start()
        for copy in self.stages[number]:
            copy.start()

    def wait(self, number):
        for copy in self.stages[number]:
            copy.wait_recv()
        if number == 0:
            self.own.wait()

    def wait_sent(self):
        for stage in self.stages:
            for copy in stage:
                copy.wait_send()


class Reduce:
    def __init__(self, grads, cs, wide_first, emit, scratch, send, recv, high):
        self.grads, self.cs, self.wide_first, self.emit, self.high = grads, cs, wide_first, emit, high
        self.from_core, self.after_core, self.from_one, self.after_one, self.from_two, self.after_two, self.last = scratch
        self.send, self.recv = send, recv
        self.sent = []

    def push(self, source, target, slot, device):
        copy = pltpu.make_async_remote_copy(
            src_ref=source, dst_ref=target, send_sem=self.send.at[slot], recv_sem=self.recv.at[slot],
            device_id=device, device_id_type=MESH)
        copy.start()
        self.sent.append(copy)
        self.copy = copy

    def start(self):
        _, _, (a, b, c, e) = my_place()
        self.push(self.grads.at[:, :, :, 1 - e, :, self.cs], self.from_core, 0, {"fsdp": c * 2 + 1 - e})

    def step(self, number):
        d, f, (a, b, c, e) = my_place()
        across = {"fsdp": (1 - c) * 2 + e}, {"dp": a * 2 + 1 - b}
        if number == 0:
            self.copy.wait_recv()

            def one(i, carry):
                mine = self.grads[i, :, :, e, :, self.cs]
                self.after_core[i] = (mine.astype(f32) + self.from_core[i].astype(f32)).astype(bf16)
                return carry

            lax.fori_loop(0, self.high, one, 0)
            if self.wide_first:
                self.push(self.after_core.at[:, :, 1 - c], self.from_one, 1, across[0])
            else:
                self.push(self.after_core.at[:, 1 - b], self.from_one, 1, across[1])
        elif number == 1:
            self.copy.wait_recv()

            def two(i, carry):
                mine = self.after_core[i, :, c] if self.wide_first else self.after_core[i, b]
                self.after_one[i] = (mine.astype(f32) + self.from_one[i].astype(f32)).astype(bf16)
                return carry

            lax.fori_loop(0, self.high, two, 0)
            if self.wide_first:
                self.push(self.after_one.at[:, 1 - b], self.from_two, 2, across[1])
            else:
                self.push(self.after_one.at[:, 1 - c], self.from_two, 2, across[0])
        elif number == 2:
            self.copy.wait_recv()

            def three(i, carry):
                mine = self.after_one[i, b] if self.wide_first else self.after_one[i, c]
                self.after_two[i] = (mine.astype(f32) + self.from_two[i].astype(f32)).astype(bf16)
                return carry

            lax.fori_loop(0, self.high, three, 0)
            self.copies = []
            for s in range(1, self.high):
                other = lax.rem(a + s, self.high)
                self.push(self.after_two.at[other], self.last.at[a], 2 + s, {"dp": other * 2 + b})
                self.copies.append(self.copy)
        else:
            for copy in self.copies:
                copy.wait_recv()
            total = self.after_two[a].astype(f32)
            for s in range(1, self.high):
                total = total + self.last[lax.rem(a + s, self.high)].astype(f32)
            self.emit(total)

    def wait_sent(self):
        for copy in self.sent:
            copy.wait_send()


def reduce_scratch(high, rows, columns):
    shapes = [(high, 2, 2), (high, 2, 2), (high, 2), (high, 2), (high,), (high,), (high,)]
    return [pltpu.VMEM(lead + (rows, columns), bf16) for lead in shapes]


def gather_kernel(sizes, members, others, ranges, shard, tokens, grads, out, tokens_out, grads_out, wsend, wrecv, tsend, trecv, local):
    greet(members, others)
    micro = tokens.shape[0]
    swaps = []
    for step in range(micro):
        for kind, (src, dst) in enumerate(((tokens, tokens_out), (grads, grads_out))):
            n = step * 2 + kind
            swaps.append(Swap(src.at[step], dst.at[step], local.at[n], tsend.at[n], trecv.at[n], members))
    gathers = [
        Gather(shard, out, cs, order, local.at[2 * micro + n], wsend.at[n], wrecv.at[n], sizes)
        for n, (cs, order) in enumerate(ranges)
    ]
    swaps[0].start()
    for gather in gathers:
        gather.start(0)
    for number in range(1, 4):
        for gather in gathers:
            gather.wait(number - 1)
            gather.start(number)
        if number == 1:
            for swap in swaps[1:]:
                swap.start()
    for gather in gathers:
        gather.wait(3)
    for swap in swaps:
        swap.wait()
    for item in swaps + gathers:
        item.wait_sent()


def scatter_kernel(high, members, others, widths, grads, extra, *refs):
    sources, refs = refs[:4], refs[4:]
    outs, refs = refs[:5], refs[5:]
    returned, refs = refs[:4], refs[4:]
    wsend, wrecv, tsend, trecv, local = refs[-5:]
    scratch = refs[:-5]
    greet(members, others)
    width, hidden = widths
    swaps = [
        Swap(src, dst, local.at[n], tsend.at[n], trecv.at[n], members)
        for n, (src, dst) in enumerate(zip(sources, returned))
    ]

    def emit_first(total):
        outs[0][...] = total[:, : 3 * width]
        outs[1][...] = total[:, 3 * width :]

    def emit_to(ref):
        def emit(total):
            ref[...] = total
        return emit

    up_at, down_at = 4 * width, 4 * width + hidden
    items = [
        Reduce(grads, pl.ds(down_at, hidden), True, emit_to(outs[3]), scratch[0:7], wsend.at[0], wrecv.at[0], high),
        Reduce(grads, pl.ds(up_at, hidden), False, emit_to(outs[2]), scratch[7:14], wsend.at[1], wrecv.at[1], high),
        Reduce(grads, pl.ds(0, up_at), True, emit_first, scratch[14:21], wsend.at[2], wrecv.at[2], high),
        Reduce(extra, pl.ds(0, 128), False, emit_to(outs[4]), scratch[21:28], wsend.at[3], wrecv.at[3], high),
    ]
    for item in items:
        item.start()
    for swap in swaps:
        swap.start()
    for number in range(4):
        for item in items:
            item.step(number)
    for swap in swaps:
        swap.wait()
    for item in items + swaps:
        item.wait_sent()


def order_kernel(scatter, table, *refs):
    count = (len(refs) - 3) // 2
    sources, targets = refs[:count], refs[count : 2 * count]
    held, in_sem, out_sem = refs[2 * count :]
    micro, members = sources[0].shape[:2]
    incoming, outgoing = [], []
    for n in range(count):
        for m in range(micro):
            for p in range(members):
                other = table[m, p]
                src, dst = (p, other) if scatter else (other, p)
                slot = (n * micro + m) * members + p
                copy = pltpu.make_async_copy(sources[n].at[m, src], held.at[slot], in_sem.at[slot])
                copy.start()
                incoming.append(copy)
                outgoing.append(pltpu.make_async_copy(held.at[slot], targets[n].at[m, dst], out_sem.at[slot]))
    for one, two in zip(incoming, outgoing):
        one.wait()
        two.start()
    for two in outgoing:
        two.wait()


ANY = pl.BlockSpec(memory_space=pl.ANY)
VMEM = pl.BlockSpec(memory_space=pltpu.VMEM)


def reorder(scatter, table, *arrays):
    micro, members, piece, width = arrays[0].shape
    slots = len(arrays) * micro * members
    return pl.pallas_call(
        functools.partial(order_kernel, scatter),
        out_shape=tuple(jax.ShapeDtypeStruct(item.shape, item.dtype) for item in arrays),
        in_specs=[pl.BlockSpec(memory_space=pltpu.SMEM)] + [ANY] * len(arrays),
        out_specs=(ANY,) * len(arrays),
        scratch_shapes=[
            pltpu.VMEM((slots, piece, width), arrays[0].dtype),
            pltpu.SemaphoreType.DMA((slots,)),
            pltpu.SemaphoreType.DMA((slots,)),
        ],
        name="order_out" if scatter else "order_in",
    )(table, *arrays)


def gather_call(shard, tokens, grads, members, others):
    rows, columns = shard.shape
    high, wide = members // 2, others // 2
    sizes = (high, 2, wide, 2)
    micro = tokens.shape[0]
    third = 2048
    ranges = (
        (pl.ds(0, third), (0, 1, 2, 3)),
        (pl.ds(third, third), (0, 2, 1, 3)),
        (pl.ds(2 * third, columns - 2 * third), (0, 1, 2, 3)),
    )
    slots = high + 1 + wide
    return pl.pallas_call(
        functools.partial(gather_kernel, sizes, members, others, ranges),
        out_shape=(
            jax.ShapeDtypeStruct(sizes + (rows, columns), shard.dtype),
            jax.ShapeDtypeStruct(tokens.shape, tokens.dtype),
            jax.ShapeDtypeStruct(grads.shape, grads.dtype),
        ),
        in_specs=[VMEM, ANY, ANY],
        out_specs=(ANY,) * 3,
        scratch_shapes=[
            pltpu.SemaphoreType.DMA((len(ranges), slots)),
            pltpu.SemaphoreType.DMA((len(ranges), slots)),
            pltpu.SemaphoreType.DMA((2 * micro, members)),
            pltpu.SemaphoreType.DMA((2 * micro, members)),
            pltpu.SemaphoreType.DMA((2 * micro + len(ranges),)),
        ],
        compiler_params=pltpu.CompilerParams(collective_id=0, has_side_effects=True),
        name="gather_in",
    )(shard, tokens, grads)


def scatter_call(grads, extra, arrays, members, others, width, hidden):
    high = members // 2
    rows = grads.shape[4]
    scratch = []
    for columns in (hidden, hidden, 4 * width, 128):
        scratch += reduce_scratch(high, rows, columns)
    shapes = [(rows, 3 * width), (rows, width), (rows, hidden), (rows, hidden), (rows, 128)]
    return pl.pallas_call(
        functools.partial(scatter_kernel, high, members, others, (width, hidden)),
        out_shape=tuple(jax.ShapeDtypeStruct(shape, f32) for shape in shapes)
        + tuple(jax.ShapeDtypeStruct(item.shape, item.dtype) for item in arrays),
        in_specs=[VMEM, VMEM] + [ANY] * 4,
        out_specs=(VMEM,) * 5 + (ANY,) * 4,
        scratch_shapes=scratch + [
            pltpu.SemaphoreType.DMA((4, high + 2)),
            pltpu.SemaphoreType.DMA((4, high + 2)),
            pltpu.SemaphoreType.DMA((4, members)),
            pltpu.SemaphoreType.DMA((4, members)),
            pltpu.SemaphoreType.DMA((4,)),
        ],
        compiler_params=pltpu.CompilerParams(
            collective_id=1, has_side_effects=True, vmem_limit_bytes=67_043_328),
        name="scatter_out",
    )(grads, extra, *arrays)


def body(
    tokens, out_grad, seq_lengths, send_to, slot_of, first_gain, first_shift, joint_weight, query_bias,
    value_bias, mix_weight, mix_bias, second_gain, second_shift, up_weight, up_bias, down_weight, down_bias,
):
    members, others = lax.axis_size("dp"), lax.axis_size("fsdp")
    devices = members * others
    micro, rows, width = tokens.shape
    piece = rows // members
    own = first_gain.shape[0]
    hidden = down_weight.shape[0]
    per = hidden // width
    vectors = (first_gain, first_shift, query_bias, value_bias, mix_bias, second_gain, second_shift, down_bias)
    small = jnp.concatenate(
        [jnp.stack(vectors, axis=1), up_bias.reshape(own, per), jnp.zeros((own, 128 - 8 - per), bf16)], axis=1)
    shard = jnp.concatenate([joint_weight, mix_weight, up_weight, down_weight.T, small], axis=1)
    table = send_to[:, 0]
    pieces = (micro, members, piece, width)
    sent = reorder(True, table, tokens.reshape(pieces), out_grad.reshape(pieces))
    gathered, routed, routed_grad = gather_call(shard, *sent, members, others)
    whole = gathered.reshape(width, shard.shape[1])
    tail = whole[:, 4 * width + 2 * hidden :].astype(f32)
    vec = tail[:, :8].T
    upb = tail[:, 8 : 8 + per].reshape(1, hidden)
    spots = slot_of[:, 0, :, None] * piece + jnp.arange(piece, dtype=jnp.int32)
    live = (spots.reshape(micro, rows) < seq_lengths).astype(f32)[:, :, None]
    previous = None
    results = []
    for step in range(micro):
        final, token_grad, *previous = micro_call(
            routed[step].reshape(rows, width), routed_grad[step].reshape(rows, width), live[step], whole, vec, upb,
            previous and tuple(previous))
        results += [final.reshape(members, piece, width), token_grad.reshape(members, piece, width)]
    total, vsum, usum = previous
    sizes = (members // 2, 2, others // 2, 2, own)
    grads = total.reshape(sizes + (total.shape[1],))
    extra = jnp.concatenate(
        [vsum.T, usum.reshape(width, per), jnp.zeros((width, 128 - 8 - per), f32)], axis=1
    ).astype(bf16).reshape(sizes + (128,))
    joint, mix, up, down, tail, *returned = scatter_call(grads, extra, results, members, others, width, hidden)
    layer_output, input_grad = reorder(
        False, table, jnp.stack([returned[0], returned[2]]), jnp.stack([returned[1], returned[3]]))
    vec_grad = [tail[:, n] for n in range(8)]
    return (
        layer_output.reshape(tokens.shape), input_grad.reshape(tokens.shape),
        vec_grad[0], vec_grad[1], joint, vec_grad[2], vec_grad[3], mix, vec_grad[4], vec_grad[5], vec_grad[6],
        up, tail[:, 8 : 8 + per].reshape(up_bias.shape), down.T, vec_grad[7],
    )


SMALL = 256


class Layer:
    def __init__(self, x, g, live, weight, offsets, vec, upb, final, tg, put, vsum, usum, scratch):
        self.x, self.g, self.live, self.weight, self.offsets = x, g, live, weight, offsets
        self.vec, self.upb, self.final, self.tg, self.put, self.vsum, self.usum = vec, upb, final, tg, put, vsum, usum
        (self.q, self.k, self.v, self.att, self.qaug, self.first_t, self.second_t, self.down_t, self.att_t, self.mixin,
         self.mg, self.dout, self.hid, self.pre, self.kaug, self.vaug_a, self.vaug_b, self.dk, self.dv, self.acc_a,
         self.acc_b) = scratch
        self.rows, self.width = self.q.shape
        self.hidden = upb.shape[1]
        self.blocks = self.rows // BLK
        self.pairs = self.width // 128
        self.lane = lax.broadcasted_iota(jnp.int32, (1, 128), 1)
        self.low = self.lane < HEAD_DIM

    def at(self, i, size=BLK):
        return pl.ds(pl.multiple_of(i * size, size), size)

    def row(self, n):
        return self.vec[n : n + 1, :]

    def load(self, ref, i):
        per = BLK // ref.shape[1]
        return ref[pl.ds(i * per, per)].reshape(BLK, self.width)

    def save(self, ref, i, value):
        per = BLK // ref.shape[1]
        ref[pl.ds(i * per, per)] = value.reshape(per, ref.shape[1], self.width)

    def masks(self):
        rows, lane = self.rows, self.lane
        self.kaug[:, 128:] = jnp.where(
            lane == 0, (self.live[...] - 1.0) * (-masked_score), jnp.where(lane < 4, 1.0, 0.0)
        ).astype(bf16)
        self.vaug_a[:, 128:] = jnp.ones((rows, 128), bf16)
        self.vaug_b[:, 128:] = jnp.ones((rows, 128), bf16)

    def project(self, turn, arrive):
        width = self.width

        def one(s, carry):
            arrive(s)
            i = turn(s)
            rs = self.at(i)
            normed, _ = normalize(self.load(self.x, i).astype(f32))
            first_in = (normed * self.row(0) + self.row(1)).astype(bf16)
            self.first_t[:, rs] = first_in.T
            query = (nn(first_in, self.weight(0, width)) + self.row(2)).astype(bf16)
            self.q[rs, :] = query * jnp.array(HEAD_DIM ** (-0.5), bf16)
            self.k[rs, :] = nn(first_in, self.weight(width, width)).astype(bf16)
            self.v[rs, :] = (nn(first_in, self.weight(2 * width, width)) + self.row(3)).astype(bf16)
            return carry

        lax.fori_loop(0, self.blocks, one, 0)

    def attend(self, hook):
        lane, low = self.lane, self.low

        def pair(p, carry):
            ls = self.at(p, 128)
            self.kaug[:, :128] = self.k[:, ls]
            values = self.v[:, ls]
            zero = jnp.zeros_like(values)
            self.vaug_a[:, :128] = jnp.where(low, values, zero)
            self.vaug_b[:, :128] = jnp.where(low, zero, values)

            def one(i, carry):
                rs = self.at(i)
                query = self.q[rs, ls]
                qzero = jnp.zeros_like(query)
                lead = jnp.broadcast_to(jnp.where(lane == 0, 1.0, 0.0), (BLK, 128)).astype(bf16)
                out = None
                for half, vaug in ((0, self.vaug_a), (1, self.vaug_b)):
                    mine = jnp.where(low if half == 0 else jnp.logical_not(low), query, qzero)
                    scores = nt(jnp.concatenate([mine, lead], axis=1), self.kaug[...])
                    peak = jnp.max(scores, axis=-1, keepdims=True)
                    chances = jnp.exp(scores - peak).astype(bf16)
                    got = nn(chances, vaug[...])
                    total = got[:, 128:]
                    hi, mid, lo = three_parts(peak + jnp.log(total))
                    self.qaug[2 * p + half, rs, :] = jnp.where(
                        lane == 0, 1.0,
                        jnp.where(lane == 1, -hi, jnp.where(lane == 2, -mid, jnp.where(lane == 3, -lo, 0.0))),
                    ).astype(bf16)
                    part = got[:, :128] / total
                    out = part if out is None else out + part
                self.att[rs, ls] = out
                hook(p * self.blocks + i)
                return carry

            return lax.fori_loop(0, self.blocks, one, carry)

        lax.fori_loop(0, self.pairs, pair, 0)

    def feed(self, turn, arrive, ready):
        chunk = 512
        mix_at, up_at, down_at = self.offsets

        def one(s, carry):
            arrive(s)
            i = turn(s)
            rs = self.at(i)
            live = self.live[rs, :]
            attended = self.att[rs, :].astype(bf16)
            self.att_t[:, rs] = attended.T
            mix_w = self.weight(mix_at, self.width)
            middle = self.load(self.x, i).astype(f32) + live * (nn(attended, mix_w) + self.row(4))
            second_norm, factor = normalize(middle)
            second_in = (second_norm * self.row(5) + self.row(6)).astype(bf16)
            self.second_t[:, rs] = second_in.T
            outer = self.load(self.g, i).astype(f32)
            down_in = (live * outer).astype(bf16)
            self.down_t[:, rs] = down_in.T
            self.vsum[7:8, :] += col_sum(down_in.astype(f32))
            self.acc_a[...] = jnp.zeros_like(self.acc_a)
            self.acc_b[...] = jnp.zeros_like(self.acc_b)

            def part(c, carry):
                ready(s, c)
                cs = self.at(c, chunk)
                up = self.weight(pl.multiple_of(up_at + c * chunk, 128), chunk)
                down = self.weight(pl.multiple_of(down_at + c * chunk, 128), chunk)
                pre = nn(second_in, up) + self.upb[:, cs]
                phi = 0.5 * (1.0 + lax.erf(pre * root_half))
                hid = (pre * phi).astype(bf16)
                slope = phi + pre * jnp.exp(-0.5 * pre * pre) * gauss_norm
                self.hid[c, rs, :] = hid
                self.acc_a[...] += nt(hid, down)
                pre_grad = (nn(down_in, down) * slope).astype(bf16)
                self.pre[c, rs, :] = pre_grad
                self.usum[:, cs] += col_sum(pre_grad.astype(f32))
                self.acc_b[...] += nt(pre_grad, up)
                return carry

            lax.fori_loop(0, self.hidden // chunk, part, 0)
            self.save(self.final, i, (middle + live * (self.acc_a[...] + self.row(7))).astype(bf16))
            second_in_grad = self.acc_b[...]
            self.vsum[5:6, :] += col_sum(second_in_grad * second_norm)
            self.vsum[6:7, :] += col_sum(second_in_grad)
            middle_grad = outer + norm_back(second_in_grad * self.row(5), second_norm, factor)
            self.mg[rs, :] = middle_grad
            mix_in = (live * middle_grad).astype(bf16)
            self.mixin[rs, :] = mix_in
            self.vsum[4:5, :] += col_sum(mix_in.astype(f32))
            self.dout[rs, :] = nt(mix_in, mix_w).astype(bf16)
            return carry

        lax.fori_loop(0, self.blocks, one, 0)

    def wide(self, lhs_t, rhs, base, count):
        def one(c, carry):
            self.put(base + c, nn(lhs_t[...], rhs[c]))
            return carry

        lax.fori_loop(0, count, one, 0)

    def down_grad(self):
        self.wide(self.down_t, self.hid, 0, self.hidden // 512)

    def up_grad(self):
        self.wide(self.second_t, self.pre, self.hidden // 512, self.hidden // 512)

    def mix_grad(self):
        self.put(2 * self.hidden // 512, nn(self.att_t[...], self.mixin[...]))

    def joint_grad(self):
        self.wide(self.first_t, self.hid, (2 * self.hidden + self.width) // 512, 3 * self.width // 512)

    def attend_back(self, hook):
        lane, low = self.lane, self.low
        joint = self.hid

        def pair(p, carry):
            ls = self.at(p, 128)
            keys = self.k[:, ls]
            self.kaug[:, :128] = keys
            self.vaug_a[:, :128] = self.v[:, ls]
            self.vaug_a[:, 128:] = self.kaug[:, 128:]
            zero = jnp.zeros_like(keys)
            self.vaug_b[:, :128] = jnp.where(low, keys, zero)
            self.vaug_b[:, 128:] = jnp.where(low, zero, keys)
            self.dk[...] = jnp.zeros_like(self.dk)
            self.dv[...] = jnp.zeros_like(self.dv)

            def one(i, carry):
                rs = self.at(i)
                query = self.q[rs, ls]
                grad = self.dout[rs, ls]
                both = grad.astype(f32) * self.att[rs, ls]
                dq = None
                for half in (0, 1):
                    keep = low if half == 0 else jnp.logical_not(low)
                    mine = jnp.where(keep, query, jnp.zeros_like(query))
                    grads = jnp.where(keep, grad, jnp.zeros_like(grad))
                    hi, mid, lo = three_parts(jnp.sum(jnp.where(keep, both, 0.0), axis=-1, keepdims=True))
                    gaug = jnp.where(
                        lane == 1, -hi, jnp.where(lane == 2, -mid, jnp.where(lane == 3, -lo, 0.0))
                    ).astype(bf16)
                    scores = nt(self.kaug[...], jnp.concatenate([mine, self.qaug[2 * p + half, rs, :]], axis=1))
                    chances = jnp.exp(scores)
                    centered = nt(self.vaug_a[...], jnp.concatenate([grads, gaug], axis=1))
                    score_grad = (chances * centered).astype(bf16)
                    self.dv[...] += nn(chances.astype(bf16), grads)
                    self.dk[...] += nn(score_grad, mine)
                    part = tn(score_grad, self.vaug_b[:, 128 * half : 128 * half + 128])
                    dq = part if dq is None else dq + part
                joint[0, rs, ls] = (dq * HEAD_DIM ** (-0.5)).astype(bf16)
                hook(p * self.blocks + i)
                return carry

            lax.fori_loop(0, self.blocks, one, 0)
            joint[1, :, ls] = self.dk[...].astype(bf16)
            joint[2, :, ls] = self.dv[...].astype(bf16)
            return carry

        lax.fori_loop(0, self.pairs, pair, 0)

    def first_back(self, turn, done):
        width = self.width

        def one(s, carry):
            i = turn(s)
            rs = self.at(i)
            grads = jnp.concatenate([self.hid[0, rs, :], self.hid[1, rs, :], self.hid[2, rs, :]], axis=1)
            self.vsum[2:3, :] += col_sum(grads[:, :width].astype(f32))
            self.vsum[3:4, :] += col_sum(grads[:, 2 * width :].astype(f32))
            first_in_grad = nt(grads, self.weight(0, 3 * width))
            normed, factor = normalize(self.load(self.x, i).astype(f32))
            self.vsum[0:1, :] += col_sum(first_in_grad * normed)
            self.vsum[1:2, :] += col_sum(first_in_grad)
            token_grad = self.mg[rs, :] + norm_back(first_in_grad * self.row(0), normed, factor)
            self.save(self.tg, i, token_grad.astype(bf16))
            done(s)
            return carry

        lax.fori_loop(0, self.blocks, one, 0)


def layer_scratch(rows, width, hidden):
    return [
        pltpu.VMEM((rows, width), bf16),
        pltpu.VMEM((rows, width), bf16),
        pltpu.VMEM((rows, width), bf16),
        pltpu.VMEM((rows, width), f32),
        pltpu.VMEM((HEADS, rows, 128), bf16),
        pltpu.VMEM((width, rows), bf16),
        pltpu.VMEM((width, rows), bf16),
        pltpu.VMEM((width, rows), bf16),
        pltpu.VMEM((width, rows), bf16),
        pltpu.VMEM((rows, width), bf16),
        pltpu.VMEM((rows, width), f32),
        pltpu.VMEM((rows, width), bf16),
        pltpu.VMEM((hidden // 512, rows, 512), bf16),
        pltpu.VMEM((hidden // 512, rows, 512), bf16),
        pltpu.VMEM((rows, 256), bf16),
        pltpu.VMEM((rows, 256), bf16),
        pltpu.VMEM((rows, 256), bf16),
        pltpu.VMEM((rows, 128), f32),
        pltpu.VMEM((rows, 128), f32),
        pltpu.VMEM((BLK, width), f32),
        pltpu.VMEM((BLK, width), f32),
    ]


class Route:
    def __init__(self, src, dst, local, send, recv, members):
        self.src, self.dst, self.send, self.recv, self.members = src, dst, send, recv, members
        self.me = lax.axis_index("dp")
        self.own = pltpu.make_async_copy(src.at[self.me], dst.at[self.me], local)

    def outgoing(self, to):
        slot = lax.rem(to - self.me + self.members, self.members)
        return pltpu.make_async_remote_copy(
            src_ref=self.src.at[to], dst_ref=self.dst.at[self.me], send_sem=self.send.at[slot],
            recv_sem=self.recv.at[slot], device_id={"dp": to}, device_id_type=MESH)

    def incoming(self, source):
        slot = lax.rem(self.me - source + self.members, self.members)
        return pltpu.make_async_remote_copy(
            src_ref=self.src.at[source], dst_ref=self.dst.at[source], send_sem=self.send.at[slot],
            recv_sem=self.recv.at[slot], device_id={"dp": source}, device_id_type=MESH)

    def beside(self):
        return self.me + 1 - 2 * lax.rem(self.me, 2)

    def pair(self, s):
        block = lax.rem(self.me // 2 + s, self.members // 2)
        return 2 * block, 2 * block + 1

    def start(self):
        self.start_direct()
        self.start_others()

    def start_direct(self):
        for s in range(1, self.members // 2):
            self.outgoing(lax.rem(self.me + 2 * s, self.members)).start()
        self.outgoing(self.beside()).start()
        self.own.start()

    def start_others(self):
        for s in range(1, self.members // 2):
            self.outgoing(lax.rem(self.beside() + 2 * s, self.members)).start()

    def give(self, s):
        @pl.when(s > 0)
        def _():
            self.outgoing(lax.rem(self.me + 2 * s, self.members)).start()

        @pl.when(s == 0)
        def _():
            self.outgoing(self.beside()).start()
            self.own.start()

    def take(self, s):
        @pl.when(s > 0)
        def _():
            for source in self.pair(s):
                self.incoming(source).wait_recv()

        @pl.when(s == 0)
        def _():
            self.own.wait()
            self.incoming(self.beside()).wait_recv()

    def wait(self):
        for s in range(1, self.members):
            self.incoming(lax.rem(self.me + s, self.members)).wait_recv()
        self.own.wait()

    def wait_sent(self):
        for s in range(1, self.members):
            self.outgoing(lax.rem(self.me + s, self.members)).wait_send()


class Exchange:
    def __init__(self, grads, cs, wide_first, emit, scratch, send, recv, high):
        self.grads, self.cs, self.wide_first, self.emit, self.high = grads, cs, wide_first, emit, high
        self.from_core, self.from_one, self.from_two, self.last = scratch
        _, _, (a, b, c, e) = my_place()
        self.place = (a, b, c, e)
        across = {"fsdp": (1 - c) * 2 + e}, {"dp": a * 2 + 1 - b}

        def describe(source, target, slot, device):
            return pltpu.make_async_remote_copy(
                src_ref=source, dst_ref=target, send_sem=send.at[slot], recv_sem=recv.at[slot],
                device_id=device, device_id_type=MESH)

        stages = [[describe(grads.at[:, :, :, 1 - e, :, cs], self.from_core, 0, {"fsdp": c * 2 + 1 - e})]]
        if wide_first:
            stages.append([describe(grads.at[:, :, 1 - c, e, :, cs], self.from_one, 1, across[0])])
            stages.append([describe(grads.at[:, 1 - b, c, e, :, cs], self.from_two, 2, across[1])])
        else:
            stages.append([describe(grads.at[:, 1 - b, :, e, :, cs], self.from_one, 1, across[1])])
            stages.append([describe(grads.at[:, b, 1 - c, e, :, cs], self.from_two, 2, across[0])])
        copies = []
        for s in range(1, high):
            other = lax.rem(a + s, high)
            copies.append(describe(
                grads.at[other, b, c, e, :, cs], self.last.at[a], 2 + s, {"dp": other * 2 + b}))
        stages.append(copies)
        self.stages = stages

    def launch(self, number):
        for copy in self.stages[number]:
            copy.start()

    def start(self):
        self.launch(0)

    def step(self, number):
        a, b, c, e = self.place
        grads, cs = self.grads, self.cs
        for copy in self.stages[number]:
            copy.wait_recv()
        if number == 0:
            def one(i, carry):
                mine = grads[i, :, :, e, :, cs].astype(f32)
                grads[i, :, :, e, :, cs] = (mine + self.from_core[i].astype(f32)).astype(bf16)
                return carry
        elif number == 1 and self.wide_first:
            def one(i, carry):
                mine = grads[i, :, c, e, :, cs].astype(f32)
                grads[i, :, c, e, :, cs] = (mine + self.from_one[i].astype(f32)).astype(bf16)
                return carry
        elif number == 1:
            def one(i, carry):
                mine = grads[i, b, :, e, :, cs].astype(f32)
                grads[i, b, :, e, :, cs] = (mine + self.from_one[i].astype(f32)).astype(bf16)
                return carry
        elif number == 2:
            def one(i, carry):
                mine = grads[i, b, c, e, :, cs].astype(f32)
                grads[i, b, c, e, :, cs] = (mine + self.from_two[i].astype(f32)).astype(bf16)
                return carry
        if number < 3:
            lax.fori_loop(0, self.high, one, 0)
            self.launch(number + 1)
        else:
            total = grads[a, b, c, e, :, cs].astype(f32)
            for s in range(1, self.high):
                total = total + self.last[lax.rem(a + s, self.high)].astype(f32)
            self.emit(total)

    def wait_sent(self):
        for stage in self.stages:
            for copy in stage:
                copy.wait_send()


def exchange_scratch(high, rows, columns):
    return [pltpu.VMEM(lead + (rows, columns), bf16) for lead in ((high, 2, 2), (high, 2), (high,), (high,))]


def fill_vectors(small, vec, upb):
    devices, own, _ = small.shape
    rows = small[:, :, :128].reshape(devices * own, 128).astype(f32)
    spot = lax.broadcasted_iota(jnp.int32, rows.shape, 1)
    turn = lax.broadcasted_iota(jnp.int32, rows.shape, 0)
    mine = jnp.where(lax.rem(spot, own) == lax.rem(turn, own), rows, 0.0).astype(bf16)
    lanes = lax.broadcasted_iota(jnp.int32, (16, 128), 1)
    picks = lax.broadcasted_iota(jnp.int32, (16, 128), 0)
    choose = jnp.where(lanes - picks * own == lax.rem(lanes, own), 1.0, 0.0).astype(bf16)
    vec[...] = nt(choose, mine)[:8]
    low = lax.broadcasted_iota(jnp.int32, (1, 128), 1) < 64
    for i in range(devices // 2):
        left, right = small[2 * i, :, 128:].astype(f32), small[2 * i + 1, :, 128:].astype(f32)
        upb[:, 128 * i : 128 * i + 128] = jnp.where(low, left[0:1], right[0:1])


def at_points(index, plan):
    for point, action in plan:
        @pl.when(index == point)
        def _(action=action):
            action()


def permute(target, source, table, m, inverse=False):
    count = target.shape[0]

    def one(n, carry):
        if inverse:
            spot = jnp.int32(0)
            for k in range(1, count):
                spot = jnp.where(table[m, k] == n, k, spot)
        else:
            spot = table[m, n]
        target[n] = source[spot]
        return carry

    lax.fori_loop(0, count, one, 0)


def layer_kernel(sizes, members, others, *refs):
    goes_to, slot, length, joint, mix, up, down, *vectors, tokens, grads = refs[:18]
    joint_out, mix_out, up_out, down_out, tail_out, bias_out, layer_out, input_out = refs[18:26]
    (shard, weights, held, taken, back_0, back_1, back_2, back_3, total, extra, live, vec, upb, vsum, usum,
     wsend, wrecv, tsend, trecv, rsend, rrecv, local) = refs[26:48]
    back = (back_0, back_1, back_2, back_3)
    pools = [refs[48 + 4 * n : 52 + 4 * n] for n in range(4)]
    scratch = refs[64:]
    high = sizes[0]
    own, hidden = up.shape
    width = mix.shape[1]
    piece = tokens.shape[2]
    devices = members * others
    z = lax.axis_index("dp") // 2

    loads = [
        pltpu.make_async_copy((grads if n % 2 else tokens).at[n // 2], back[n], local.at[n]) for n in range(4)
    ]
    for load in loads:
        load.start()
    mix_at = 3 * width + SMALL
    up_at = mix_at + width
    down_at = up_at + hidden
    shard[:, : 3 * width] = joint[...]
    spread = [jnp.broadcast_to(vector[...].astype(f32), (own, vector.shape[1])) for vector in vectors]
    shard[:, 3 * width : mix_at] = jnp.concatenate(spread + spread[-1:], axis=1).astype(bf16)
    shard[:, mix_at:up_at] = mix[...]
    shard[:, up_at:down_at] = up[...]
    shard[:, down_at:] = down[...]
    loads[0].wait()
    permute(held.at[0], back[0], goes_to, 0, inverse=True)
    greet(members, others)

    into = [
        Route(held.at[n], taken.at[n], local.at[4 + n], tsend.at[n], trecv.at[n], members) for n in range(4)
    ]
    returns = [
        Route(held.at[n], back[n], local.at[8 + n], tsend.at[4 + n], trecv.at[4 + n], members) for n in range(4)
    ]
    results = [
        pltpu.make_async_copy(taken.at[n], (input_out if n % 2 else layer_out).at[n // 2], local.at[12 + n])
        for n in range(4)
    ]
    ranges = (
        (pl.ds(0, 1024), (0, 1, 2, 3)),
        (pl.ds(1024, mix_at - 1024), (0, 2, 1, 3)),
        (pl.ds(mix_at, width), (0, 1, 2, 3)),
        (pl.ds(up_at, hidden // 2), (0, 1, 2, 3)),
        (pl.ds(down_at, hidden // 2), (0, 2, 1, 3)),
        (pl.ds(up_at + hidden // 2, hidden // 2), (0, 1, 2, 3)),
        (pl.ds(down_at + hidden // 2, hidden // 2), (0, 2, 1, 3)),
    )
    gathers = [
        Gather(shard, weights, cs, order, local.at[16 + n], wsend.at[n], wrecv.at[n], sizes)
        for n, (cs, order) in enumerate(ranges)
    ]
    early, late = gathers[:2], gathers[2:]
    for gather in early:
        gather.start(0)
    into[0].start_direct()
    for n in range(1, 4):
        loads[n].wait()
        permute(held.at[n], back[n], goes_to, n // 2, inverse=True)
    for number in range(1, 4):
        for gather in early:
            gather.wait(number - 1)
            gather.start(number)
        if number == 2:
            into[0].start_others()
    vsum[...] = jnp.zeros_like(vsum)
    usum[...] = jnp.zeros_like(usum)

    def mark(m):
        places = lax.broadcasted_iota(jnp.int32, (piece, 1), 0)
        for n in range(members):
            live[n * piece : (n + 1) * piece, :] = jnp.where(
                places + slot[m, n] * piece < length[0, m], 1.0, 0.0)

    def weight(start, size):
        return weights[:, :, :, :, :, pl.ds(start, size)].reshape(width, size)

    def columns(k):
        return pl.ds(pl.multiple_of(k * 512, 512), 512)

    def put_first(k, value):
        total[:, :, :, :, :, columns(k)] = value.astype(bf16).reshape(sizes + (own, 512))

    def put_second(k, value):
        value = value + total[:, :, :, :, :, columns(k)].reshape(width, 512).astype(f32)
        total[:, :, :, :, :, columns(k)] = value.astype(bf16).reshape(sizes + (own, 512))

    def turn(s):
        return lax.rem(z + s, high)

    def turn_last(s):
        return lax.rem(z + 1 + s, high)

    def nothing(s):
        pass

    first, second = (
        Layer(taken.at[2 * m], taken.at[2 * m + 1], live, weight, (mix_at, up_at, down_at), vec, upb,
              held.at[2 * m], held.at[2 * m + 1], put, vsum, usum, scratch)
        for m, put in enumerate((put_first, put_second))
    )

    mark(0)
    first.masks()
    for gather in early:
        gather.wait(3)
    fill_vectors(weights[:, :, :, :, :, 3 * width : mix_at].reshape(devices, own, SMALL), vec, upb)

    def arrive_tokens(s):
        @pl.when(s == high - 1)
        def _():
            for gather in late:
                gather.start(0)
            into[1].start_direct()

        into[0].take(s)

    first.project(turn, arrive_tokens)

    def relay(gather, number):
        def action():
            gather.wait(number - 1)
            gather.start(number)
        return action

    mixed, up_0, down_0, up_1, down_1 = late
    plan = [
        (0, relay(mixed, 1)), (1, relay(up_0, 1)), (2, relay(mixed, 2)), (3, relay(down_0, 1)), (4, relay(up_0, 2)),
        (5, relay(mixed, 3)), (6, relay(up_1, 1)), (6, relay(down_0, 2)), (8, relay(down_1, 1)), (11, relay(up_1, 2)),
        (12, relay(up_0, 3)), (13, relay(down_1, 2)), (13, into[1].start_others), (14, relay(down_0, 3)),
    ]
    first.attend(lambda h: at_points(h, plan))
    for gather in late[:3]:
        gather.wait(3)
    into[0].wait_sent()

    def ready(s, c):
        @pl.when((s == 0) & (c == 1))
        def _():
            relay(up_1, 3)()
            relay(down_1, 3)()

        @pl.when((s == 0) & (c == 2))
        def _():
            up_1.wait(3)
            down_1.wait(3)

    def arrive_grads(s):
        into[1].take(s)

        @pl.when(s == high - 1)
        def _():
            into[2].start()
            into[3].start()

    first.feed(turn, arrive_grads, ready)
    returns[0].start()
    into[1].wait_sent()
    first.down_grad()
    first.up_grad()
    first.mix_grad()
    first.attend_back(nothing)
    first.joint_grad()
    first.first_back(turn, nothing)
    returns[1].start()

    def emit_to(ref):
        def emit(value):
            ref[...] = value
        return emit

    def emit_tail(value):
        tail_out[...] = value[:, :128].T[:8]
        odd = lax.rem(lax.axis_index("fsdp"), 2) == 1
        bias_out[...] = jnp.where(odd, value[:1, 192:256], value[:1, 128:192])

    def emit_pair(value):
        up_out[...] = value[:, :hidden]
        mix_out[...] = value[:, hidden:]

    downs, ups, rest, last = (
        Exchange(source, cs, wide_first, emit, pools[n], rsend.at[n], rrecv.at[n], high)
        for n, (source, cs, wide_first, emit) in enumerate((
            (total, pl.ds(0, hidden), True, emit_to(down_out)),
            (total, pl.ds(hidden, hidden + width), False, emit_pair),
            (total, pl.ds(2 * hidden + width, 3 * width), False, emit_to(joint_out)),
            (extra, pl.ds(0, SMALL), False, emit_tail),
        ))
    )
    mark(1)
    second.masks()
    into[2].wait()
    second.project(turn, nothing)
    second.attend(nothing)
    into[2].wait_sent()
    into[3].wait()
    second.feed(turn, nothing, lambda s, c: None)
    returns[2].start()
    into[3].wait_sent()
    second.down_grad()
    downs.start()
    second.up_grad()
    second.mix_grad()
    ups.start()

    def result(n):
        def action():
            returns[n].wait()
            permute(taken.at[n], back[n], goes_to, n // 2)
            results[n].start()
        return action

    def step(exchange, number):
        return lambda: exchange.step(number)

    plan_back = [
        (0, step(downs, 0)), (1, step(ups, 0)), (3, result(0)), (6, step(downs, 1)), (8, step(ups, 1)),
        (9, result(1)), (10, step(downs, 2)), (12, step(ups, 2)), (15, step(downs, 3)),
    ]
    second.attend_back(lambda h: at_points(h, plan_back))

    def send_grads(s):
        returns[3].give(lax.rem(s + 1, high))

    second.first_back(turn_last, send_grads)
    second.joint_grad()
    rest.start()
    turned = jnp.concatenate([vsum[...], jnp.zeros((120, width), f32)], axis=0).T
    extra[:, :, :, :, :, :128] = turned.astype(bf16).reshape(sizes + (own, 128))
    for n in range(devices):
        a, b, c, e = n // (2 * others), (n // others) % 2, (n % others) // 2, n % 2
        part = usum[:, 128 * (n // 2) : 128 * (n // 2) + 128]
        extra[a, b, c, e, :, 128:] = jnp.broadcast_to(part, (own, 128)).astype(bf16)
    last.start()
    rest.step(0)
    last.step(0)
    returns[3].start_others()
    ups.step(3)
    result(2)()
    for number in range(1, 4):
        rest.step(number)
        last.step(number)
    result(3)()
    for item in gathers + returns + [downs, ups, rest, last]:
        item.wait_sent()
    for item in results:
        item.wait()


def layer_call(tables, shards, tokens, grads, members, others):
    joint, mix, up, down, *vectors = shards
    own, hidden = up.shape
    _, _, piece, width = tokens.shape
    rows = members * piece
    sizes = (members // 2, 2, others // 2, 2)
    high = sizes[0]
    slots = high + 1 + sizes[2]
    columns = 4 * width + 2 * hidden
    dma = pltpu.SemaphoreType.DMA
    smem = pl.BlockSpec(memory_space=pltpu.SMEM)
    pools = []
    for count in (hidden, hidden + width, 3 * width, SMALL):
        pools += exchange_scratch(high, own, count)
    shapes = [(own, 3 * width), (own, width), (own, hidden), (own, hidden), (8, own), (1, 2 * SMALL // 8)]
    blocks = pltpu.VMEM((4, members, piece, width), bf16)
    return pl.pallas_call(
        functools.partial(layer_kernel, sizes, members, others),
        out_shape=tuple(jax.ShapeDtypeStruct(shape, f32) for shape in shapes)
        + (jax.ShapeDtypeStruct(tokens.shape, bf16),) * 2,
        in_specs=[smem] * 3 + [VMEM] * (4 + len(vectors)) + [ANY] * 2,
        out_specs=(VMEM,) * 6 + (ANY,) * 2,
        scratch_shapes=[
            pltpu.VMEM((own, columns + SMALL), bf16),
            pltpu.VMEM(sizes + (own, columns + SMALL), bf16),
            blocks, blocks,
        ] + [pltpu.VMEM((members, piece, width), bf16)] * 4 + [
            pltpu.VMEM(sizes + (own, columns), bf16),
            pltpu.VMEM(sizes + (own, SMALL), bf16),
            pltpu.VMEM((rows, 1), f32),
            pltpu.VMEM((8, width), f32), pltpu.VMEM((1, hidden), f32),
            pltpu.VMEM((8, width), f32), pltpu.VMEM((1, hidden), f32),
            dma((7, slots)), dma((7, slots)), dma((8, members)), dma((8, members)),
            dma((4, high + 2)), dma((4, high + 2)), dma((23,)),
        ] + pools + layer_scratch(rows, width, hidden),
        compiler_params=pltpu.CompilerParams(
            collective_id=2, has_side_effects=True, vmem_limit_bytes=67_043_328),
        name="layer",
    )(*tables, *shards, tokens, grads)


def fused_body(
    tokens, out_grad, seq_lengths, send_to, slot_of, first_gain, first_shift, joint_weight, query_bias,
    value_bias, mix_weight, mix_bias, second_gain, second_shift, up_weight, up_bias, down_weight, down_bias,
):
    members, others = lax.axis_size("dp"), lax.axis_size("fsdp")
    micro, rows, width = tokens.shape
    vectors = (first_gain, first_shift, query_bias, value_bias, mix_bias, second_gain, second_shift, down_bias, up_bias)
    pieces = (micro, members, rows // members, width)
    joint, mix, up, down, tail, bias, layer_output, input_grad = layer_call(
        (send_to[:, 0], slot_of[:, 0], seq_lengths.reshape(1, micro)),
        (joint_weight, mix_weight, up_weight, down_weight.T) + tuple(vector[None] for vector in vectors),
        tokens.reshape(pieces), out_grad.reshape(pieces), members, others)
    vec_grad = [tail[n] for n in range(8)]
    return (
        layer_output.reshape(tokens.shape), input_grad.reshape(tokens.shape),
        vec_grad[0], vec_grad[1], joint, vec_grad[2], vec_grad[3], mix, vec_grad[4], vec_grad[5], vec_grad[6],
        up, bias[0], down.T, vec_grad[7],
    )


def solution(mesh):
    both = ("dp", "fsdp")
    row3, row2, vector, matrix = P(None, both, None), P(None, both), P(both), P(both, None)
    turned = P(None, both)
    members, others = mesh.shape["dp"], mesh.shape["fsdp"]
    fits = members * others == 32 and others == 4
    return jax.shard_map(
        fused_body if fits else body,
        mesh=mesh,
        in_specs=(row3, row3, row2, row3, row3, vector, vector, matrix, vector, vector, matrix, vector, vector,
                  vector, matrix, vector, turned, vector),
        out_specs=(row3, row3, vector, vector, matrix, vector, vector, matrix, vector, vector, vector, matrix,
                   vector, turned, vector),
        check_vma=False,
    )
```

```python
import functools
import math

import jax
import jax.numpy as jnp
from jax import lax
from jax.experimental import pallas as pl
from jax.experimental.pallas import tpu as pltpu
from jax.sharding import PartitionSpec as P

HEADS = 8
HEAD_DIM = 64
BLK = 256

f32, bf16 = jnp.float32, jnp.bfloat16
epsilon = 1e-05
masked_score = -1e30
root_half = math.sqrt(0.5)
gauss_norm = 1.0 / math.sqrt(2.0 * math.pi)


def nn(a, b):
    return lax.dot_general(a, b, (((1,), (0,)), ((), ())), preferred_element_type=f32)


def nt(a, b):
    return lax.dot_general(a, b, (((1,), (1,)), ((), ())), preferred_element_type=f32)


def tn(a, b):
    return lax.dot_general(a, b, (((0,), (0,)), ((), ())), preferred_element_type=f32)


def normalize(rows):
    center = rows - jnp.mean(rows, axis=-1, keepdims=True)
    spread = jnp.mean(center * center, axis=-1, keepdims=True)
    factor = lax.rsqrt(spread + epsilon)
    return center * factor, factor


def norm_back(grad_norm, normed, factor):
    first_mean = jnp.mean(grad_norm, axis=-1, keepdims=True)
    second_mean = jnp.mean(grad_norm * normed, axis=-1, keepdims=True)
    return factor * (grad_norm - first_mean - normed * second_mean)


def three_parts(v):
    hi = v.astype(bf16).astype(f32)
    mid = (v - hi).astype(bf16).astype(f32)
    return hi, mid, v - hi - mid


def col_sum(v):
    return jnp.sum(v, axis=0, keepdims=True)


def micro_kernel(first, *refs):
    x_ref, g_ref, live_ref, w_ref, vec_ref, upb_ref = refs[:6]
    refs = refs[6:]
    if not first:
        prev_ref, vprev_ref, uprev_ref = refs[:3]
        refs = refs[3:]
    final_ref, tg_ref, grad_ref, vsum_ref, usum_ref = refs[:5]
    (q_ref, k_ref, v_ref, att_ref, qaug_ref, first_t, second_t, down_t, att_t, mixin_ref, mg_ref,
     dout_ref, hid_ref, pre_ref, kaug, vaug_a, vaug_b, dk_acc, dv_acc, acc_a, acc_b) = refs[5:]
    rows, width = x_ref.shape
    hidden = upb_ref.shape[1]
    blocks = rows // BLK
    pairs = width // 128
    mix_at = 3 * width
    up_at = mix_at + width
    down_at = up_at + hidden
    lane = lax.broadcasted_iota(jnp.int32, (1, 128), 1)
    low_half = lane < HEAD_DIM

    def at(i, size=BLK):
        return pl.ds(pl.multiple_of(i * size, size), size)

    if first:
        vsum_ref[...] = jnp.zeros_like(vsum_ref)
        usum_ref[...] = jnp.zeros_like(usum_ref)
    else:
        vsum_ref[...] = vprev_ref[...]
        usum_ref[...] = uprev_ref[...]

    def row(ref, n):
        return ref[n : n + 1, :]

    live_all = live_ref[...]
    mask_aug = jnp.where(
        lane == 0, (live_all - 1.0) * (-masked_score), jnp.where(lane < 4, 1.0, 0.0)
    ).astype(bf16)
    kaug[:, 128:] = mask_aug
    vaug_a[:, 128:] = jnp.ones((rows, 128), bf16)
    vaug_b[:, 128:] = jnp.ones((rows, 128), bf16)

    def project(i, carry):
        rs = at(i)
        normed, _ = normalize(x_ref[rs, :].astype(f32))
        first_in = (normed * row(vec_ref, 0) + row(vec_ref, 1)).astype(bf16)
        first_t[:, rs] = first_in.T
        query = (nn(first_in, w_ref[:, :width]) + row(vec_ref, 2)).astype(bf16)
        q_ref[rs, :] = query * jnp.array(HEAD_DIM ** (-0.5), bf16)
        k_ref[rs, :] = nn(first_in, w_ref[:, width : 2 * width]).astype(bf16)
        v_ref[rs, :] = (nn(first_in, w_ref[:, 2 * width : 3 * width]) + row(vec_ref, 3)).astype(bf16)
        return carry

    lax.fori_loop(0, blocks, project, 0)

    def attend_pair(p, carry):
        ls = at(p, 128)
        kaug[:, :128] = k_ref[:, ls]
        values = v_ref[:, ls]
        zero = jnp.zeros_like(values)
        vaug_a[:, :128] = jnp.where(low_half, values, zero)
        vaug_b[:, :128] = jnp.where(low_half, zero, values)

        def attend(i, carry):
            rs = at(i)
            query = q_ref[rs, ls]
            qzero = jnp.zeros_like(query)
            one = jnp.broadcast_to(jnp.where(lane == 0, 1.0, 0.0), (BLK, 128)).astype(bf16)
            out = None
            for half, vaug in ((0, vaug_a), (1, vaug_b)):
                mine = jnp.where(low_half if half == 0 else jnp.logical_not(low_half), query, qzero)
                scores = nt(jnp.concatenate([mine, one], axis=1), kaug[...])
                peak = jnp.max(scores, axis=-1, keepdims=True)
                chances = jnp.exp(scores - peak).astype(bf16)
                got = nn(chances, vaug[...])
                total = got[:, 128:]
                lse = peak + jnp.log(total)
                hi, mid, lo = three_parts(lse)
                qaug_ref[2 * p + half, rs, :] = jnp.where(
                    lane == 0, 1.0,
                    jnp.where(lane == 1, -hi, jnp.where(lane == 2, -mid, jnp.where(lane == 3, -lo, 0.0))),
                ).astype(bf16)
                part = got[:, :128] / total
                out = part if out is None else out + part
            att_ref[rs, ls] = out
            return carry

        return lax.fori_loop(0, blocks, attend, carry)

    lax.fori_loop(0, pairs, attend_pair, 0)

    chunk = 512
    mix_w = w_ref.at[:, mix_at:up_at]

    def feed(i, carry):
        rs = at(i)
        live = live_ref[rs, :]
        attended = att_ref[rs, :].astype(bf16)
        att_t[:, rs] = attended.T
        middle = x_ref[rs, :].astype(f32) + live * (nn(attended, mix_w[...]) + row(vec_ref, 4))
        second_norm, factor = normalize(middle)
        second_in = (second_norm * row(vec_ref, 5) + row(vec_ref, 6)).astype(bf16)
        second_t[:, rs] = second_in.T
        outer = g_ref[rs, :].astype(f32)
        down_in = (live * outer).astype(bf16)
        down_t[:, rs] = down_in.T
        vsum_ref[7:8, :] += col_sum(down_in.astype(f32))
        acc_a[...] = jnp.zeros_like(acc_a)
        acc_b[...] = jnp.zeros_like(acc_b)

        def part(c, carry):
            cs = at(c, chunk)
            up = w_ref[:, pl.ds(pl.multiple_of(up_at + c * chunk, chunk), chunk)]
            down = w_ref[:, pl.ds(pl.multiple_of(down_at + c * chunk, chunk), chunk)]
            pre = nn(second_in, up) + upb_ref[:, cs]
            phi = 0.5 * (1.0 + lax.erf(pre * root_half))
            hid = (pre * phi).astype(bf16)
            slope = phi + pre * jnp.exp(-0.5 * pre * pre) * gauss_norm
            hid_ref[rs, cs] = hid
            acc_a[...] += nt(hid, down)
            pre_grad = (nn(down_in, down) * slope).astype(bf16)
            pre_ref[rs, cs] = pre_grad
            usum_ref[:, cs] += col_sum(pre_grad.astype(f32))
            acc_b[...] += nt(pre_grad, up)
            return carry

        lax.fori_loop(0, hidden // chunk, part, 0)
        final_ref[rs, :] = (middle + live * (acc_a[...] + row(vec_ref, 7))).astype(bf16)
        second_in_grad = acc_b[...]
        vsum_ref[5:6, :] += col_sum(second_in_grad * second_norm)
        vsum_ref[6:7, :] += col_sum(second_in_grad)
        middle_grad = outer + norm_back(second_in_grad * row(vec_ref, 5), second_norm, factor)
        mg_ref[rs, :] = middle_grad
        mix_in = (live * middle_grad).astype(bf16)
        mixin_ref[rs, :] = mix_in
        vsum_ref[4:5, :] += col_sum(mix_in.astype(f32))
        dout_ref[rs, :] = nt(mix_in, mix_w[...]).astype(bf16)
        return carry

    lax.fori_loop(0, blocks, feed, 0)

    def put(value, cs):
        if not first:
            value = value + prev_ref[:, cs]
        grad_ref[:, cs] = value.astype(grad_ref.dtype)

    def wide(lhs_t, rhs_ref, base, count):
        def one(c, carry):
            put(nn(lhs_t[...], rhs_ref[:, at(c, chunk)]),
                pl.ds(pl.multiple_of(base + c * chunk, chunk), chunk))
            return carry
        lax.fori_loop(0, count, one, 0)

    wide(down_t, hid_ref, down_at, hidden // chunk)
    wide(second_t, pre_ref, up_at, hidden // chunk)
    wide(att_t, mixin_ref, mix_at, width // chunk)

    joint_grad = hid_ref

    def back_pair(p, carry):
        ls = at(p, 128)
        keys = k_ref[:, ls]
        kaug[:, :128] = keys
        vaug_a[:, :128] = v_ref[:, ls]
        vaug_a[:, 128:] = kaug[:, 128:]
        zero = jnp.zeros_like(keys)
        vaug_b[:, :128] = jnp.where(low_half, keys, zero)
        vaug_b[:, 128:] = jnp.where(low_half, zero, keys)
        dk_acc[...] = jnp.zeros_like(dk_acc)
        dv_acc[...] = jnp.zeros_like(dv_acc)

        def back(i, carry):
            rs = at(i)
            query = q_ref[rs, ls]
            grad = dout_ref[rs, ls]
            both = grad.astype(f32) * att_ref[rs, ls]
            dq = None
            for half in (0, 1):
                keep = low_half if half == 0 else jnp.logical_not(low_half)
                mine = jnp.where(keep, query, jnp.zeros_like(query))
                grads = jnp.where(keep, grad, jnp.zeros_like(grad))
                inner = jnp.sum(jnp.where(keep, both, 0.0), axis=-1, keepdims=True)
                hi, mid, lo = three_parts(inner)
                gaug = jnp.where(
                    lane == 1, -hi, jnp.where(lane == 2, -mid, jnp.where(lane == 3, -lo, 0.0))
                ).astype(bf16)
                scores = nt(kaug[...], jnp.concatenate([mine, qaug_ref[2 * p + half, rs, :]], axis=1))
                chances = jnp.exp(scores)
                centered = nt(vaug_a[...], jnp.concatenate([grads, gaug], axis=1))
                score_grad = (chances * centered).astype(bf16)
                dv_acc[...] += nn(chances.astype(bf16), grads)
                dk_acc[...] += nn(score_grad, mine)
                part = tn(score_grad, vaug_b[:, 128 * half : 128 * half + 128])
                dq = part if dq is None else dq + part
            joint_grad[rs, ls] = (dq * HEAD_DIM ** (-0.5)).astype(bf16)
            return carry

        lax.fori_loop(0, blocks, back, 0)
        joint_grad[:, pl.ds(pl.multiple_of(width + p * 128, 128), 128)] = dk_acc[...].astype(bf16)
        joint_grad[:, pl.ds(pl.multiple_of(2 * width + p * 128, 128), 128)] = dv_acc[...].astype(bf16)
        return carry

    lax.fori_loop(0, pairs, back_pair, 0)

    wide(first_t, joint_grad, 0, 3 * width // chunk)

    def back_first(i, carry):
        rs = at(i)
        grads = joint_grad[rs, : 3 * width]
        vsum_ref[2:3, :] += col_sum(grads[:, :width].astype(f32))
        vsum_ref[3:4, :] += col_sum(grads[:, 2 * width :].astype(f32))
        first_in_grad = nt(grads, w_ref[:, : 3 * width])
        normed, factor = normalize(x_ref[rs, :].astype(f32))
        vsum_ref[0:1, :] += col_sum(first_in_grad * normed)
        vsum_ref[1:2, :] += col_sum(first_in_grad)
        tg_ref[rs, :] = (
            mg_ref[rs, :] + norm_back(first_in_grad * row(vec_ref, 0), normed, factor)
        ).astype(bf16)
        return carry

    lax.fori_loop(0, blocks, back_first, 0)


def micro_call(x, g, live, weights, vec, upb, previous=None):
    rows, width = x.shape
    hidden = upb.shape[1]
    columns = weights.shape[1]
    first = previous is None
    vmem = pl.BlockSpec(memory_space=pltpu.VMEM)
    args = (x, g, live, weights, vec, upb) + (() if first else previous)
    scratch = [
        pltpu.VMEM((rows, width), bf16),
        pltpu.VMEM((rows, width), bf16),
        pltpu.VMEM((rows, width), bf16),
        pltpu.VMEM((rows, width), f32),
        pltpu.VMEM((HEADS, rows, 128), bf16),
        pltpu.VMEM((width, rows), bf16),
        pltpu.VMEM((width, rows), bf16),
        pltpu.VMEM((width, rows), bf16),
        pltpu.VMEM((width, rows), bf16),
        pltpu.VMEM((rows, width), bf16),
        pltpu.VMEM((rows, width), f32),
        pltpu.VMEM((rows, width), bf16),
        pltpu.VMEM((rows, hidden), bf16),
        pltpu.VMEM((rows, hidden), bf16),
        pltpu.VMEM((rows, 256), bf16),
        pltpu.VMEM((rows, 256), bf16),
        pltpu.VMEM((rows, 256), bf16),
        pltpu.VMEM((rows, 128), f32),
        pltpu.VMEM((rows, 128), f32),
        pltpu.VMEM((BLK, width), f32),
        pltpu.VMEM((BLK, width), f32),
    ]
    flops = 2 * rows * width * columns * 3 + 7 * 2 * rows * rows * width * 4
    return pl.pallas_call(
        functools.partial(micro_kernel, first),
        out_shape=(
            jax.ShapeDtypeStruct((rows, width), bf16),
            jax.ShapeDtypeStruct((rows, width), bf16),
            jax.ShapeDtypeStruct((width, 4 * width + 2 * hidden), f32 if first else bf16),
            jax.ShapeDtypeStruct((8, width), f32),
            jax.ShapeDtypeStruct((1, hidden), f32),
        ),
        in_specs=[vmem] * len(args),
        out_specs=(vmem,) * 5,
        scratch_shapes=scratch,
        compiler_params=pltpu.CompilerParams(vmem_limit_bytes=67_043_328),
        cost_estimate=pl.CostEstimate(flops=flops, bytes_accessed=30_000_000, transcendentals=3 * HEADS * rows * rows),
        name="micro_first" if first else "micro_second",
    )(*args)


MESH = pl.DeviceIdType.MESH


def split_axes():
    members, others = lax.axis_size("dp"), lax.axis_size("fsdp")
    return members // 2, 2, others // 2, 2


def my_place():
    d, f = lax.axis_index("dp"), lax.axis_index("fsdp")
    return d, f, (d // 2, lax.rem(d, 2), f // 2, lax.rem(f, 2))


def greet(members, others):
    d, f = lax.axis_index("dp"), lax.axis_index("fsdp")
    barrier = pltpu.get_barrier_semaphore()
    for s in range(1, members):
        pl.semaphore_signal(barrier, inc=1, device_id={"dp": lax.rem(d + s, members)}, device_id_type=MESH)
    for s in range(1, others):
        pl.semaphore_signal(barrier, inc=1, device_id={"fsdp": lax.rem(f + s, others)}, device_id_type=MESH)
    pl.semaphore_wait(barrier, members + others - 2)


class Swap:
    def __init__(self, src, dst, local, send, recv, members):
        d = lax.axis_index("dp")
        self.copies = []
        for s in range(1, members):
            to = lax.rem(d + s, members)
            self.copies.append(pltpu.make_async_remote_copy(
                src_ref=src.at[to], dst_ref=dst.at[d], send_sem=send.at[s], recv_sem=recv.at[s],
                device_id={"dp": to}, device_id_type=MESH))
        self.own = pltpu.make_async_copy(src.at[d], dst.at[d], local)

    def start(self):
        for copy in self.copies:
            copy.start()
        self.own.start()

    def wait(self):
        for copy in self.copies:
            copy.wait_recv()
        self.own.wait()

    def wait_sent(self):
        for copy in self.copies:
            copy.wait_send()


class Gather:
    def __init__(self, src, out, cs, order, local, send, recv, sizes):
        a, b, c, e = my_place()[2]
        d, f = lax.axis_index("dp"), lax.axis_index("fsdp")
        high, _, wide, _ = sizes
        every = slice(None)
        place = [a, b, c, e]
        self.own = pltpu.make_async_copy(src.at[:, cs], out.at[a, b, c, e, :, cs], local)
        self.stages = []
        done = [False] * 4
        slot = 0
        for number, axis in enumerate(order):
            copies = []
            size = (high, 2, wide, 2)[axis]
            for s in range(1, size):
                other = lax.rem(place[axis] + s, size)
                if axis == 0:
                    target = {"dp": other * 2 + b}
                elif axis == 1:
                    target = {"dp": a * 2 + other}
                elif axis == 2:
                    target = {"fsdp": other * 2 + e}
                else:
                    target = {"fsdp": c * 2 + other}
                where = tuple(every if done[k] else place[k] for k in range(4)) + (every, cs)
                source = src.at[:, cs] if number == 0 else out.at[where]
                copies.append(pltpu.make_async_remote_copy(
                    src_ref=source, dst_ref=out.at[where], send_sem=send.at[slot], recv_sem=recv.at[slot],
                    device_id=target, device_id_type=MESH))
                slot += 1
            self.stages.append(copies)
            done[axis] = True

    def start(self, number):
        if number == 0:
            self.own.start()
        for copy in self.stages[number]:
            copy.start()

    def wait(self, number):
        for copy in self.stages[number]:
            copy.wait_recv()
        if number == 0:
            self.own.wait()

    def wait_sent(self):
        for stage in self.stages:
            for copy in stage:
                copy.wait_send()


class Reduce:
    def __init__(self, grads, cs, wide_first, emit, scratch, send, recv, high):
        self.grads, self.cs, self.wide_first, self.emit, self.high = grads, cs, wide_first, emit, high
        self.from_core, self.after_core, self.from_one, self.after_one, self.from_two, self.after_two, self.last = scratch
        self.send, self.recv = send, recv
        self.sent = []

    def push(self, source, target, slot, device):
        copy = pltpu.make_async_remote_copy(
            src_ref=source, dst_ref=target, send_sem=self.send.at[slot], recv_sem=self.recv.at[slot],
            device_id=device, device_id_type=MESH)
        copy.start()
        self.sent.append(copy)
        self.copy = copy

    def start(self):
        _, _, (a, b, c, e) = my_place()
        self.push(self.grads.at[:, :, :, 1 - e, :, self.cs], self.from_core, 0, {"fsdp": c * 2 + 1 - e})

    def step(self, number):
        d, f, (a, b, c, e) = my_place()
        across = {"fsdp": (1 - c) * 2 + e}, {"dp": a * 2 + 1 - b}
        if number == 0:
            self.copy.wait_recv()

            def one(i, carry):
                mine = self.grads[i, :, :, e, :, self.cs]
                self.after_core[i] = (mine.astype(f32) + self.from_core[i].astype(f32)).astype(bf16)
                return carry

            lax.fori_loop(0, self.high, one, 0)
            if self.wide_first:
                self.push(self.after_core.at[:, :, 1 - c], self.from_one, 1, across[0])
            else:
                self.push(self.after_core.at[:, 1 - b], self.from_one, 1, across[1])
        elif number == 1:
            self.copy.wait_recv()

            def two(i, carry):
                mine = self.after_core[i, :, c] if self.wide_first else self.after_core[i, b]
                self.after_one[i] = (mine.astype(f32) + self.from_one[i].astype(f32)).astype(bf16)
                return carry

            lax.fori_loop(0, self.high, two, 0)
            if self.wide_first:
                self.push(self.after_one.at[:, 1 - b], self.from_two, 2, across[1])
            else:
                self.push(self.after_one.at[:, 1 - c], self.from_two, 2, across[0])
        elif number == 2:
            self.copy.wait_recv()

            def three(i, carry):
                mine = self.after_one[i, b] if self.wide_first else self.after_one[i, c]
                self.after_two[i] = (mine.astype(f32) + self.from_two[i].astype(f32)).astype(bf16)
                return carry

            lax.fori_loop(0, self.high, three, 0)
            self.copies = []
            for s in range(1, self.high):
                other = lax.rem(a + s, self.high)
                self.push(self.after_two.at[other], self.last.at[a], 2 + s, {"dp": other * 2 + b})
                self.copies.append(self.copy)
        else:
            for copy in self.copies:
                copy.wait_recv()
            total = self.after_two[a].astype(f32)
            for s in range(1, self.high):
                total = total + self.last[lax.rem(a + s, self.high)].astype(f32)
            self.emit(total)

    def wait_sent(self):
        for copy in self.sent:
            copy.wait_send()


def reduce_scratch(high, rows, columns):
    shapes = [(high, 2, 2), (high, 2, 2), (high, 2), (high, 2), (high,), (high,), (high,)]
    return [pltpu.VMEM(lead + (rows, columns), bf16) for lead in shapes]


def gather_kernel(sizes, members, others, ranges, shard, tokens, grads, out, tokens_out, grads_out, wsend, wrecv, tsend, trecv, local):
    greet(members, others)
    micro = tokens.shape[0]
    swaps = []
    for step in range(micro):
        for kind, (src, dst) in enumerate(((tokens, tokens_out), (grads, grads_out))):
            n = step * 2 + kind
            swaps.append(Swap(src.at[step], dst.at[step], local.at[n], tsend.at[n], trecv.at[n], members))
    gathers = [
        Gather(shard, out, cs, order, local.at[2 * micro + n], wsend.at[n], wrecv.at[n], sizes)
        for n, (cs, order) in enumerate(ranges)
    ]
    swaps[0].start()
    for gather in gathers:
        gather.start(0)
    for number in range(1, 4):
        for gather in gathers:
            gather.wait(number - 1)
            gather.start(number)
        if number == 1:
            for swap in swaps[1:]:
                swap.start()
    for gather in gathers:
        gather.wait(3)
    for swap in swaps:
        swap.wait()
    for item in swaps + gathers:
        item.wait_sent()


def scatter_kernel(high, members, others, widths, grads, extra, *refs):
    sources, refs = refs[:4], refs[4:]
    outs, refs = refs[:5], refs[5:]
    returned, refs = refs[:4], refs[4:]
    wsend, wrecv, tsend, trecv, local = refs[-5:]
    scratch = refs[:-5]
    greet(members, others)
    width, hidden = widths
    swaps = [
        Swap(src, dst, local.at[n], tsend.at[n], trecv.at[n], members)
        for n, (src, dst) in enumerate(zip(sources, returned))
    ]

    def emit_first(total):
        outs[0][...] = total[:, : 3 * width]
        outs[1][...] = total[:, 3 * width :]

    def emit_to(ref):
        def emit(total):
            ref[...] = total
        return emit

    up_at, down_at = 4 * width, 4 * width + hidden
    items = [
        Reduce(grads, pl.ds(down_at, hidden), True, emit_to(outs[3]), scratch[0:7], wsend.at[0], wrecv.at[0], high),
        Reduce(grads, pl.ds(up_at, hidden), False, emit_to(outs[2]), scratch[7:14], wsend.at[1], wrecv.at[1], high),
        Reduce(grads, pl.ds(0, up_at), True, emit_first, scratch[14:21], wsend.at[2], wrecv.at[2], high),
        Reduce(extra, pl.ds(0, 128), False, emit_to(outs[4]), scratch[21:28], wsend.at[3], wrecv.at[3], high),
    ]
    for item in items:
        item.start()
    for swap in swaps:
        swap.start()
    for number in range(4):
        for item in items:
            item.step(number)
    for swap in swaps:
        swap.wait()
    for item in items + swaps:
        item.wait_sent()


def order_kernel(scatter, table, *refs):
    count = (len(refs) - 3) // 2
    sources, targets = refs[:count], refs[count : 2 * count]
    held, in_sem, out_sem = refs[2 * count :]
    micro, members = sources[0].shape[:2]
    incoming, outgoing = [], []
    for n in range(count):
        for m in range(micro):
            for p in range(members):
                other = table[m, p]
                src, dst = (p, other) if scatter else (other, p)
                slot = (n * micro + m) * members + p
                copy = pltpu.make_async_copy(sources[n].at[m, src], held.at[slot], in_sem.at[slot])
                copy.start()
                incoming.append(copy)
                outgoing.append(pltpu.make_async_copy(held.at[slot], targets[n].at[m, dst], out_sem.at[slot]))
    for one, two in zip(incoming, outgoing):
        one.wait()
        two.start()
    for two in outgoing:
        two.wait()


ANY = pl.BlockSpec(memory_space=pl.ANY)
VMEM = pl.BlockSpec(memory_space=pltpu.VMEM)


def reorder(scatter, table, *arrays):
    micro, members, piece, width = arrays[0].shape
    slots = len(arrays) * micro * members
    return pl.pallas_call(
        functools.partial(order_kernel, scatter),
        out_shape=tuple(jax.ShapeDtypeStruct(item.shape, item.dtype) for item in arrays),
        in_specs=[pl.BlockSpec(memory_space=pltpu.SMEM)] + [ANY] * len(arrays),
        out_specs=(ANY,) * len(arrays),
        scratch_shapes=[
            pltpu.VMEM((slots, piece, width), arrays[0].dtype),
            pltpu.SemaphoreType.DMA((slots,)),
            pltpu.SemaphoreType.DMA((slots,)),
        ],
        name="order_out" if scatter else "order_in",
    )(table, *arrays)


def gather_call(shard, tokens, grads, members, others):
    rows, columns = shard.shape
    high, wide = members // 2, others // 2
    sizes = (high, 2, wide, 2)
    micro = tokens.shape[0]
    third = 2048
    ranges = (
        (pl.ds(0, third), (0, 1, 2, 3)),
        (pl.ds(third, third), (0, 2, 1, 3)),
        (pl.ds(2 * third, columns - 2 * third), (0, 1, 2, 3)),
    )
    slots = high + 1 + wide
    return pl.pallas_call(
        functools.partial(gather_kernel, sizes, members, others, ranges),
        out_shape=(
            jax.ShapeDtypeStruct(sizes + (rows, columns), shard.dtype),
            jax.ShapeDtypeStruct(tokens.shape, tokens.dtype),
            jax.ShapeDtypeStruct(grads.shape, grads.dtype),
        ),
        in_specs=[VMEM, ANY, ANY],
        out_specs=(ANY,) * 3,
        scratch_shapes=[
            pltpu.SemaphoreType.DMA((len(ranges), slots)),
            pltpu.SemaphoreType.DMA((len(ranges), slots)),
            pltpu.SemaphoreType.DMA((2 * micro, members)),
            pltpu.SemaphoreType.DMA((2 * micro, members)),
            pltpu.SemaphoreType.DMA((2 * micro + len(ranges),)),
        ],
        compiler_params=pltpu.CompilerParams(collective_id=0, has_side_effects=True),
        name="gather_in",
    )(shard, tokens, grads)


def scatter_call(grads, extra, arrays, members, others, width, hidden):
    high = members // 2
    rows = grads.shape[4]
    scratch = []
    for columns in (hidden, hidden, 4 * width, 128):
        scratch += reduce_scratch(high, rows, columns)
    shapes = [(rows, 3 * width), (rows, width), (rows, hidden), (rows, hidden), (rows, 128)]
    return pl.pallas_call(
        functools.partial(scatter_kernel, high, members, others, (width, hidden)),
        out_shape=tuple(jax.ShapeDtypeStruct(shape, f32) for shape in shapes)
        + tuple(jax.ShapeDtypeStruct(item.shape, item.dtype) for item in arrays),
        in_specs=[VMEM, VMEM] + [ANY] * 4,
        out_specs=(VMEM,) * 5 + (ANY,) * 4,
        scratch_shapes=scratch + [
            pltpu.SemaphoreType.DMA((4, high + 2)),
            pltpu.SemaphoreType.DMA((4, high + 2)),
            pltpu.SemaphoreType.DMA((4, members)),
            pltpu.SemaphoreType.DMA((4, members)),
            pltpu.SemaphoreType.DMA((4,)),
        ],
        compiler_params=pltpu.CompilerParams(
            collective_id=1, has_side_effects=True, vmem_limit_bytes=67_043_328),
        name="scatter_out",
    )(grads, extra, *arrays)


def body(
    tokens, out_grad, seq_lengths, send_to, slot_of, first_gain, first_shift, joint_weight, query_bias,
    value_bias, mix_weight, mix_bias, second_gain, second_shift, up_weight, up_bias, down_weight, down_bias,
):
    members, others = lax.axis_size("dp"), lax.axis_size("fsdp")
    devices = members * others
    micro, rows, width = tokens.shape
    piece = rows // members
    own = first_gain.shape[0]
    hidden = down_weight.shape[0]
    per = hidden // width
    vectors = (first_gain, first_shift, query_bias, value_bias, mix_bias, second_gain, second_shift, down_bias)
    small = jnp.concatenate(
        [jnp.stack(vectors, axis=1), up_bias.reshape(own, per), jnp.zeros((own, 128 - 8 - per), bf16)], axis=1)
    shard = jnp.concatenate([joint_weight, mix_weight, up_weight, down_weight.T, small], axis=1)
    table = send_to[:, 0]
    pieces = (micro, members, piece, width)
    sent = reorder(True, table, tokens.reshape(pieces), out_grad.reshape(pieces))
    gathered, routed, routed_grad = gather_call(shard, *sent, members, others)
    whole = gathered.reshape(width, shard.shape[1])
    tail = whole[:, 4 * width + 2 * hidden :].astype(f32)
    vec = tail[:, :8].T
    upb = tail[:, 8 : 8 + per].reshape(1, hidden)
    spots = slot_of[:, 0, :, None] * piece + jnp.arange(piece, dtype=jnp.int32)
    live = (spots.reshape(micro, rows) < seq_lengths).astype(f32)[:, :, None]
    previous = None
    results = []
    for step in range(micro):
        final, token_grad, *previous = micro_call(
            routed[step].reshape(rows, width), routed_grad[step].reshape(rows, width), live[step], whole, vec, upb,
            previous and tuple(previous))
        results += [final.reshape(members, piece, width), token_grad.reshape(members, piece, width)]
    total, vsum, usum = previous
    sizes = (members // 2, 2, others // 2, 2, own)
    grads = total.reshape(sizes + (total.shape[1],))
    extra = jnp.concatenate(
        [vsum.T, usum.reshape(width, per), jnp.zeros((width, 128 - 8 - per), f32)], axis=1
    ).astype(bf16).reshape(sizes + (128,))
    joint, mix, up, down, tail, *returned = scatter_call(grads, extra, results, members, others, width, hidden)
    layer_output, input_grad = reorder(
        False, table, jnp.stack([returned[0], returned[2]]), jnp.stack([returned[1], returned[3]]))
    vec_grad = [tail[:, n] for n in range(8)]
    return (
        layer_output.reshape(tokens.shape), input_grad.reshape(tokens.shape),
        vec_grad[0], vec_grad[1], joint, vec_grad[2], vec_grad[3], mix, vec_grad[4], vec_grad[5], vec_grad[6],
        up, tail[:, 8 : 8 + per].reshape(up_bias.shape), down.T, vec_grad[7],
    )


SMALL = 256


class Layer:
    def __init__(self, x, g, live, weight, offsets, vec, upb, final, tg, put, vsum, usum, scratch):
        self.x, self.g, self.live, self.weight, self.offsets = x, g, live, weight, offsets
        self.vec, self.upb, self.final, self.tg, self.put, self.vsum, self.usum = vec, upb, final, tg, put, vsum, usum
        (self.q, self.k, self.v, self.att, self.qaug, self.first_t, self.second_t, self.down_t, self.att_t, self.mixin,
         self.mg, self.dout, self.hid, self.pre, self.kaug, self.vaug_a, self.vaug_b, self.dk, self.dv, self.acc_a,
         self.acc_b) = scratch
        self.rows, self.width = self.q.shape
        self.hidden = upb.shape[1]
        self.blocks = self.rows // BLK
        self.pairs = self.width // 128
        self.lane = lax.broadcasted_iota(jnp.int32, (1, 128), 1)
        self.low = self.lane < HEAD_DIM

    def at(self, i, size=BLK):
        return pl.ds(pl.multiple_of(i * size, size), size)

    def row(self, n):
        return self.vec[n : n + 1, :]

    def load(self, ref, i):
        per = BLK // ref.shape[1]
        return ref[pl.ds(i * per, per)].reshape(BLK, self.width)

    def save(self, ref, i, value):
        per = BLK // ref.shape[1]
        ref[pl.ds(i * per, per)] = value.reshape(per, ref.shape[1], self.width)

    def masks(self):
        rows, lane = self.rows, self.lane
        self.kaug[:, 128:] = jnp.where(
            lane == 0, (self.live[...] - 1.0) * (-masked_score), jnp.where(lane < 4, 1.0, 0.0)
        ).astype(bf16)
        self.vaug_a[:, 128:] = jnp.ones((rows, 128), bf16)
        self.vaug_b[:, 128:] = jnp.ones((rows, 128), bf16)

    def project(self, turn, arrive):
        width = self.width

        def one(s, carry):
            arrive(s)
            i = turn(s)
            rs = self.at(i)
            normed, _ = normalize(self.load(self.x, i).astype(f32))
            first_in = (normed * self.row(0) + self.row(1)).astype(bf16)
            self.first_t[:, rs] = first_in.T
            query = (nn(first_in, self.weight(0, width)) + self.row(2)).astype(bf16)
            self.q[rs, :] = query * jnp.array(HEAD_DIM ** (-0.5), bf16)
            self.k[rs, :] = nn(first_in, self.weight(width, width)).astype(bf16)
            self.v[rs, :] = (nn(first_in, self.weight(2 * width, width)) + self.row(3)).astype(bf16)
            return carry

        lax.fori_loop(0, self.blocks, one, 0)

    def attend(self, hook):
        lane, low = self.lane, self.low

        def pair(p, carry):
            ls = self.at(p, 128)
            self.kaug[:, :128] = self.k[:, ls]
            values = self.v[:, ls]
            zero = jnp.zeros_like(values)
            self.vaug_a[:, :128] = jnp.where(low, values, zero)
            self.vaug_b[:, :128] = jnp.where(low, zero, values)

            def one(i, carry):
                rs = self.at(i)
                query = self.q[rs, ls]
                qzero = jnp.zeros_like(query)
                lead = jnp.broadcast_to(jnp.where(lane == 0, 1.0, 0.0), (BLK, 128)).astype(bf16)
                out = None
                for half, vaug in ((0, self.vaug_a), (1, self.vaug_b)):
                    mine = jnp.where(low if half == 0 else jnp.logical_not(low), query, qzero)
                    scores = nt(jnp.concatenate([mine, lead], axis=1), self.kaug[...])
                    peak = jnp.max(scores, axis=-1, keepdims=True)
                    chances = jnp.exp(scores - peak).astype(bf16)
                    got = nn(chances, vaug[...])
                    total = got[:, 128:]
                    hi, mid, lo = three_parts(peak + jnp.log(total))
                    self.qaug[2 * p + half, rs, :] = jnp.where(
                        lane == 0, 1.0,
                        jnp.where(lane == 1, -hi, jnp.where(lane == 2, -mid, jnp.where(lane == 3, -lo, 0.0))),
                    ).astype(bf16)
                    part = got[:, :128] / total
                    out = part if out is None else out + part
                self.att[rs, ls] = out
                hook(p * self.blocks + i)
                return carry

            return lax.fori_loop(0, self.blocks, one, carry)

        lax.fori_loop(0, self.pairs, pair, 0)

    def feed(self, turn, arrive, ready):
        chunk = 512
        mix_at, up_at, down_at = self.offsets

        def one(s, carry):
            arrive(s)
            i = turn(s)
            rs = self.at(i)
            live = self.live[rs, :]
            attended = self.att[rs, :].astype(bf16)
            self.att_t[:, rs] = attended.T
            mix_w = self.weight(mix_at, self.width)
            middle = self.load(self.x, i).astype(f32) + live * (nn(attended, mix_w) + self.row(4))
            second_norm, factor = normalize(middle)
            second_in = (second_norm * self.row(5) + self.row(6)).astype(bf16)
            self.second_t[:, rs] = second_in.T
            outer = self.load(self.g, i).astype(f32)
            down_in = (live * outer).astype(bf16)
            self.down_t[:, rs] = down_in.T
            self.vsum[7:8, :] += col_sum(down_in.astype(f32))
            self.acc_a[...] = jnp.zeros_like(self.acc_a)
            self.acc_b[...] = jnp.zeros_like(self.acc_b)

            def part(c, carry):
                ready(s, c)
                cs = self.at(c, chunk)
                up = self.weight(pl.multiple_of(up_at + c * chunk, 128), chunk)
                down = self.weight(pl.multiple_of(down_at + c * chunk, 128), chunk)
                pre = nn(second_in, up) + self.upb[:, cs]
                phi = 0.5 * (1.0 + lax.erf(pre * root_half))
                hid = (pre * phi).astype(bf16)
                slope = phi + pre * jnp.exp(-0.5 * pre * pre) * gauss_norm
                self.hid[c, rs, :] = hid
                self.acc_a[...] += nt(hid, down)
                pre_grad = (nn(down_in, down) * slope).astype(bf16)
                self.pre[c, rs, :] = pre_grad
                self.usum[:, cs] += col_sum(pre_grad.astype(f32))
                self.acc_b[...] += nt(pre_grad, up)
                return carry

            lax.fori_loop(0, self.hidden // chunk, part, 0)
            self.save(self.final, i, (middle + live * (self.acc_a[...] + self.row(7))).astype(bf16))
            second_in_grad = self.acc_b[...]
            self.vsum[5:6, :] += col_sum(second_in_grad * second_norm)
            self.vsum[6:7, :] += col_sum(second_in_grad)
            middle_grad = outer + norm_back(second_in_grad * self.row(5), second_norm, factor)
            self.mg[rs, :] = middle_grad
            mix_in = (live * middle_grad).astype(bf16)
            self.mixin[rs, :] = mix_in
            self.vsum[4:5, :] += col_sum(mix_in.astype(f32))
            self.dout[rs, :] = nt(mix_in, mix_w).astype(bf16)
            return carry

        lax.fori_loop(0, self.blocks, one, 0)

    def wide(self, lhs_t, rhs, base, count):
        def one(c, carry):
            self.put((base + c) * 512, nn(lhs_t[...], rhs[c]))
            return carry

        lax.fori_loop(0, count, one, 0)

    def down_grad(self):
        self.wide(self.down_t, self.hid, 0, self.hidden // 512)

    def up_grad(self):
        self.wide(self.second_t, self.pre, self.hidden // 512, self.hidden // 512)

    def mix_grad(self):
        self.put(2 * self.hidden, nn(self.att_t[...], self.mixin[...]))

    def attend_back(self, hook, done):
        lane, low = self.lane, self.low
        joint = self.hid

        def pair(p, carry):
            ls = self.at(p, 128)
            keys = self.k[:, ls]
            self.kaug[:, :128] = keys
            self.vaug_a[:, :128] = self.v[:, ls]
            self.vaug_a[:, 128:] = self.kaug[:, 128:]
            zero = jnp.zeros_like(keys)
            self.vaug_b[:, :128] = jnp.where(low, keys, zero)
            self.vaug_b[:, 128:] = jnp.where(low, zero, keys)
            self.dk[...] = jnp.zeros_like(self.dk)
            self.dv[...] = jnp.zeros_like(self.dv)

            def one(i, carry):
                rs = self.at(i)
                query = self.q[rs, ls]
                grad = self.dout[rs, ls]
                both = grad.astype(f32) * self.att[rs, ls]
                dq = None
                for half in (0, 1):
                    keep = low if half == 0 else jnp.logical_not(low)
                    mine = jnp.where(keep, query, jnp.zeros_like(query))
                    grads = jnp.where(keep, grad, jnp.zeros_like(grad))
                    hi, mid, lo = three_parts(jnp.sum(jnp.where(keep, both, 0.0), axis=-1, keepdims=True))
                    gaug = jnp.where(
                        lane == 1, -hi, jnp.where(lane == 2, -mid, jnp.where(lane == 3, -lo, 0.0))
                    ).astype(bf16)
                    scores = nt(self.kaug[...], jnp.concatenate([mine, self.qaug[2 * p + half, rs, :]], axis=1))
                    chances = jnp.exp(scores)
                    centered = nt(self.vaug_a[...], jnp.concatenate([grads, gaug], axis=1))
                    score_grad = (chances * centered).astype(bf16)
                    self.dv[...] += nn(chances.astype(bf16), grads)
                    self.dk[...] += nn(score_grad, mine)
                    part = tn(score_grad, self.vaug_b[:, 128 * half : 128 * half + 128])
                    dq = part if dq is None else dq + part
                joint[0, rs, ls] = (dq * HEAD_DIM ** (-0.5)).astype(bf16)
                hook(p * self.blocks + i)
                return carry

            lax.fori_loop(0, self.blocks, one, 0)
            joint[1, :, ls] = self.dk[...].astype(bf16)
            joint[2, :, ls] = self.dv[...].astype(bf16)
            grads = jnp.concatenate([joint[0, :, ls], joint[1, :, ls], joint[2, :, ls]], axis=1)
            self.put(2 * self.hidden + self.width + p * 384, nn(self.first_t[...], grads))
            done(p)
            return carry

        lax.fori_loop(0, self.pairs, pair, 0)

    def first_back(self, turn, done):
        width = self.width

        def one(s, carry):
            i = turn(s)
            rs = self.at(i)
            grads = jnp.concatenate([self.hid[0, rs, :], self.hid[1, rs, :], self.hid[2, rs, :]], axis=1)
            self.vsum[2:3, :] += col_sum(grads[:, :width].astype(f32))
            self.vsum[3:4, :] += col_sum(grads[:, 2 * width :].astype(f32))
            first_in_grad = nt(grads, self.weight(0, 3 * width))
            normed, factor = normalize(self.load(self.x, i).astype(f32))
            self.vsum[0:1, :] += col_sum(first_in_grad * normed)
            self.vsum[1:2, :] += col_sum(first_in_grad)
            token_grad = self.mg[rs, :] + norm_back(first_in_grad * self.row(0), normed, factor)
            self.save(self.tg, i, token_grad.astype(bf16))
            done(s)
            return carry

        lax.fori_loop(0, self.blocks, one, 0)


def layer_scratch(rows, width, hidden):
    return [
        pltpu.VMEM((rows, width), bf16),
        pltpu.VMEM((rows, width), bf16),
        pltpu.VMEM((rows, width), bf16),
        pltpu.VMEM((rows, width), f32),
        pltpu.VMEM((HEADS, rows, 128), bf16),
        pltpu.VMEM((width, rows), bf16),
        pltpu.VMEM((width, rows), bf16),
        pltpu.VMEM((width, rows), bf16),
        pltpu.VMEM((width, rows), bf16),
        pltpu.VMEM((rows, width), bf16),
        pltpu.VMEM((rows, width), f32),
        pltpu.VMEM((rows, width), bf16),
        pltpu.VMEM((hidden // 512, rows, 512), bf16),
        pltpu.VMEM((hidden // 512, rows, 512), bf16),
        pltpu.VMEM((rows, 256), bf16),
        pltpu.VMEM((rows, 256), bf16),
        pltpu.VMEM((rows, 256), bf16),
        pltpu.VMEM((rows, 128), f32),
        pltpu.VMEM((rows, 128), f32),
        pltpu.VMEM((BLK, width), f32),
        pltpu.VMEM((BLK, width), f32),
    ]


class Route:
    def __init__(self, src, dst, local, send, recv, members):
        self.src, self.dst, self.send, self.recv, self.members = src, dst, send, recv, members
        self.me = lax.axis_index("dp")
        self.own = pltpu.make_async_copy(src.at[self.me], dst.at[self.me], local)

    def outgoing(self, to):
        slot = lax.rem(to - self.me + self.members, self.members)
        return pltpu.make_async_remote_copy(
            src_ref=self.src.at[to], dst_ref=self.dst.at[self.me], send_sem=self.send.at[slot],
            recv_sem=self.recv.at[slot], device_id={"dp": to}, device_id_type=MESH)

    def incoming(self, source):
        slot = lax.rem(self.me - source + self.members, self.members)
        return pltpu.make_async_remote_copy(
            src_ref=self.src.at[source], dst_ref=self.dst.at[source], send_sem=self.send.at[slot],
            recv_sem=self.recv.at[slot], device_id={"dp": source}, device_id_type=MESH)

    def beside(self):
        return self.me + 1 - 2 * lax.rem(self.me, 2)

    def pair(self, s):
        block = lax.rem(self.me // 2 + s, self.members // 2)
        return 2 * block, 2 * block + 1

    def start(self):
        self.start_direct()
        self.start_others()

    def start_direct(self):
        for s in range(1, self.members // 2):
            self.outgoing(lax.rem(self.me + 2 * s, self.members)).start()
        self.outgoing(self.beside()).start()
        self.own.start()

    def start_others(self):
        for s in range(1, self.members // 2):
            self.outgoing(lax.rem(self.beside() + 2 * s, self.members)).start()

    def give(self, s):
        @pl.when(s > 0)
        def _():
            self.outgoing(lax.rem(self.me + 2 * s, self.members)).start()

        @pl.when(s == 0)
        def _():
            self.outgoing(self.beside()).start()
            self.own.start()

    def take(self, s):
        @pl.when(s > 0)
        def _():
            for source in self.pair(s):
                self.incoming(source).wait_recv()

        @pl.when(s == 0)
        def _():
            self.own.wait()
            self.incoming(self.beside()).wait_recv()

    def wait(self):
        for s in range(1, self.members):
            self.incoming(lax.rem(self.me + s, self.members)).wait_recv()
        self.own.wait()

    def wait_sent(self):
        for s in range(1, self.members):
            self.outgoing(lax.rem(self.me + s, self.members)).wait_send()


class Exchange:
    def __init__(self, grads, cs, wide_first, emit, scratch, send, recv, high):
        self.grads, self.cs, self.wide_first, self.emit, self.high = grads, cs, wide_first, emit, high
        self.from_core, self.from_one, self.from_two, self.last = scratch
        _, _, (a, b, c, e) = my_place()
        self.place = (a, b, c, e)
        across = {"fsdp": (1 - c) * 2 + e}, {"dp": a * 2 + 1 - b}

        def describe(source, target, slot, device):
            return pltpu.make_async_remote_copy(
                src_ref=source, dst_ref=target, send_sem=send.at[slot], recv_sem=recv.at[slot],
                device_id=device, device_id_type=MESH)

        stages = [[describe(grads.at[:, :, :, 1 - e, :, cs], self.from_core, 0, {"fsdp": c * 2 + 1 - e})]]
        if wide_first:
            stages.append([describe(grads.at[:, :, 1 - c, e, :, cs], self.from_one, 1, across[0])])
            stages.append([describe(grads.at[:, 1 - b, c, e, :, cs], self.from_two, 2, across[1])])
        else:
            stages.append([describe(grads.at[:, 1 - b, :, e, :, cs], self.from_one, 1, across[1])])
            stages.append([describe(grads.at[:, b, 1 - c, e, :, cs], self.from_two, 2, across[0])])
        copies = []
        for s in range(1, high):
            other = lax.rem(a + s, high)
            copies.append(describe(
                grads.at[other, b, c, e, :, cs], self.last.at[a], 2 + s, {"dp": other * 2 + b}))
        stages.append(copies)
        self.stages = stages

    def launch(self, number):
        for copy in self.stages[number]:
            copy.start()

    def start(self):
        self.launch(0)

    def step(self, number):
        a, b, c, e = self.place
        grads, cs = self.grads, self.cs
        for copy in self.stages[number]:
            copy.wait_recv()
        if number == 0:
            def one(i, carry):
                mine = grads[i, :, :, e, :, cs].astype(f32)
                grads[i, :, :, e, :, cs] = (mine + self.from_core[i].astype(f32)).astype(bf16)
                return carry
        elif number == 1 and self.wide_first:
            def one(i, carry):
                mine = grads[i, :, c, e, :, cs].astype(f32)
                grads[i, :, c, e, :, cs] = (mine + self.from_one[i].astype(f32)).astype(bf16)
                return carry
        elif number == 1:
            def one(i, carry):
                mine = grads[i, b, :, e, :, cs].astype(f32)
                grads[i, b, :, e, :, cs] = (mine + self.from_one[i].astype(f32)).astype(bf16)
                return carry
        elif number == 2:
            def one(i, carry):
                mine = grads[i, b, c, e, :, cs].astype(f32)
                grads[i, b, c, e, :, cs] = (mine + self.from_two[i].astype(f32)).astype(bf16)
                return carry
        if number < 3:
            lax.fori_loop(0, self.high, one, 0)
            self.launch(number + 1)
        else:
            total = grads[a, b, c, e, :, cs].astype(f32)
            for s in range(1, self.high):
                total = total + self.last[lax.rem(a + s, self.high)].astype(f32)
            self.emit(total)

    def wait_sent(self):
        for stage in self.stages:
            for copy in stage:
                copy.wait_send()


def exchange_scratch(high, rows, columns):
    return [pltpu.VMEM(lead + (rows, columns), bf16) for lead in ((high, 2, 2), (high, 2), (high,), (high,))]


def fill_vectors(small, vec, upb):
    devices, own, _ = small.shape
    rows = small[:, :, :128].reshape(devices * own, 128).astype(f32)
    spot = lax.broadcasted_iota(jnp.int32, rows.shape, 1)
    turn = lax.broadcasted_iota(jnp.int32, rows.shape, 0)
    mine = jnp.where(lax.rem(spot, own) == lax.rem(turn, own), rows, 0.0).astype(bf16)
    lanes = lax.broadcasted_iota(jnp.int32, (16, 128), 1)
    picks = lax.broadcasted_iota(jnp.int32, (16, 128), 0)
    choose = jnp.where(lanes - picks * own == lax.rem(lanes, own), 1.0, 0.0).astype(bf16)
    vec[...] = nt(choose, mine)[:8]
    low = lax.broadcasted_iota(jnp.int32, (1, 128), 1) < 64
    for i in range(devices // 2):
        left, right = small[2 * i, :, 128:].astype(f32), small[2 * i + 1, :, 128:].astype(f32)
        upb[:, 128 * i : 128 * i + 128] = jnp.where(low, left[0:1], right[0:1])


def at_points(index, plan):
    for point, action in plan:
        @pl.when(index == point)
        def _(action=action):
            action()


def permute(target, source, table, m, inverse=False):
    count = target.shape[0]

    def one(n, carry):
        if inverse:
            spot = jnp.int32(0)
            for k in range(1, count):
                spot = jnp.where(table[m, k] == n, k, spot)
        else:
            spot = table[m, n]
        target[n] = source[spot]
        return carry

    lax.fori_loop(0, count, one, 0)


def hail(members, others):
    d, f = lax.axis_index("dp"), lax.axis_index("fsdp")
    barrier = pltpu.get_barrier_semaphore()
    for s in range(1, members):
        pl.semaphore_signal(barrier, inc=1, device_id={"dp": lax.rem(d + s, members)}, device_id_type=MESH)
    for s in range(1, others):
        pl.semaphore_signal(barrier, inc=1, device_id={"fsdp": lax.rem(f + s, others)}, device_id_type=MESH)


def layer_kernel(sizes, members, others, *refs):
    goes_to, slot, length, joint, mix, up, down, *vectors, tokens, grads = refs[:18]
    joint_out, mix_out, up_out, down_out, tail_out, bias_out, layer_out, input_out = refs[18:26]
    (shard, weights, held, taken, back_0, back_1, back_2, back_3, total, extra, live, vec, upb, vsum, usum,
     wsend, wrecv, tsend, trecv, rsend, rrecv, local) = refs[26:48]
    back = (back_0, back_1, back_2, back_3)
    pools = [refs[48 + 4 * n : 52 + 4 * n] for n in range(5)]
    scratch = refs[68:]
    high = sizes[0]
    own, hidden = up.shape
    width = mix.shape[1]
    piece = tokens.shape[2]
    devices = members * others
    z = lax.axis_index("dp") // 2

    hail(members, others)

    loads = [
        pltpu.make_async_copy((grads if n % 2 else tokens).at[n // 2], back[n], local.at[n]) for n in range(4)
    ]
    for load in loads:
        load.start()
    mix_at = 3 * width + SMALL
    up_at = mix_at + width
    down_at = up_at + hidden
    shard[:, : 3 * width] = joint[...]
    spread = [jnp.broadcast_to(vector[...].astype(f32), (own, vector.shape[1])) for vector in vectors]
    shard[:, 3 * width : mix_at] = jnp.concatenate(spread + spread[-1:], axis=1).astype(bf16)
    shard[:, mix_at:up_at] = mix[...]
    shard[:, up_at:down_at] = up[...]
    shard[:, down_at:] = down[...]
    loads[0].wait()
    permute(held.at[0], back[0], goes_to, 0, inverse=True)
    pl.semaphore_wait(pltpu.get_barrier_semaphore(), members + others - 2)

    into = [
        Route(held.at[n], taken.at[n], local.at[4 + n], tsend.at[n], trecv.at[n], members) for n in range(4)
    ]
    returns = [
        Route(held.at[n], back[n], local.at[8 + n], tsend.at[4 + n], trecv.at[4 + n], members) for n in range(4)
    ]
    results = [
        pltpu.make_async_copy(taken.at[n], (input_out if n % 2 else layer_out).at[n // 2], local.at[12 + n])
        for n in range(4)
    ]
    ranges = (
        (pl.ds(0, 1024), (0, 1, 2, 3)),
        (pl.ds(1024, mix_at - 1024), (0, 2, 1, 3)),
        (pl.ds(mix_at, width), (0, 1, 2, 3)),
        (pl.ds(up_at, hidden // 2), (0, 1, 2, 3)),
        (pl.ds(down_at, hidden // 2), (0, 2, 1, 3)),
        (pl.ds(up_at + hidden // 2, hidden // 2), (0, 1, 2, 3)),
        (pl.ds(down_at + hidden // 2, hidden // 2), (0, 2, 1, 3)),
    )
    gathers = [
        Gather(shard, weights, cs, order, local.at[16 + n], wsend.at[n], wrecv.at[n], sizes)
        for n, (cs, order) in enumerate(ranges)
    ]
    early, late = gathers[:2], gathers[2:]
    for gather in early:
        gather.start(0)
    into[0].start_direct()
    for n in range(1, 4):
        loads[n].wait()
        permute(held.at[n], back[n], goes_to, n // 2, inverse=True)
    for number in range(1, 4):
        for gather in early:
            gather.wait(number - 1)
            gather.start(number)
        if number == 2:
            into[0].start_others()
            for gather in late:
                gather.start(0)
    into[1].start_direct()
    vsum[...] = jnp.zeros_like(vsum)
    usum[...] = jnp.zeros_like(usum)

    def mark(m):
        places = lax.broadcasted_iota(jnp.int32, (piece, 1), 0)
        for n in range(members):
            live[n * piece : (n + 1) * piece, :] = jnp.where(
                places + slot[m, n] * piece < length[0, m], 1.0, 0.0)

    def weight(start, size):
        return weights[:, :, :, :, :, pl.ds(start, size)].reshape(width, size)

    def put_first(start, value):
        cs = pl.ds(pl.multiple_of(start, 128), value.shape[1])
        total[:, :, :, :, :, cs] = value.astype(bf16).reshape(sizes + (own, value.shape[1]))

    def put_second(start, value):
        cs = pl.ds(pl.multiple_of(start, 128), value.shape[1])
        value = value + total[:, :, :, :, :, cs].reshape(value.shape).astype(f32)
        total[:, :, :, :, :, cs] = value.astype(bf16).reshape(sizes + (own, value.shape[1]))

    def turn(s):
        return lax.rem(z + s, high)

    def turn_last(s):
        return lax.rem(z + 1 + s, high)

    def nothing(s):
        pass

    first, second = (
        Layer(taken.at[2 * m], taken.at[2 * m + 1], live, weight, (mix_at, up_at, down_at), vec, upb,
              held.at[2 * m], held.at[2 * m + 1], put, vsum, usum, scratch)
        for m, put in enumerate((put_first, put_second))
    )

    mark(0)
    first.masks()
    for gather in early:
        gather.wait(3)
    fill_vectors(weights[:, :, :, :, :, 3 * width : mix_at].reshape(devices, own, SMALL), vec, upb)

    def arrive_tokens(s):
        into[0].take(s)

    first.project(turn, arrive_tokens)

    def relay(gather, number):
        def action():
            gather.wait(number - 1)
            gather.start(number)
        return action

    mixed, up_0, down_0, up_1, down_1 = late
    plan = [
        (0, relay(mixed, 1)), (1, relay(up_0, 1)), (2, relay(mixed, 2)), (3, relay(down_0, 1)), (4, relay(up_0, 2)),
        (5, relay(mixed, 3)), (6, relay(up_1, 1)), (6, relay(down_0, 2)), (8, relay(down_1, 1)), (11, relay(up_1, 2)),
        (12, relay(up_0, 3)), (13, relay(down_1, 2)), (13, into[1].start_others), (14, relay(down_0, 3)),
    ]
    first.attend(lambda h: at_points(h, plan))
    for gather in late[:3]:
        gather.wait(3)
    into[0].wait_sent()

    def ready(s, c):
        @pl.when((s == 0) & (c == 1))
        def _():
            relay(up_1, 3)()
            relay(down_1, 3)()

        @pl.when((s == 0) & (c == 2))
        def _():
            up_1.wait(3)
            down_1.wait(3)

    def arrive_grads(s):
        into[1].take(s)

        @pl.when(s == high - 1)
        def _():
            into[2].start()
            into[3].start()

    first.feed(turn, arrive_grads, ready)
    returns[0].start()
    into[1].wait_sent()
    first.down_grad()
    first.up_grad()
    first.mix_grad()
    first.attend_back(nothing, nothing)
    first.first_back(turn, nothing)
    returns[1].start()

    def emit_to(ref):
        def emit(value):
            ref[...] = value
        return emit

    def emit_tail(value):
        tail_out[...] = value[:, :128].T[:8]
        odd = lax.rem(lax.axis_index("fsdp"), 2) == 1
        bias_out[...] = jnp.where(odd, value[:1, 192:256], value[:1, 128:192])

    def emit_pair(value):
        up_out[...] = value[:, :hidden]
        mix_out[...] = value[:, hidden:]

    def emit_joint(start, count):
        def emit(value):
            for p in range(count):
                for j in range(3):
                    spot = j * width + (start + p) * 128
                    joint_out[:, spot : spot + 128] = value[:, p * 384 + j * 128 : p * 384 + j * 128 + 128]
        return emit

    joint_at, pairs = 2 * hidden + width, width // 128
    downs, ups, rest, rest_last, last = (
        Exchange(source, cs, wide_first, emit, pools[n], rsend.at[n], rrecv.at[n], high)
        for n, (source, cs, wide_first, emit) in enumerate((
            (total, pl.ds(0, hidden), True, emit_to(down_out)),
            (total, pl.ds(hidden, hidden + width), False, emit_pair),
            (total, pl.ds(joint_at, 384 * (pairs - 1)), False, emit_joint(0, pairs - 1)),
            (total, pl.ds(joint_at + 384 * (pairs - 1), 384), False, emit_joint(pairs - 1, 1)),
            (extra, pl.ds(0, SMALL), False, emit_tail),
        ))
    )
    mark(1)
    second.masks()
    into[2].wait()
    second.project(turn, nothing)
    second.attend(nothing)
    into[2].wait_sent()
    into[3].wait()
    second.feed(turn, nothing, lambda s, c: None)
    returns[2].start()
    into[3].wait_sent()
    second.down_grad()
    downs.start()
    second.up_grad()
    second.mix_grad()
    ups.start()

    def result(n):
        def action():
            returns[n].wait()
            permute(taken.at[n], back[n], goes_to, n // 2)
            results[n].start()
        return action

    def step(exchange, number):
        return lambda: exchange.step(number)

    plan_back = [
        (0, step(downs, 0)), (1, step(ups, 0)), (3, result(0)), (6, step(downs, 1)), (8, step(ups, 1)),
        (9, result(1)), (10, step(downs, 2)), (12, step(ups, 2)), (14, step(rest, 0)), (15, step(downs, 3)),
    ]
    second.attend_back(
        lambda h: at_points(h, plan_back), lambda p: at_points(p, [(pairs - 2, rest.start), (pairs - 1, rest_last.start)]))

    def send_grads(s):
        returns[3].give(lax.rem(s + 1, high))
        at_points(s, [(0, step(rest_last, 0)), (high - 1, step(rest, 1))])

    second.first_back(turn_last, send_grads)
    turned = jnp.concatenate([vsum[...], jnp.zeros((120, width), f32)], axis=0).T
    extra[:, :, :, :, :, :128] = turned.astype(bf16).reshape(sizes + (own, 128))
    for n in range(devices):
        a, b, c, e = n // (2 * others), (n // others) % 2, (n % others) // 2, n % 2
        part = usum[:, 128 * (n // 2) : 128 * (n // 2) + 128]
        extra[a, b, c, e, :, 128:] = jnp.broadcast_to(part, (own, 128)).astype(bf16)
    last.start()
    rest_last.step(1)
    last.step(0)
    returns[3].start_others()
    rest.step(2)
    ups.step(3)
    rest_last.step(2)
    last.step(1)
    last.step(2)
    result(2)()
    for item in (rest, rest_last, last):
        item.step(3)
    result(3)()
    for item in gathers + returns + [downs, ups, rest, rest_last, last]:
        item.wait_sent()
    for item in results:
        item.wait()


def layer_call(tables, shards, tokens, grads, members, others):
    joint, mix, up, down, *vectors = shards
    own, hidden = up.shape
    _, _, piece, width = tokens.shape
    rows = members * piece
    sizes = (members // 2, 2, others // 2, 2)
    high = sizes[0]
    slots = high + 1 + sizes[2]
    columns = 4 * width + 2 * hidden
    dma = pltpu.SemaphoreType.DMA
    smem = pl.BlockSpec(memory_space=pltpu.SMEM)
    pools = []
    for count in (hidden, hidden + width, 3 * width - 384, 384, SMALL):
        pools += exchange_scratch(high, own, count)
    shapes = [(own, 3 * width), (own, width), (own, hidden), (own, hidden), (8, own), (1, 2 * SMALL // 8)]
    blocks = pltpu.VMEM((4, members, piece, width), bf16)
    return pl.pallas_call(
        functools.partial(layer_kernel, sizes, members, others),
        out_shape=tuple(jax.ShapeDtypeStruct(shape, f32) for shape in shapes)
        + (jax.ShapeDtypeStruct(tokens.shape, bf16),) * 2,
        in_specs=[smem] * 3 + [VMEM] * (4 + len(vectors)) + [ANY] * 2,
        out_specs=(VMEM,) * 6 + (ANY,) * 2,
        scratch_shapes=[
            pltpu.VMEM((own, columns + SMALL), bf16),
            pltpu.VMEM(sizes + (own, columns + SMALL), bf16),
            blocks, blocks,
        ] + [pltpu.VMEM((members, piece, width), bf16)] * 4 + [
            pltpu.VMEM(sizes + (own, columns), bf16),
            pltpu.VMEM(sizes + (own, SMALL), bf16),
            pltpu.VMEM((rows, 1), f32),
            pltpu.VMEM((8, width), f32), pltpu.VMEM((1, hidden), f32),
            pltpu.VMEM((8, width), f32), pltpu.VMEM((1, hidden), f32),
            dma((7, slots)), dma((7, slots)), dma((8, members)), dma((8, members)),
            dma((5, high + 2)), dma((5, high + 2)), dma((23,)),
        ] + pools + layer_scratch(rows, width, hidden),
        compiler_params=pltpu.CompilerParams(
            collective_id=2, has_side_effects=True, vmem_limit_bytes=67_043_328),
        name="layer",
    )(*tables, *shards, tokens, grads)


def fused_body(
    tokens, out_grad, seq_lengths, send_to, slot_of, first_gain, first_shift, joint_weight, query_bias,
    value_bias, mix_weight, mix_bias, second_gain, second_shift, up_weight, up_bias, down_weight, down_bias,
):
    members, others = lax.axis_size("dp"), lax.axis_size("fsdp")
    micro, rows, width = tokens.shape
    vectors = (first_gain, first_shift, query_bias, value_bias, mix_bias, second_gain, second_shift, down_bias, up_bias)
    pieces = (micro, members, rows // members, width)
    joint, mix, up, down, tail, bias, layer_output, input_grad = layer_call(
        (send_to[:, 0], slot_of[:, 0], seq_lengths.reshape(1, micro)),
        (joint_weight, mix_weight, up_weight, down_weight.T) + tuple(vector[None] for vector in vectors),
        tokens.reshape(pieces), out_grad.reshape(pieces), members, others)
    vec_grad = [tail[n] for n in range(8)]
    return (
        layer_output.reshape(tokens.shape), input_grad.reshape(tokens.shape),
        vec_grad[0], vec_grad[1], joint, vec_grad[2], vec_grad[3], mix, vec_grad[4], vec_grad[5], vec_grad[6],
        up, bias[0], down.T, vec_grad[7],
    )


def solution(mesh):
    both = ("dp", "fsdp")
    row3, row2, vector, matrix = P(None, both, None), P(None, both), P(both), P(both, None)
    turned = P(None, both)
    members, others = mesh.shape["dp"], mesh.shape["fsdp"]
    fits = members * others == 32 and others == 4
    return jax.shard_map(
        fused_body if fits else body,
        mesh=mesh,
        in_specs=(row3, row3, row2, row3, row3, vector, vector, matrix, vector, vector, matrix, vector, vector,
                  vector, matrix, vector, turned, vector),
        out_specs=(row3, row3, vector, vector, matrix, vector, vector, matrix, vector, vector, vector, matrix,
                   vector, turned, vector),
        check_vma=False,
    )
```
